32 devices in a mesh: tm: 8 (over z, x), hid: 4 (over y, core).
Axes of the slice: x: 2, y: 2, z: 4, core: 2. Of those that a mesh axis runs over, the one named last changes fastest.
Arguments:
- token_ids: int32 [4096], P('tm'), may hold values from 0 to 255
- input_table: float32 [256, 3, 2048], P(None, None, 'hid'), may hold values from -6 to 6
- recur_weight: bfloat16 [2048, 3, 2048], P(None, None, 'hid'), may hold values from -0.125 to 0.125
- z_bias: float32 [2048], P('hid'), may hold values from -1 to 9
- hn_bias: float32 [2048], P('hid'), may hold values from -4 to 4
- init_state: float32 [2048], P('hid'), may hold values from -0.9 to 0.9
- guess: float32 [4096, 2048], P('tm', 'hid'), may hold values from -3 to 3
Outputs:
- states: float32 [4096, 2048], P('tm', 'hid')
- residual_norm: float32 [2], replicated
The draws below stay inside these ranges and needn't reach their ends.
All inputs are finite; a program needn't handle non-finite values.
Results may differ from the reference program's by a relative error of at most 0.00063.
Values may be sent and summed in bfloat16 or wider, within the bound.
No kernel may reach another device: no remote copies, remote signals or barrier semaphores. Data moves between devices by JAX's collectives and lax.ppermute only.
A program may use at most 128 MiB of HBM per device.

```python
import math
import jax
import jax.numpy as jnp
import numpy as np
from jax import lax

H = 2048
V = 256
TOK_DEV = 512
ITERS = 2
TOKENS = 4096


def draw_guess(key, part):
    ramp = jnp.arange(TOKENS, dtype=jnp.float32) / TOKENS
    scale = 0.3 * jnp.exp(jnp.log(3.0) * ramp)
    values = jax.random.truncated_normal(key, -2.5, 2.5, (TOKENS, H), jnp.float32)
    return values * scale[:, None]


def set_ends(array, stream_key, low, top_value):
    index_at = [jax.random.randint(jax.random.fold_in(stream_key, axis), (), 0, length) for axis, length in enumerate(array.shape)]
    widest = array.shape.index(max(array.shape))
    neighbour = index_at[:widest] + [(index_at[widest] + 1) % array.shape[widest]] + index_at[widest + 1:]
    return array.at[tuple(index_at)].set(low).at[tuple(neighbour)].set(top_value)


def block_levels(key, extent, shards, least, high):
    factor_of, own = 1.0, jax.random.fold_in(key, 6)
    for position, parts in shards:
        heights = jnp.exp(jax.random.uniform(jax.random.fold_in(own, position), (parts,), jnp.float32, least / len(shards), high / len(shards)))
        factor_of = factor_of * jnp.repeat(heights, extent[position] // parts).reshape([-1 if axis == position else 1 for axis in range(len(extent))])
    return factor_of


def cumulative_ranks(number_of, lean):
    portions = [(1 << 20) // math.isqrt(grade ** lean) + 1 for grade in range(1, number_of + 1)]
    width = 1 + sum(portions) // (1 << 30)
    return np.cumsum(np.array([max(1, weight // width) for weight in portions]))


def skewed_ids(rng, extent, count, skew):
    listing = cumulative_ranks(count, skew)
    lot = jax.random.randint(jax.random.fold_in(rng, 1), extent, 0, int(listing[count - 1]))
    grade = jnp.searchsorted(jnp.asarray(listing, jnp.int32), lot, side="right")
    return jax.random.permutation(jax.random.fold_in(rng, 2), count)[grade].astype(jnp.int32)


def scatter_about(stream_key, extent, scale, bound, pieces=(), held_as=jnp.bfloat16):
    gain = block_levels(stream_key, extent, pieces, -0.22, 0.18) if pieces else 1.0
    array = jax.random.normal(stream_key, extent, jnp.float32) * scale * gain
    return jnp.minimum(jnp.maximum(array, -bound), bound).astype(held_as)


def setup_inputs(seed: int = 0) -> dict:
    key_of = jax.random.split(jax.random.key(seed), 8)
    token_ids = set_ends(skewed_ids(key_of[0], (TOKENS,), V, 2), jax.random.fold_in(key_of[0], 3), 0, V - 1).astype(jnp.int32)
    input_table = scatter_about(key_of[1], (V, 3, H), 1.0, 6.0, ((2, 4),), jnp.float32)
    recur_weight = scatter_about(key_of[2], (H, 3, H), H ** -0.5, 0.125, ((2, 4),))
    z_bias = jnp.clip(-1.0 + 10.0 * jax.random.uniform(key_of[3], (H,), jnp.float32) ** block_levels(key_of[3], (H,), ((0, 4),), -0.2, 0.2), -1.0, 9.0)
    hn_bias = scatter_about(key_of[4], (H,), 1.0, 4.0, ((0, 4),), jnp.float32)
    init_state = jnp.clip(jax.random.uniform(key_of[5], (H,), jnp.float32, -0.9, 0.9) * block_levels(key_of[5], (H,), ((0, 4),), -0.4, 0.0), -0.9, 0.9)
    guess = draw_guess(jax.random.fold_in(key_of[7], 71), 0)
    return dict(token_ids=token_ids, input_table=input_table, recur_weight=recur_weight, z_bias=z_bias, hn_bias=hn_bias, init_state=init_state, guess=guess)


def cell(prev, inputs, products, z_bias, hn_bias, diag_z, diag_r, diag_n):
    zeta = jax.nn.sigmoid(inputs[:, 0] + products[:, 0] + z_bias)
    reset = jax.nn.sigmoid(inputs[:, 1] + products[:, 1])
    cand_pre = products[:, 2] + hn_bias
    cand = jnp.tanh(inputs[:, 2] + reset * cand_pre)
    value = (1.0 - zeta) * cand + zeta * prev
    slope = zeta + (prev - cand) * zeta * (1.0 - zeta) * diag_z
    slope = slope + (1.0 - zeta) * (1.0 - cand * cand) * (reset * diag_n + cand_pre * reset * (1.0 - reset) * diag_r)
    return (value, slope)

def reference(token_ids, input_table, recur_weight, z_bias, hn_bias, init_state, guess):
    weight_mat = recur_weight.reshape(H, 3 * H)
    diag_z = jnp.diagonal(recur_weight[:, 0, :]).astype(jnp.float32)
    diag_r = jnp.diagonal(recur_weight[:, 1, :]).astype(jnp.float32)
    diag_n = jnp.diagonal(recur_weight[:, 2, :]).astype(jnp.float32)
    blocks = TOKENS // TOK_DEV
    state = guess
    norms = []
    for step in range(ITERS):
        prev = jnp.concatenate([init_state[None], state[:-1]], 0)

        def evaluate(packed):
            ids, prev_block, state_block = packed
            inputs = input_table[ids]
            products = jnp.dot(prev_block.astype(jnp.bfloat16), weight_mat, preferred_element_type=jnp.float32)
            products = products.reshape(prev_block.shape[0], 3, H)
            value, slope = cell(prev_block, inputs, products, z_bias, hn_bias, diag_z, diag_r, diag_n)
            return (value - slope * prev_block, slope, jnp.sum((state_block - value) ** 2))
        offsets, slopes, squares = lax.map(evaluate, (token_ids.reshape(blocks, TOK_DEV), prev.reshape(blocks, TOK_DEV, H), state.reshape(blocks, TOK_DEV, H)))
        norms.append(jnp.sqrt(jnp.sum(squares) / (TOKENS * H)))

        def advance(carry, pair):
            carry = pair[0] * carry + pair[1]
            return (carry, carry)
        _, state = lax.scan(advance, init_state, (slopes.reshape(TOKENS, H), offsets.reshape(TOKENS, H)))
    return (state, jnp.stack(norms))
```

```python
import functools

import jax
import jax.numpy as jnp
from jax import lax
from jax.experimental import pallas as pl
from jax.experimental.pallas import tpu as pltpu
from jax.sharding import PartitionSpec as P

ITERS = 2
GROUP = 8
F32 = jnp.float32
BF16 = jnp.bfloat16


def swapped(block, axis, bit):
    route = [(i, i ^ bit) for i in range(lax.axis_size(axis))]
    return lax.ppermute(block, axis, route)


def shifted(block, axis, distance):
    devices = range(lax.axis_size(axis))
    route = [(i - distance, i) for i in devices if i - distance in devices]
    return lax.ppermute(block, axis, route)


def sigmoid(x):
    return 0.5 * jnp.tanh(0.5 * x) + 0.5


def vmem(count):
    return [pl.BlockSpec(memory_space=pltpu.VMEM)] * count


def params(mib):
    return pltpu.CompilerParams(vmem_limit_bytes=mib * 1024 * 1024)


def inputs_kernel(ids_ref, table_ref, bias_ref, out_ref):
    rows = ids_ref.shape[0]
    vocab = table_ref.shape[1]
    hot = (lax.broadcasted_iota(jnp.int32, (rows, vocab), 1) == ids_ref[...]).astype(F32).astype(BF16)
    for gate in range(3):
        table = table_ref[gate]
        if gate == 0:
            table = table + bias_ref[...]
        total = None
        for _ in range(3):
            part = table.astype(BF16)
            table = table - part.astype(F32)
            picked = jnp.dot(hot, part, preferred_element_type=F32)
            total = picked if total is None else total + picked
        out_ref[gate] = total


def diagonal_kernel(own_ref, out_ref):
    width = own_ref.shape[2]
    row = lax.broadcasted_iota(jnp.int32, (width, width), 0)
    col = lax.broadcasted_iota(jnp.int32, (width, width), 1)
    for gate in range(3):
        block = own_ref[gate].astype(F32)
        line = jnp.sum(jnp.where(row == col, block, 0.0), axis=0, keepdims=True)
        out_ref[pl.ds(gate * GROUP, GROUP), :] = jnp.broadcast_to(line, (GROUP, width))


def step_kernel(count, chunk, index_ref, *refs):
    blocks = refs[:count]
    weight_ref, inputs_ref, state_ref, edge_ref, bias_ref, diag_ref, a_ref, b_ref, ends_ref, prod_ref = refs[count:]
    rows, width = state_ref.shape
    hid = index_ref[0]
    for start in range(0, rows, chunk):
        for gate in range(3):
            total = None
            for offset in range(count):
                first = pl.multiple_of((hid ^ offset) * width, width)
                term = jnp.dot(
                    blocks[offset][pl.ds(start, chunk), :],
                    weight_ref[gate, pl.ds(first, width), :],
                    preferred_element_type=F32,
                )
                total = term if total is None else total + term
            prod_ref[gate, pl.ds(start, chunk), :] = total
    row = lax.broadcasted_iota(jnp.int32, (GROUP, width), 0)
    hn_bias = jnp.broadcast_to(bias_ref[...], (GROUP, width))
    diag_z = diag_ref[pl.ds(0, GROUP), :]
    diag_r = diag_ref[pl.ds(GROUP, GROUP), :]
    diag_n = diag_ref[pl.ds(2 * GROUP, GROUP), :]

    def advance(group, carry):
        before, run_a, run_b, squares = carry
        here = pl.ds(pl.multiple_of(group * GROUP, GROUP), GROUP)
        state = state_ref[here, :]
        turned = pltpu.roll(state, 1, 0)
        prev = jnp.where(row == 0, before, turned)
        zeta = sigmoid(inputs_ref[0, here, :] + prod_ref[0, here, :])
        reset = sigmoid(inputs_ref[1, here, :] + prod_ref[1, here, :])
        cand_pre = prod_ref[2, here, :] + hn_bias
        gated = reset * cand_pre
        cand = jnp.tanh(inputs_ref[2, here, :] + gated)
        rest = 1.0 - zeta
        gap = prev - cand
        value = cand + zeta * gap
        slope = zeta + gap * (zeta * rest) * diag_z
        slope = slope + rest * (1.0 - cand * cand) * (reset * diag_n + gated * (1.0 - reset) * diag_r)
        error = state - value
        squares = squares + error * error
        a = slope
        b = value - slope * prev
        for distance in (1, 2, 4):
            keep = row >= distance
            a_up = jnp.where(keep, pltpu.roll(a, distance, 0), 1.0)
            b_up = jnp.where(keep, pltpu.roll(b, distance, 0), 0.0)
            b = a * b_up + b
            a = a * a_up
        a_ref[here, :] = a * run_a
        b_ref[here, :] = a * run_b + b
        last_a = jnp.broadcast_to(a[GROUP - 1 :], (GROUP, width))
        last_b = jnp.broadcast_to(b[GROUP - 1 :], (GROUP, width))
        return (turned, last_a * run_a, last_a * run_b + last_b, squares)

    start = (
        jnp.broadcast_to(edge_ref[...], (GROUP, width)),
        jnp.ones((GROUP, width), F32),
        jnp.zeros((GROUP, width), F32),
        jnp.zeros((GROUP, width), F32),
    )
    _, run_a, run_b, squares = lax.fori_loop(0, rows // GROUP, advance, start, unroll=2)
    ends_ref[0:1, :] = run_a[0:1]
    ends_ref[1:2, :] = run_b[0:1]
    ends_ref[2:3, :] = jnp.sum(squares, axis=0, keepdims=True)


def apply_kernel(a_ref, b_ref, enter_ref, state_ref, *shifted_refs):
    rows, width = a_ref.shape
    row = lax.broadcasted_iota(jnp.int32, (2 * GROUP, width), 0)
    enter = jnp.broadcast_to(enter_ref[...], (2 * GROUP, width))

    def advance(group, before):
        here = pl.ds(pl.multiple_of(group * 2 * GROUP, 2 * GROUP), 2 * GROUP)
        state = a_ref[here, :] * enter + b_ref[here, :]
        state_ref[here, :] = state
        turned = pltpu.roll(state, 1, 0)
        if shifted_refs:
            shifted_refs[0][here, :] = jnp.where(row == 0, before, turned).astype(BF16)
        return turned

    lax.fori_loop(0, rows // (2 * GROUP), advance, enter, unroll=2)


def exchange(ends, axis):
    index = lax.axis_index(axis)
    before_a = jnp.ones_like(ends[0])
    before_b = jnp.zeros_like(ends[1])
    bit = 1
    while bit < lax.axis_size(axis):
        other = swapped(ends, axis, bit)
        upper = (index & bit) != 0
        before_b = jnp.where(upper, before_a * other[1] + before_b, before_b)
        before_a = jnp.where(upper, before_a * other[0], before_a)
        early = jnp.where(upper, other, ends)
        late = jnp.where(upper, ends, other)
        ends = jnp.stack([late[0] * early[0], late[0] * early[1] + late[1], late[2] + early[2]])
        bit *= 2
    return before_a, before_b, ends[2]


def gathered(block, axis):
    blocks = {0: block}
    bit = lax.axis_size(axis) // 2
    while bit:
        for offset in list(blocks):
            blocks[offset | bit] = swapped(blocks[offset], axis, bit)
        bit //= 2
    return [blocks[offset] for offset in range(len(blocks))]


def per_device(token_ids, input_table, recur_weight, z_bias, hn_bias, init_state, guess):
    rows, width = guess.shape
    full = recur_weight.shape[0]
    count = lax.axis_size("hid")
    hid = lax.axis_index("hid")
    is_first = lax.axis_index("tm") == 0
    weight = jnp.transpose(recur_weight, (1, 0, 2))
    table = jnp.transpose(input_table, (1, 0, 2))
    total = lax.axis_size("tm") * rows * count * width

    enter = shifted(guess[-1:], "tm", 1)
    enter = jnp.where(is_first, init_state[None], enter)
    moved = jnp.concatenate([enter, guess[:-1]], 0).astype(BF16)
    state = guess

    inputs = pl.pallas_call(
        inputs_kernel,
        out_shape=jax.ShapeDtypeStruct((3, rows, width), F32),
        in_specs=vmem(3),
        out_specs=vmem(1)[0],
        compiler_params=params(24),
        name="inputs",
    )(token_ids[:, None], table, z_bias[None])
    own = lax.dynamic_slice_in_dim(weight, hid * width, width, 1)
    diag = pl.pallas_call(
        diagonal_kernel,
        out_shape=jax.ShapeDtypeStruct((3 * GROUP, width), F32),
        in_specs=vmem(1),
        out_specs=vmem(1)[0],
        compiler_params=params(16),
        name="diagonal",
    )(own)

    chunk = min(rows, 256)
    flops = 2 * rows * full * 3 * width
    sums = []
    for step in range(ITERS):
        blocks = gathered(moved, "hid")
        a, b, ends = pl.pallas_call(
            functools.partial(step_kernel, count, chunk),
            out_shape=[
                jax.ShapeDtypeStruct((rows, width), F32),
                jax.ShapeDtypeStruct((rows, width), F32),
                jax.ShapeDtypeStruct((3, width), F32),
            ],
            in_specs=[pl.BlockSpec(memory_space=pltpu.SMEM)] + vmem(count + 6),
            out_specs=vmem(3),
            scratch_shapes=[pltpu.VMEM((3, rows, width), F32)],
            compiler_params=params(40),
            cost_estimate=pl.CostEstimate(flops=flops, bytes_accessed=4 * rows * width, transcendentals=0),
            name="step",
        )(hid[None], *blocks, weight, inputs, state, enter, hn_bias[None], diag)
        before_a, before_b, squares = exchange(ends, "tm")
        sums.append(squares)
        enter = (before_a * init_state + before_b)[None]
        last = step == ITERS - 1
        outs = [jax.ShapeDtypeStruct((rows, width), F32)]
        if not last:
            outs.append(jax.ShapeDtypeStruct((rows, width), BF16))
        result = pl.pallas_call(
            apply_kernel,
            out_shape=outs,
            in_specs=vmem(3),
            out_specs=vmem(len(outs)),
            compiler_params=params(16),
            name="apply",
        )(a, b, enter)
        state = result[0]
        if not last:
            moved = result[1]
    squares = jnp.stack(sums)
    bit = 1
    while bit < count:
        squares = squares + swapped(squares, "hid", bit)
        bit *= 2
    residual_norm = jnp.sqrt(jnp.sum(squares, axis=1) / total)
    return (state, residual_norm)


def solution(mesh):
    return jax.shard_map(
        per_device,
        mesh=mesh,
        in_specs=(
            P("tm"),
            P(None, None, "hid"),
            P(None, None, "hid"),
            P("hid"),
            P("hid"),
            P("hid"),
            P("tm", "hid"),
        ),
        out_specs=(P("tm", "hid"), P()),
        check_vma=False,
    )
```

```python
import functools

import jax
import jax.numpy as jnp
from jax import lax
from jax.experimental import pallas as pl
from jax.experimental.pallas import tpu as pltpu
from jax.sharding import PartitionSpec as P


ITERS = 2
CHUNKS = 2
GROUP = 8
EXTRA = 16
TILE = 256
F32 = jnp.float32
BF16 = jnp.bfloat16


def swapped(block, axis, bit):
    route = [(i, i ^ bit) for i in range(lax.axis_size(axis))]
    return lax.ppermute(block, axis, route)


def from_next(block, axis):
    route = [(i + 1, i) for i in range(lax.axis_size(axis) - 1)]
    return lax.ppermute(block, axis, route)


def sigmoid(x):
    return 0.5 * jnp.tanh(0.5 * x) + 0.5


def vmem(count):
    return [pl.BlockSpec(memory_space=pltpu.VMEM)] * count


def hbm(count):
    return [pl.BlockSpec(memory_space=pltpu.HBM)] * count


def smem():
    return [pl.BlockSpec(memory_space=pltpu.SMEM)]


def params(mib):
    return pltpu.CompilerParams(vmem_limit_bytes=mib * 1024 * 1024)


def cost(flops, moved):
    return pl.CostEstimate(flops=flops, bytes_accessed=moved, transcendentals=0)


def prepare_kernel(where_ref, ids_ref, table_ref, bias_ref, weight_ref, out_ref, diag_ref, own, held, sems):
    rows = ids_ref.shape[0]
    vocab = table_ref.shape[1]
    width = own.shape[2]
    first = pl.multiple_of(where_ref[0] * width, width)
    fetch = pltpu.make_async_copy(weight_ref.at[:, pl.ds(first, width), :], own, sems.at[0])
    fetch.start()
    hot = (lax.broadcasted_iota(jnp.int32, (rows, vocab), 1) == ids_ref[...]).astype(F32).astype(BF16)
    stores = []
    for gate in range(3):
        table = table_ref[gate]
        if gate == 0:
            table = table + bias_ref[...]
        total = None
        for _ in range(3):
            part = table.astype(BF16)
            table = table - part.astype(F32)
            picked = jnp.dot(hot, part, preferred_element_type=F32)
            total = picked if total is None else total + picked
        held[gate] = total
        stores.append(pltpu.make_async_copy(held.at[gate], out_ref.at[gate], sems.at[1 + gate]))
        stores[-1].start()
    fetch.wait()
    row = lax.broadcasted_iota(jnp.int32, (width, width), 0)
    col = lax.broadcasted_iota(jnp.int32, (width, width), 1)
    for gate in range(3):
        block = own[gate].astype(F32)
        line = jnp.sum(jnp.where(row == col, block, 0.0), axis=0, keepdims=True)
        diag_ref[pl.ds(gate * GROUP, GROUP), :] = jnp.broadcast_to(line, (GROUP, width))
    for store in stores:
        store.wait()


def gates(inputs, products, prev, hn_bias):
    zeta = sigmoid(inputs[0] + products[0])
    reset = sigmoid(inputs[1] + products[1])
    cand_pre = products[2] + hn_bias
    gated = reset * cand_pre
    cand = jnp.tanh(inputs[2] + gated)
    gap = prev - cand
    return zeta, reset, gated, cand, gap, cand + zeta * gap


def step_kernel(count, start, chunk, first, last, copies, where_ref, *refs):
    refs = list(refs)
    blocks = [refs.pop(0) for _ in range(count)]
    weight_ref, inputs_ref, state_ref, next_ref, bias_ref, diag_ref = [refs.pop(0) for _ in range(6)]
    before_ref = None if first == 1 else refs.pop(0)
    init_ref = refs.pop(0) if first == 1 else None
    a_ref, b_ref, ends_ref = [refs.pop(0) for _ in range(3)]
    send_ref = refs.pop(0) if last else None
    weights, inputs, lhs, products, sems = refs
    rows, width = state_ref.shape
    hid = where_ref[0]
    is_first = where_ref[1]
    is_last = where_ref[2]
    tiles = width // TILE
    groups = chunk // GROUP

    fetches = []
    for tile in range(tiles):
        lanes = pl.ds(tile * TILE, TILE)
        for gate in range(3):
            fetches.append(
                pltpu.make_async_copy(
                    weight_ref.at[gate, :, lanes], weights.at[gate, :, lanes], sems.at[tile * 4 + gate]
                )
            )
        fetches.append(
            pltpu.make_async_copy(
                inputs_ref.at[:, pl.ds(start, chunk), lanes], inputs.at[:, pl.ds(0, chunk), lanes], sems.at[tile * 4 + 3]
            )
        )
    if first == 1:
        fetches.append(
            pltpu.make_async_copy(
                inputs_ref.at[:, pl.ds(rows, GROUP), :], inputs.at[:, pl.ds(chunk, GROUP), :], sems.at[tiles * 4]
            )
        )
    for fetch in fetches:
        fetch.start()
    for offset in range(count):
        place = pl.multiple_of((hid ^ offset) * width, width)
        lhs[:, pl.ds(place, width)] = blocks[offset][...]
    row = lax.broadcasted_iota(jnp.int32, (GROUP, TILE), 0)
    if first == 1:
        fetches[-1].wait()

    for tile in range(tiles):
        lanes = pl.ds(tile * TILE, TILE)
        for gate in range(3):
            fetches[tile * 4 + gate].wait()
            products[gate] = jnp.dot(lhs[...], weights[gate, :, lanes], preferred_element_type=F32)
        fetches[tile * 4 + 3].wait()
        hn_bias = jnp.broadcast_to(bias_ref[:, lanes], (GROUP, TILE))
        diag_z = diag_ref[pl.ds(0, GROUP), lanes]
        diag_r = diag_ref[pl.ds(GROUP, GROUP), lanes]
        diag_n = diag_ref[pl.ds(2 * GROUP, GROUP), lanes]

        def advance(group, carry):
            turned, run_a, run_b, squares = carry
            here = pl.ds(pl.multiple_of(group * GROUP, GROUP), GROUP)
            prev = state_ref[pl.ds(pl.multiple_of(start + group * GROUP, GROUP), GROUP), lanes]
            if last:
                after = jnp.minimum(start + group * GROUP + GROUP, rows - GROUP)
                following = state_ref[pl.ds(pl.multiple_of(after, GROUP), GROUP), lanes]
                following = jnp.where(group == groups - 1, jnp.broadcast_to(next_ref[:, lanes], (GROUP, TILE)), following)
            else:
                following = state_ref[pl.ds(pl.multiple_of(start + group * GROUP + GROUP, GROUP), GROUP), lanes]
            turned_next = pltpu.roll(following, GROUP - 1, 0)
            state = jnp.where(row == GROUP - 1, turned_next, turned)
            zeta, reset, gated, cand, gap, value = gates(
                [inputs[gate, here, lanes] for gate in range(3)],
                [products[gate, here, :] for gate in range(3)],
                prev,
                hn_bias,
            )
            rest = 1.0 - zeta
            slope = zeta + gap * (zeta * rest) * diag_z
            slope = slope + rest * (1.0 - cand * cand) * (reset * diag_n + gated * (1.0 - reset) * diag_r)
            error = state - value
            if last:
                outside = (row == GROUP - 1) & (group == groups - 1) & (is_last == 1)
                error = jnp.where(outside, 0.0, error)
            squares = squares + error * error
            a = slope
            b = value - slope * prev
            for distance in (1, 2, 4):
                keep = row >= distance
                a_up = jnp.where(keep, pltpu.roll(a, distance, 0), 1.0)
                b_up = jnp.where(keep, pltpu.roll(b, distance, 0), 0.0)
                b = a * b_up + b
                a = a * a_up
            a_ref[here, lanes] = a * run_a
            b_ref[here, lanes] = a * run_b + b
            last_a = jnp.broadcast_to(a[GROUP - 1 :], (GROUP, TILE))
            last_b = jnp.broadcast_to(b[GROUP - 1 :], (GROUP, TILE))
            return (turned_next, last_a * run_a, last_a * run_b + last_b, squares)

        turned = pltpu.roll(state_ref[pl.ds(start, GROUP), lanes], GROUP - 1, 0)
        zeros = jnp.zeros((GROUP, TILE), F32)
        if first:
            carry = (turned, jnp.ones((GROUP, TILE), F32), zeros, zeros)
        else:
            carry = (
                turned,
                jnp.broadcast_to(before_ref[0:1, lanes], (GROUP, TILE)),
                jnp.broadcast_to(before_ref[1:2, lanes], (GROUP, TILE)),
                jnp.where(row == 0, before_ref[2:3, lanes], 0.0),
            )
        _, run_a, run_b, squares = lax.fori_loop(0, groups, advance, carry, unroll=4)
        if first == 1:
            begin = gates(
                [inputs[gate, pl.ds(chunk, GROUP), lanes] for gate in range(3)],
                [products[gate, pl.ds(chunk, GROUP), :] for gate in range(3)],
                jnp.broadcast_to(init_ref[:, lanes], (GROUP, TILE)),
                hn_bias,
            )[-1]
            error = state_ref[pl.ds(0, GROUP), lanes] - begin
            squares = squares + jnp.where((row == 0) & (is_first == 1), error * error, 0.0)
            begin = begin[0:1]
        else:
            begin = before_ref[3:4, lanes]
        total = jnp.sum(squares, axis=0, keepdims=True)
        ends_ref[0:1, lanes] = run_a[0:1]
        ends_ref[1:2, lanes] = run_b[0:1]
        ends_ref[2:3, lanes] = total
        ends_ref[3:4, lanes] = begin
        if last:
            fixed = run_a[0:1] * begin + run_b[0:1]
            send_a = jnp.where(is_first == 1, 0.0, run_a[0:1])
            send_b = jnp.where(is_first == 1, fixed, run_b[0:1])
            for peer in range(copies):
                send_ref[peer, 0:1, lanes] = send_a
                send_ref[peer, 1:2, lanes] = send_b
                send_ref[peer, 2:3, lanes] = total


def apply_kernel(chunks, final, where_ref, *refs):
    maps, refs = refs[: 2 * chunks], refs[2 * chunks :]
    begin_ref, all_ref, state_ref, sum_ref = refs[:4]
    outs = refs[4:]
    copies = all_ref.shape[0]
    chunk, width = maps[0].shape
    place = where_ref[3]

    def compose(peer, carry):
        enter, total = carry
        moved = all_ref[peer, 0:1, :] * enter + all_ref[peer, 1:2, :]
        return (jnp.where(peer < place, moved, enter), total + all_ref[peer, 2:3, :])

    enter, total = lax.fori_loop(0, copies, compose, (begin_ref[3:4, :], jnp.zeros((1, width), F32)), unroll=min(copies, 8))
    sum_ref[...] = total
    step = 2 * GROUP
    row = lax.broadcasted_iota(jnp.int32, (step, width), 0)
    enter = jnp.broadcast_to(enter, (step, width))
    before = enter
    for index in range(chunks):
        a_ref, b_ref = maps[2 * index], maps[2 * index + 1]

        def advance(group, before):
            here = pl.ds(pl.multiple_of(group * step, step), step)
            turned = pltpu.roll(a_ref[here, :] * enter + b_ref[here, :], 1, 0)
            moved = jnp.where(row == 0, before, turned)
            state_ref[pl.ds(pl.multiple_of(index * chunk + group * step, step), step), :] = moved
            if not final:
                outs[1 + index][here, :] = moved.astype(BF16)
            return turned

        before = lax.fori_loop(0, chunk // step, advance, before, unroll=2)
    if not final:
        outs[0][...] = before[0:1]


def newton(token_ids, input_table, recur_weight, z_bias, hn_bias, init_state, guess):
    rows, width = guess.shape
    full = recur_weight.shape[0]
    count = lax.axis_size("hid")
    blocks_tm = lax.axis_size("tm")
    hid = lax.axis_index("hid")
    tm = lax.axis_index("tm")
    weight = jnp.transpose(recur_weight, (1, 0, 2))
    table = jnp.transpose(input_table, (1, 0, 2))
    chunk = rows // CHUNKS
    where = jnp.stack([hid, (tm == 0).astype(jnp.int32), (tm == blocks_tm - 1).astype(jnp.int32), tm])

    state = guess
    moved = [guess[index * chunk : (index + 1) * chunk].astype(BF16) for index in range(CHUNKS)]
    moved[0] = jnp.concatenate([moved[0], init_state.astype(BF16)[None], jnp.zeros((EXTRA - 1, width), BF16)], 0)

    def gather(block):
        found = {0: block}
        bit = count // 2
        while bit:
            for offset in list(found):
                found[offset | bit] = swapped(found[offset], "hid", bit)
            bit //= 2
        return [found[offset] for offset in range(count)]

    following = from_next(guess[:1], "tm")
    next_id = from_next(token_ids[:1], "tm")
    ids = jnp.concatenate([token_ids[1:], next_id, token_ids[:1], jnp.zeros((GROUP - 1,), jnp.int32)])
    inputs, diag = pl.pallas_call(
        prepare_kernel,
        out_shape=[jax.ShapeDtypeStruct((3, rows + GROUP, width), F32), jax.ShapeDtypeStruct((3 * GROUP, width), F32)],
        in_specs=smem() + vmem(3) + hbm(1),
        out_specs=hbm(1) + vmem(1),
        scratch_shapes=[
            pltpu.VMEM((3, width, width), BF16),
            pltpu.VMEM((3, rows + GROUP, width), F32),
            pltpu.SemaphoreType.DMA((4,)),
        ],
        compiler_params=params(40),
        cost_estimate=cost(18 * rows * table.shape[1] * width, 8 * rows * width),
        name="prepare",
    )(where, ids[:, None], table, z_bias[None], weight)

    sums = []
    for step in range(ITERS):
        gathered = [gather(block) for block in moved]
        maps = []
        ends = begin if step else None
        for index in range(CHUNKS):
            first = 0 if index else (2 if step else 1)
            last = index == CHUNKS - 1
            height = gathered[index][0].shape[0]
            operands = [where, *gathered[index], weight, inputs, state, following, hn_bias[None], diag]
            specs = smem() + vmem(count) + hbm(2) + vmem(4)
            if first != 1:
                operands.append(ends)
                specs += vmem(1)
            else:
                operands.append(init_state[None])
                specs += vmem(1)
            outs = [
                jax.ShapeDtypeStruct((chunk, width), F32),
                jax.ShapeDtypeStruct((chunk, width), F32),
                jax.ShapeDtypeStruct((4, width), F32),
            ]
            if last:
                outs.append(jax.ShapeDtypeStruct((blocks_tm, 3, width), F32))
            found = pl.pallas_call(
                functools.partial(step_kernel, count, index * chunk, chunk, first, last, blocks_tm),
                out_shape=outs,
                in_specs=specs,
                out_specs=vmem(len(outs)),
                scratch_shapes=[
                    pltpu.VMEM((3, full, width), BF16),
                    pltpu.VMEM((3, chunk + GROUP, width), F32),
                    pltpu.VMEM((height, full), BF16),
                    pltpu.VMEM((3, height, TILE), F32),
                    pltpu.SemaphoreType.DMA((width // TILE * 4 + 1,)),
                ],
                compiler_params=params(32),
                cost_estimate=cost(2 * height * full * 3 * width, 6 * full * width),
            )(*operands)
            maps += found[:2]
            ends = found[2]
        begin = ends
        every = lax.all_to_all(found[3], "tm", 0, 0)
        final = step == ITERS - 1
        outs = [jax.ShapeDtypeStruct((rows, width), F32), jax.ShapeDtypeStruct((1, width), F32)]
        if not final:
            outs.append(jax.ShapeDtypeStruct((1, width), F32))
            outs += [jax.ShapeDtypeStruct((chunk, width), BF16)] * CHUNKS
        result = pl.pallas_call(
            functools.partial(apply_kernel, CHUNKS, final),
            out_shape=outs,
            in_specs=smem() + vmem(2 * CHUNKS + 2),
            out_specs=vmem(len(outs)),
            compiler_params=params(16),
        )(where, *maps, begin, every)
        state = result[0]
        sums.append(result[1])
        if not final:
            following = result[2]
            moved = list(result[3:])
    squares = jnp.concatenate(sums, 0)
    bit = 1
    while bit < count:
        squares = squares + swapped(squares, "hid", bit)
        bit *= 2
    size = blocks_tm * rows * count * width
    residual_norm = jnp.sqrt(jnp.sum(squares, axis=1) / size)
    return (state, residual_norm)


def solution(mesh):
    return jax.shard_map(
        newton,
        mesh=mesh,
        in_specs=(
            P("tm"),
            P(None, None, "hid"),
            P(None, None, "hid"),
            P("hid"),
            P("hid"),
            P("hid"),
            P("tm", "hid"),
        ),
        out_specs=(P("tm", "hid"), P()),
        check_vma=False,
    )
```

```python
import functools

import jax
import jax.numpy as jnp
from jax import lax
from jax.experimental import pallas as pl
from jax.experimental.pallas import tpu as pltpu
from jax.sharding import PartitionSpec as P


ITERS = 2
CHUNKS = 2
GROUP = 8
EXTRA = 16
TILE = 256
LANES = 128
F32 = jnp.float32
BF16 = jnp.bfloat16


def swapped(block, axis, bit):
    route = [(i, i ^ bit) for i in range(lax.axis_size(axis))]
    return lax.ppermute(block, axis, route)


def from_next(block, axis):
    route = [(i + 1, i) for i in range(lax.axis_size(axis) - 1)]
    return lax.ppermute(block, axis, route)


def sigmoid(x):
    return 0.5 * jnp.tanh(0.5 * x) + 0.5


def vmem(count):
    return [pl.BlockSpec(memory_space=pltpu.VMEM)] * count


def smem():
    return [pl.BlockSpec(memory_space=pltpu.SMEM)]


def params(mib):
    return pltpu.CompilerParams(vmem_limit_bytes=mib * 1024 * 1024)


def cost(flops, moved):
    return pl.CostEstimate(flops=flops, bytes_accessed=moved, transcendentals=0)


def round_kernel(chunks, guess_ref, init_ref, whole_ref, *parts):
    rows, width = guess_ref.shape
    chunk = rows // chunks
    row = lax.broadcasted_iota(jnp.int32, (EXTRA, width), 0)
    lead = jnp.where(row == 0, jnp.broadcast_to(init_ref[...], (EXTRA, width)), 0.0).astype(BF16)
    whole_ref[pl.ds(0, EXTRA), :] = lead
    parts[0][pl.ds(0, EXTRA), :] = lead
    for index, part in enumerate(parts):
        skip = 0 if index else EXTRA
        for start in range(0, chunk, GROUP * 4):
            block = guess_ref[pl.ds(index * chunk + start, GROUP * 4), :].astype(BF16)
            whole_ref[pl.ds(EXTRA + index * chunk + start, GROUP * 4), :] = block
            part[pl.ds(skip + start, GROUP * 4), :] = block


def prepare_kernel(where_ref, ids_ref, next_ref, table_ref, bias_ref, out_ref):
    rows = ids_ref.shape[0]
    vocab, width = table_ref.shape[1:]
    token = lax.broadcasted_iota(jnp.int32, (rows, 1), 0)
    ids = jnp.where(token == rows - GROUP - 1, jnp.broadcast_to(next_ref[:, width : width + 1], (rows, 1)), ids_ref[...])
    entry = lax.broadcasted_iota(jnp.int32, (rows, vocab), 1).astype(F32)
    hot = (entry == ids).astype(F32).astype(BF16)
    for gate in range(3):
        table = table_ref[gate]
        if gate == 0:
            table = table + bias_ref[...]
        total = None
        for _ in range(3):
            part = table.astype(BF16)
            table = table - part.astype(F32)
            picked = jnp.dot(hot, part, preferred_element_type=F32)
            total = picked if total is None else total + picked
        out_ref[gate] = total


def diagonals(weight_ref, hid, diag_ref):
    width = diag_ref.shape[1]
    row = lax.broadcasted_iota(jnp.int32, (width, width), 0)
    col = lax.broadcasted_iota(jnp.int32, (width, width), 1)
    first = pl.multiple_of(hid * width, width)
    for gate in range(3):
        block = weight_ref[gate, pl.ds(first, width), :].astype(F32)
        line = jnp.sum(jnp.where(row == col, block, 0.0), axis=0, keepdims=True)
        diag_ref[pl.ds(gate * GROUP, GROUP), :] = jnp.broadcast_to(line, (GROUP, width))


def gates(inputs, products, prev, hn_bias):
    zeta = sigmoid(inputs[0] + products[0])
    reset = sigmoid(inputs[1] + products[1])
    cand_pre = products[2] + hn_bias
    gated = reset * cand_pre
    cand = jnp.tanh(inputs[2] + gated)
    gap = prev - cand
    return zeta, reset, gated, cand, gap, cand + zeta * gap


def step_kernel(count, index, chunks, step, copies, where_ref, *refs):
    refs = list(refs)
    near = [refs.pop(0) for _ in range(count // 2)]
    far = [refs.pop(0) for _ in range(count // 2)]
    weight_ref, inputs_ref, state_ref, next_ref, bias_ref, before_ref = [refs.pop(0) for _ in range(6)]
    begins = index == 0 and step == 0
    diag_ref = None if begins else refs.pop(0)
    a_ref, b_ref, ends_ref = [refs.pop(0) for _ in range(3)]
    diag_ref = refs.pop(0) if begins else diag_ref
    last = index == chunks - 1
    send_ref = refs.pop(0) if last else None
    lhs, products = refs
    height = lhs.shape[0]
    rows, width = state_ref.shape
    chunk = rows // chunks
    start = index * chunk
    lead = height - chunk
    skip = EXTRA if step == 0 else 0
    hid = where_ref[0]
    is_first = where_ref[1]
    is_last = where_ref[2]
    groups = chunk // GROUP

    if begins:
        diagonals(weight_ref, hid, diag_ref)
    for offset in range(count):
        place = pl.multiple_of((hid ^ offset) * width, width)
        if offset < count // 2:
            lhs[:, pl.ds(place, width)] = near[offset][pl.ds(skip + start - lead, height), :]
        else:
            lhs[:, pl.ds(place, width)] = far[offset - count // 2][...]
    row = lax.broadcasted_iota(jnp.int32, (GROUP, TILE), 0)

    for tile in range(width // TILE):
        lanes = pl.ds(tile * TILE, TILE)
        for gate in range(3):
            products[gate] = jnp.dot(lhs[...], weight_ref[gate, :, lanes], preferred_element_type=F32)
        hn_bias = jnp.broadcast_to(bias_ref[:, lanes], (GROUP, TILE))
        diag_z = diag_ref[pl.ds(0, GROUP), lanes]
        diag_r = diag_ref[pl.ds(GROUP, GROUP), lanes]
        diag_n = diag_ref[pl.ds(2 * GROUP, GROUP), lanes]

        def advance(group, carry):
            turned, run_a, run_b, squares = carry
            here = pl.ds(pl.multiple_of(group * GROUP, GROUP), GROUP)
            token = pl.ds(pl.multiple_of(start + group * GROUP, GROUP), GROUP)
            prev = state_ref[token, lanes]
            after = start + group * GROUP + GROUP
            if last:
                after = jnp.minimum(after, rows - GROUP)
            following = state_ref[pl.ds(pl.multiple_of(after, GROUP), GROUP), lanes]
            if last:
                following = jnp.where(group == groups - 1, jnp.broadcast_to(next_ref[:, lanes], (GROUP, TILE)), following)
            turned_next = pltpu.roll(following, GROUP - 1, 0)
            state = jnp.where(row == GROUP - 1, turned_next, turned)
            product = pl.ds(pl.multiple_of(lead + group * GROUP, GROUP), GROUP)
            zeta, reset, gated, cand, gap, value = gates(
                [inputs_ref[gate, token, lanes] for gate in range(3)],
                [products[gate, product, :] for gate in range(3)],
                prev,
                hn_bias,
            )
            rest = 1.0 - zeta
            slope = zeta + gap * (zeta * rest) * diag_z
            slope = slope + rest * (1.0 - cand * cand) * (reset * diag_n + gated * (1.0 - reset) * diag_r)
            error = state - value
            if last:
                outside = (row == GROUP - 1) & (group == groups - 1) & (is_last == 1)
                error = jnp.where(outside, 0.0, error)
            squares = squares + error * error
            a = slope
            b = value - slope * prev
            for distance in (1, 2, 4):
                keep = row >= distance
                a_up = jnp.where(keep, pltpu.roll(a, distance, 0), 1.0)
                b_up = jnp.where(keep, pltpu.roll(b, distance, 0), 0.0)
                b = a * b_up + b
                a = a * a_up
            a_ref[here, lanes] = a * run_a
            b_ref[here, lanes] = a * run_b + b
            last_a = jnp.broadcast_to(a[GROUP - 1 :], (GROUP, TILE))
            last_b = jnp.broadcast_to(b[GROUP - 1 :], (GROUP, TILE))
            return (turned_next, last_a * run_a, last_a * run_b + last_b, squares)

        turned = pltpu.roll(state_ref[pl.ds(start, GROUP), lanes], GROUP - 1, 0)
        zeros = jnp.zeros((GROUP, TILE), F32)
        if index == 0:
            carry = (turned, jnp.ones((GROUP, TILE), F32), zeros, zeros)
        else:
            carry = (
                turned,
                jnp.broadcast_to(before_ref[0:1, lanes], (GROUP, TILE)),
                jnp.broadcast_to(before_ref[1:2, lanes], (GROUP, TILE)),
                jnp.where(row == 0, before_ref[2:3, lanes], 0.0),
            )
        _, run_a, run_b, squares = lax.fori_loop(0, groups, advance, carry, unroll=4)
        if begins:
            begin = gates(
                [inputs_ref[gate, pl.ds(rows, GROUP), lanes] for gate in range(3)],
                [products[gate, pl.ds(0, GROUP), :] for gate in range(3)],
                jnp.broadcast_to(before_ref[:, lanes], (GROUP, TILE)),
                hn_bias,
            )[-1]
            error = state_ref[pl.ds(0, GROUP), lanes] - begin
            squares = squares + jnp.where((row == 0) & (is_first == 1), error * error, 0.0)
            begin = begin[0:1]
            earlier = zeros[0:1]
        else:
            begin = before_ref[3:4, lanes]
            earlier = before_ref[2:3, lanes] if index == 0 else before_ref[4:5, lanes]
        total = jnp.sum(squares, axis=0, keepdims=True)
        ends_ref[0:1, lanes] = run_a[0:1]
        ends_ref[1:2, lanes] = run_b[0:1]
        ends_ref[2:3, lanes] = total
        ends_ref[3:4, lanes] = begin
        ends_ref[4:5, lanes] = earlier
        if last:
            send_a = jnp.where(is_first == 1, 0.0, run_a[0:1])
            send_b = jnp.where(is_first == 1, run_a[0:1] * begin + run_b[0:1], run_b[0:1])
            for part in range(TILE // LANES):
                at = tile * (TILE // LANES) + part
                for line, sent in ((at, send_a), (width // LANES + at, send_b)):
                    picked = sent[:, part * LANES : (part + 1) * LANES]
                    send_ref[:, pl.ds(line, 1), :] = jnp.broadcast_to(picked[None], (copies, 1, LANES))
    if last and step == ITERS - 1:
        lane = lax.broadcasted_iota(jnp.int32, (1, LANES), 1)
        sums = jnp.zeros((1, LANES), F32)
        for line, half in ((4, 0), (2, 1)):
            part = sum(ends_ref[pl.ds(line, 1), pl.ds(at, LANES)] for at in range(0, width, LANES))
            part = part + pltpu.roll(part, LANES // 2, 1)
            sums = jnp.where(lane // (LANES // 2) == half, part, sums)
        send_ref[:, pl.ds(2 * width // LANES, 1), :] = jnp.broadcast_to(sums[None], (copies, 1, LANES))


def apply_kernel(chunks, final, count, where_ref, *refs):
    maps, refs = refs[: 2 * chunks], refs[2 * chunks :]
    begin_ref, all_ref, state_ref = refs[:3]
    outs = refs[3:]
    chunk, width = maps[0].shape
    lines = width // LANES
    place = where_ref[3]
    hid = where_ref[0]
    copies = all_ref.shape[0]
    peers = copies // count if final else copies

    def compose(peer, enter):
        slot = peer * count + hid if final else peer
        moved = all_ref[slot, pl.ds(0, lines), :] * enter + all_ref[slot, pl.ds(lines, lines), :]
        return jnp.where(peer < place, moved, enter)

    begin = jnp.concatenate([begin_ref[3:4, pl.ds(at * LANES, LANES)] for at in range(lines)], axis=0)
    found = lax.fori_loop(0, peers, compose, begin, unroll=min(peers, 8))
    enter = jnp.concatenate([found[at : at + 1] for at in range(lines)], axis=1)
    if final:
        total = jnp.sum(all_ref[:, pl.ds(2 * lines, 1), :], axis=0)
        lane = lax.broadcasted_iota(jnp.int32, (1, LANES), 1)
        size = copies * chunk * chunks * width
        for half in range(2):
            outs[0][half] = jnp.sqrt(jnp.sum(jnp.where(lane // (LANES // 2) == half, total, 0.0)) / size)
    step = 2 * GROUP
    row = lax.broadcasted_iota(jnp.int32, (step, width), 0)
    enter = jnp.broadcast_to(enter, (step, width))
    before = enter
    for index in range(chunks):
        a_ref, b_ref = maps[2 * index], maps[2 * index + 1]

        def advance(group, before):
            here = pl.ds(pl.multiple_of(group * step, step), step)
            token = pl.ds(pl.multiple_of(index * chunk + group * step, step), step)
            turned = pltpu.roll(a_ref[here, :] * enter + b_ref[here, :], 1, 0)
            moved = jnp.where(row == 0, before, turned)
            state_ref[token, :] = moved
            if not final:
                rounded = moved.astype(BF16)
                outs[1][token, :] = rounded
                outs[2 + index][here, :] = rounded
            return turned

        before = lax.fori_loop(0, chunk // step, advance, before, unroll=2)
    if not final:
        outs[0][...] = before[0:1]


def newton(token_ids, input_table, recur_weight, z_bias, hn_bias, init_state, guess):
    rows, width = guess.shape
    full = recur_weight.shape[0]
    count = lax.axis_size("hid")
    blocks_tm = lax.axis_size("tm")
    hid = lax.axis_index("hid")
    tm = lax.axis_index("tm")
    weight = jnp.transpose(recur_weight, (1, 0, 2))
    table = jnp.transpose(input_table, (1, 0, 2))
    chunk = rows // CHUNKS
    lines = width // LANES
    where = jnp.stack([hid, (tm == 0).astype(jnp.int32), (tm == blocks_tm - 1).astype(jnp.int32), tm])

    state = guess
    whole, *moved = pl.pallas_call(
        functools.partial(round_kernel, CHUNKS),
        out_shape=[jax.ShapeDtypeStruct((rows + EXTRA, width), BF16)]
        + [jax.ShapeDtypeStruct((chunk + (0 if index else EXTRA), width), BF16) for index in range(CHUNKS)],
        in_specs=vmem(2),
        out_specs=vmem(1 + CHUNKS),
        compiler_params=params(16),
        cost_estimate=cost(rows * width, 8 * rows * width),
        name="round",
    )(guess, init_state[None])

    ids = token_ids.astype(F32)
    lead = jnp.concatenate([guess[:1], jnp.broadcast_to(ids[:1, None], (1, LANES))], 1)
    following = from_next(lead, "tm")
    ids = jnp.concatenate([ids[1:], ids[:1], ids[:1], jnp.zeros((GROUP - 1,), F32)])
    inputs = pl.pallas_call(
        prepare_kernel,
        out_shape=jax.ShapeDtypeStruct((3, rows + GROUP, width), F32),
        in_specs=smem() + vmem(4),
        out_specs=vmem(1)[0],
        compiler_params=params(32),
        cost_estimate=cost(18 * rows * table.shape[1] * width, 8 * rows * width),
        name="prepare",
    )(where, ids[:, None], following, table, z_bias[None])

    ends = init_state[None]
    diag = None
    for step in range(ITERS):
        final = step == ITERS - 1
        near = {0: whole}
        far = [{count // 2: None} for _ in range(CHUNKS)]
        for index in range(CHUNKS):
            far[index][count // 2] = swapped(moved[index], "hid", count // 2)
        bit = count // 4
        while bit:
            for offset in list(near):
                near[offset | bit] = swapped(near[offset], "hid", bit)
            for index in range(CHUNKS):
                for offset in list(far[index]):
                    far[index][offset | bit] = swapped(far[index][offset], "hid", bit)
            bit //= 2
        maps = []
        for index in range(CHUNKS):
            last = index == CHUNKS - 1
            height = moved[index].shape[0]
            operands = [near[offset] for offset in range(count // 2)]
            operands += [far[index][offset] for offset in range(count // 2, count)]
            operands += [weight, inputs, state, following, hn_bias[None], ends]
            if diag is not None:
                operands.append(diag)
            outs = [
                jax.ShapeDtypeStruct((chunk, width), F32),
                jax.ShapeDtypeStruct((chunk, width), F32),
                jax.ShapeDtypeStruct((5, width), F32),
            ]
            if diag is None:
                outs.append(jax.ShapeDtypeStruct((3 * GROUP, width), F32))
            copies = blocks_tm * count if final else blocks_tm
            if last:
                outs.append(jax.ShapeDtypeStruct((copies, 2 * lines + final, LANES), F32))
            found = pl.pallas_call(
                functools.partial(step_kernel, count, index, CHUNKS, step, copies),
                out_shape=outs,
                in_specs=smem() + vmem(len(operands)),
                out_specs=vmem(len(outs)),
                scratch_shapes=[pltpu.VMEM((height, full), BF16), pltpu.VMEM((3, height, TILE), F32)],
                compiler_params=params(32),
                cost_estimate=cost(2 * height * full * 3 * width, 6 * full * width),
            )(where, *operands)
            maps += found[:2]
            ends = found[2]
            diag = found[3] if diag is None else diag
        every = lax.all_to_all(found[-1], ("tm", "hid") if final else "tm", 0, 0)
        outs = [jax.ShapeDtypeStruct((rows, width), F32)]
        if final:
            outs.append(jax.ShapeDtypeStruct((ITERS,), F32))
            specs = vmem(1) + smem()
        else:
            outs.append(jax.ShapeDtypeStruct((1, width), F32))
            outs.append(jax.ShapeDtypeStruct((rows, width), BF16))
            outs += [jax.ShapeDtypeStruct((chunk, width), BF16)] * CHUNKS
            specs = vmem(len(outs))
        result = pl.pallas_call(
            functools.partial(apply_kernel, CHUNKS, final, count),
            out_shape=outs,
            in_specs=smem() + vmem(2 * CHUNKS + 2),
            out_specs=specs,
            compiler_params=params(16),
            cost_estimate=cost(2 * rows * width, 16 * rows * width),
        )(where, *maps, ends, every)
        if final:
            return (result[0], result[1])
        state, following, whole, *moved = result


def solution(mesh):
    return jax.shard_map(
        newton,
        mesh=mesh,
        in_specs=(
            P("tm"),
            P(None, None, "hid"),
            P(None, None, "hid"),
            P("hid"),
            P("hid"),
            P("hid"),
            P("tm", "hid"),
        ),
        out_specs=(P("tm", "hid"), P()),
        check_vma=False,
    )
```

```python
import functools

import jax
import jax.numpy as jnp
from jax import lax
from jax.experimental import pallas as pl
from jax.experimental.pallas import tpu as pltpu
from jax.sharding import PartitionSpec as P


ITERS = 2
CHUNKS = 2
GROUP = 8
EXTRA = 16
TILE = 256
LANES = 128
F32 = jnp.float32
BF16 = jnp.bfloat16


def swapped(block, axis, bit):
    route = [(i, i ^ bit) for i in range(lax.axis_size(axis))]
    return lax.ppermute(block, axis, route)


def from_next(block, axis):
    route = [(i + 1, i) for i in range(lax.axis_size(axis) - 1)]
    return lax.ppermute(block, axis, route)


def sigmoid(x):
    return 0.5 * jnp.tanh(0.5 * x) + 0.5


def vmem(count):
    return [pl.BlockSpec(memory_space=pltpu.VMEM)] * count


def smem():
    return [pl.BlockSpec(memory_space=pltpu.SMEM)]


def params(mib):
    return pltpu.CompilerParams(vmem_limit_bytes=mib * 1024 * 1024)


def cost(flops, moved):
    return pl.CostEstimate(flops=flops, bytes_accessed=moved, transcendentals=0)


def round_kernel(chunks, ids_ref, guess_ref, init_ref, whole_ref, lead_ref, *parts):
    rows, width = guess_ref.shape
    chunk = rows // chunks
    row = lax.broadcasted_iota(jnp.int32, (EXTRA, width), 0)
    head = jnp.where(row == 0, jnp.broadcast_to(init_ref[...], (EXTRA, width)), 0.0).astype(BF16)
    whole_ref[pl.ds(0, EXTRA), :] = head
    parts[0][pl.ds(0, EXTRA), :] = head
    lead_ref[:, pl.ds(0, width)] = guess_ref[0:1, :]
    lead_ref[:, pl.ds(width, LANES)] = jnp.full((1, LANES), ids_ref[0], jnp.int32).astype(F32)
    for index, part in enumerate(parts):
        skip = 0 if index else EXTRA
        for start in range(0, chunk, GROUP * 4):
            block = guess_ref[pl.ds(index * chunk + start, GROUP * 4), :].astype(BF16)
            whole_ref[pl.ds(EXTRA + index * chunk + start, GROUP * 4), :] = block
            part[pl.ds(skip + start, GROUP * 4), :] = block


def prepare_kernel(ids_ref, next_ref, table_ref, bias_ref, out_ref):
    vocab, width = table_ref.shape[1:]
    rows = ids_ref.shape[1]
    ids = ids_ref[...].astype(F32)
    lane = lax.broadcasted_iota(jnp.int32, (1, rows), 1)
    following = jnp.broadcast_to(next_ref[:, width : width + 1], (1, rows))
    ids = jnp.where(lane == rows - 1, following, pltpu.roll(ids, rows - 1, 1))
    begin = jnp.broadcast_to(ids_ref[:, 0:1].astype(F32), (1, LANES))

    def spread(line):
        entry = lax.broadcasted_iota(jnp.int32, (vocab, line.shape[1]), 0).astype(F32)
        return (entry == line).astype(F32).astype(BF16)

    def pick(hot, part):
        return lax.dot_general(hot, part, (((0,), (0,)), ((), ())), preferred_element_type=F32)

    hot, hot_begin = spread(ids), spread(begin)
    for gate in range(3):
        table = table_ref[gate]
        if gate == 0:
            table = table + bias_ref[...]
        total = None
        for _ in range(3):
            part = table.astype(BF16)
            table = table - part.astype(F32)
            picked = (pick(hot, part), pick(hot_begin, part))
            total = picked if total is None else (total[0] + picked[0], total[1] + picked[1])
        out_ref[gate, pl.ds(0, rows), :] = total[0]
        out_ref[gate, pl.ds(rows, GROUP), :] = total[1][0:GROUP]


def diagonals(weight_ref, hid, diag_ref):
    width = diag_ref.shape[1]
    row = lax.broadcasted_iota(jnp.int32, (width, width), 0)
    col = lax.broadcasted_iota(jnp.int32, (width, width), 1)
    first = pl.multiple_of(hid * width, width)
    for gate in range(3):
        block = weight_ref[gate, pl.ds(first, width), :].astype(F32)
        line = jnp.sum(jnp.where(row == col, block, 0.0), axis=0, keepdims=True)
        diag_ref[pl.ds(gate * GROUP, GROUP), :] = jnp.broadcast_to(line, (GROUP, width))


def gates(inputs, products, prev, hn_bias):
    zeta = sigmoid(inputs[0] + products[0])
    reset = sigmoid(inputs[1] + products[1])
    cand_pre = products[2] + hn_bias
    gated = reset * cand_pre
    cand = jnp.tanh(inputs[2] + gated)
    gap = prev - cand
    return zeta, reset, gated, cand, gap, cand + zeta * gap


def step_kernel(count, index, chunks, step, copies, *refs):
    refs = list(refs)
    near = [refs.pop(0) for _ in range(count // 2)]
    far = [refs.pop(0) for _ in range(count // 2)]
    weight_ref, inputs_ref, state_ref, next_ref, bias_ref, before_ref = [refs.pop(0) for _ in range(6)]
    begins = index == 0 and step == 0
    diag_ref = None if begins else refs.pop(0)
    a_ref, b_ref, ends_ref = [refs.pop(0) for _ in range(3)]
    diag_ref = refs.pop(0) if begins else diag_ref
    last = index == chunks - 1
    send_ref = refs.pop(0) if last else None
    lhs, *products = refs
    height, full = lhs.shape
    rows, width = state_ref.shape
    chunk = rows // chunks
    start = index * chunk
    lead = height - chunk
    skip = EXTRA if step == 0 else 0
    hid = lax.axis_index("hid")
    is_first = lax.axis_index("tm") == 0
    is_last = lax.axis_index("tm") == lax.axis_size("tm") - 1
    groups = chunk // GROUP
    tiles = width // TILE

    if begins:
        diagonals(weight_ref, hid, diag_ref)
    for offset in range(count):
        place = pl.multiple_of((hid ^ offset) * width, width)
        if offset < count // 2:
            lhs[:, pl.ds(place, width)] = near[offset][pl.ds(skip + start - lead, height), :]
        else:
            lhs[:, pl.ds(place, width)] = far[offset - count // 2][...]
    row = lax.broadcasted_iota(jnp.int32, (GROUP, TILE), 0)
    zeros = jnp.zeros((GROUP, TILE), F32)

    def dots(tile):
        lanes = pl.ds(tile * TILE, TILE)
        half = full // 2
        for gate in range(2):
            products[tile][gate] = jnp.dot(lhs[...], weight_ref[gate, :, lanes], preferred_element_type=F32)
        left = jnp.dot(lhs[:, pl.ds(0, half)], weight_ref[2, pl.ds(0, half), lanes], preferred_element_type=F32)
        right = jnp.dot(lhs[:, pl.ds(half, half)], weight_ref[2, pl.ds(half, half), lanes], preferred_element_type=F32)
        products[tile][2] = left + right

    def cells(tile):
        lanes = pl.ds(tile * TILE, TILE)
        hn_bias = jnp.broadcast_to(bias_ref[:, lanes], (GROUP, TILE))
        diag_z = diag_ref[pl.ds(0, GROUP), lanes]
        diag_r = diag_ref[pl.ds(GROUP, GROUP), lanes]
        diag_n = diag_ref[pl.ds(2 * GROUP, GROUP), lanes]
        squares = zeros
        if index == 0:
            run_a, run_b = jnp.ones((GROUP, TILE), F32), zeros
        else:
            run_a = jnp.broadcast_to(before_ref[0:1, lanes], (GROUP, TILE))
            run_b = jnp.broadcast_to(before_ref[1:2, lanes], (GROUP, TILE))
        turned = pltpu.roll(state_ref[pl.ds(start, GROUP), lanes], GROUP - 1, 0)
        for group in range(groups):
            here = pl.ds(group * GROUP, GROUP)
            token = pl.ds(start + group * GROUP, GROUP)
            prev = state_ref[token, lanes]
            if last and group == groups - 1:
                following = jnp.broadcast_to(next_ref[:, lanes], (GROUP, TILE))
            else:
                following = state_ref[pl.ds(start + (group + 1) * GROUP, GROUP), lanes]
            turned_next = pltpu.roll(following, GROUP - 1, 0)
            state = jnp.where(row == GROUP - 1, turned_next, turned)
            turned = turned_next
            zeta, reset, gated, cand, gap, value = gates(
                [inputs_ref[gate, token, lanes] for gate in range(3)],
                [products[tile][gate, pl.ds(lead + group * GROUP, GROUP), :] for gate in range(3)],
                prev,
                hn_bias,
            )
            rest = 1.0 - zeta
            slope = zeta + gap * (zeta * rest) * diag_z
            slope = slope + rest * (1.0 - cand * cand) * (reset * diag_n + gated * (1.0 - reset) * diag_r)
            error = state - value
            if last and group == groups - 1:
                error = jnp.where((row == GROUP - 1) & is_last, 0.0, error)
            squares = squares + error * error
            a = slope
            b = value - slope * prev
            for distance in (1, 2, 4):
                keep = row >= distance
                a_up = jnp.where(keep, pltpu.roll(a, distance, 0), 1.0)
                b_up = jnp.where(keep, pltpu.roll(b, distance, 0), 0.0)
                b = a * b_up + b
                a = a * a_up
            a_ref[here, lanes] = a * run_a
            b_ref[here, lanes] = a * run_b + b
            last_a = jnp.broadcast_to(a[GROUP - 1 :], (GROUP, TILE))
            last_b = jnp.broadcast_to(b[GROUP - 1 :], (GROUP, TILE))
            run_a, run_b = last_a * run_a, last_a * run_b + last_b
        if begins:
            begin = gates(
                [inputs_ref[gate, pl.ds(rows, GROUP), lanes] for gate in range(3)],
                [products[tile][gate, pl.ds(0, GROUP), :] for gate in range(3)],
                jnp.broadcast_to(before_ref[:, lanes], (GROUP, TILE)),
                hn_bias,
            )[-1]
            error = state_ref[pl.ds(0, GROUP), lanes] - begin
            squares = squares + jnp.where((row == 0) & is_first, error * error, 0.0)
            begin = begin[0:1]
            earlier = zeros[0:1]
        else:
            begin = before_ref[3:4, lanes]
            earlier = before_ref[2:3, lanes] if index == 0 else before_ref[4:5, lanes]
        total = jnp.sum(squares, axis=0, keepdims=True)
        if index:
            total = total + before_ref[2:3, lanes]
        ends_ref[0:1, lanes] = run_a[0:1]
        ends_ref[1:2, lanes] = run_b[0:1]
        ends_ref[2:3, lanes] = total
        ends_ref[3:4, lanes] = begin
        ends_ref[4:5, lanes] = earlier
        if last:
            send_a = jnp.where(is_first, 0.0, run_a[0:1])
            send_b = jnp.where(is_first, run_a[0:1] * begin + run_b[0:1], run_b[0:1])
            for part in range(TILE // LANES):
                at = tile * (TILE // LANES) + part
                for line, sent in ((at, send_a), (width // LANES + at, send_b)):
                    picked = sent[:, part * LANES : (part + 1) * LANES]
                    send_ref[:, pl.ds(line, 1), :] = jnp.broadcast_to(picked[None], (copies, 1, LANES))

    dots(0)
    for tile in range(1, tiles):
        dots(tile)
        cells(tile - 1)
    cells(tiles - 1)
    if last and step == ITERS - 1:
        lane = lax.broadcasted_iota(jnp.int32, (1, LANES), 1)
        sums = jnp.zeros((1, LANES), F32)
        for line, half in ((4, 0), (2, 1)):
            part = sum(ends_ref[pl.ds(line, 1), pl.ds(at, LANES)] for at in range(0, width, LANES))
            part = part + pltpu.roll(part, LANES // 2, 1)
            sums = jnp.where(lane // (LANES // 2) == half, part, sums)
        send_ref[:, pl.ds(2 * width // LANES, 1), :] = jnp.broadcast_to(sums[None], (copies, 1, LANES))


def apply_kernel(chunks, final, count, *refs):
    maps, refs = refs[: 2 * chunks], refs[2 * chunks :]
    begin_ref, all_ref, state_ref = refs[:3]
    outs = refs[3:]
    chunk, width = maps[0].shape
    lines = width // LANES
    place = lax.axis_index("tm")
    hid = lax.axis_index("hid")
    copies = all_ref.shape[0]
    peers = copies // count if final else copies

    def compose(peer, enter):
        slot = peer * count + hid if final else peer
        moved = all_ref[slot, pl.ds(0, lines), :] * enter + all_ref[slot, pl.ds(lines, lines), :]
        return jnp.where(peer < place, moved, enter)

    begin = jnp.concatenate([begin_ref[3:4, pl.ds(at * LANES, LANES)] for at in range(lines)], axis=0)
    found = lax.fori_loop(0, peers, compose, begin, unroll=min(peers, 8))
    enter = jnp.concatenate([found[at : at + 1] for at in range(lines)], axis=1)
    if final:
        total = jnp.sum(all_ref[:, pl.ds(2 * lines, 1), :], axis=0)
        lane = lax.broadcasted_iota(jnp.int32, (1, LANES), 1)
        size = copies * chunk * chunks * width
        for half in range(2):
            outs[0][half] = jnp.sqrt(jnp.sum(jnp.where(lane // (LANES // 2) == half, total, 0.0)) / size)
    step = 2 * GROUP
    row = lax.broadcasted_iota(jnp.int32, (step, width), 0)
    enter = jnp.broadcast_to(enter, (step, width))
    before = enter
    for index in range(chunks):
        a_ref, b_ref = maps[2 * index], maps[2 * index + 1]

        def advance(group, before):
            here = pl.ds(pl.multiple_of(group * step, step), step)
            token = pl.ds(pl.multiple_of(index * chunk + group * step, step), step)
            turned = pltpu.roll(a_ref[here, :] * enter + b_ref[here, :], 1, 0)
            moved = jnp.where(row == 0, before, turned)
            state_ref[token, :] = moved
            if not final:
                rounded = moved.astype(BF16)
                outs[1][token, :] = rounded
                outs[2 + index][here, :] = rounded
            return turned

        before = lax.fori_loop(0, chunk // step, advance, before, unroll=2)
    if not final:
        outs[0][...] = before[0:1]


def newton(token_ids, input_table, recur_weight, z_bias, hn_bias, init_state, guess):
    rows, width = guess.shape
    full = recur_weight.shape[0]
    count = lax.axis_size("hid")
    blocks_tm = lax.axis_size("tm")
    weight = jnp.transpose(recur_weight, (1, 0, 2))
    table = jnp.transpose(input_table, (1, 0, 2))
    chunk = rows // CHUNKS
    lines = width // LANES

    state = guess
    whole, lead, *moved = pl.pallas_call(
        functools.partial(round_kernel, CHUNKS),
        out_shape=[jax.ShapeDtypeStruct((rows + EXTRA, width), BF16), jax.ShapeDtypeStruct((1, width + LANES), F32)]
        + [jax.ShapeDtypeStruct((chunk + (0 if index else EXTRA), width), BF16) for index in range(CHUNKS)],
        in_specs=smem() + vmem(2),
        out_specs=vmem(2 + CHUNKS),
        compiler_params=params(16),
        cost_estimate=cost(rows * width, 8 * rows * width),
        name="round",
    )(token_ids, guess, init_state[None])

    following = from_next(lead, "tm")
    inputs = pl.pallas_call(
        prepare_kernel,
        out_shape=jax.ShapeDtypeStruct((3, rows + GROUP, width), F32),
        in_specs=vmem(4),
        out_specs=vmem(1)[0],
        compiler_params=params(32),
        cost_estimate=cost(18 * rows * table.shape[1] * width, 8 * rows * width),
        name="prepare",
    )(token_ids[None], following, table, z_bias[None])

    ends = init_state[None]
    diag = None
    for step in range(ITERS):
        final = step == ITERS - 1
        near = {0: whole}
        far = [{count // 2: None} for _ in range(CHUNKS)]
        for index in range(CHUNKS):
            far[index][count // 2] = swapped(moved[index], "hid", count // 2)
        bit = count // 4
        while bit:
            for offset in list(near):
                near[offset | bit] = swapped(near[offset], "hid", bit)
            for index in range(CHUNKS):
                for offset in list(far[index]):
                    far[index][offset | bit] = swapped(far[index][offset], "hid", bit)
            bit //= 2
        maps = []
        for index in range(CHUNKS):
            last = index == CHUNKS - 1
            height = moved[index].shape[0]
            operands = [near[offset] for offset in range(count // 2)]
            operands += [far[index][offset] for offset in range(count // 2, count)]
            operands += [weight, inputs, state, following, hn_bias[None], ends]
            if diag is not None:
                operands.append(diag)
            outs = [
                jax.ShapeDtypeStruct((chunk, width), F32),
                jax.ShapeDtypeStruct((chunk, width), F32),
                jax.ShapeDtypeStruct((5, width), F32),
            ]
            if diag is None:
                outs.append(jax.ShapeDtypeStruct((3 * GROUP, width), F32))
            copies = blocks_tm * count if final else blocks_tm
            if last:
                outs.append(jax.ShapeDtypeStruct((copies, 2 * lines + final, LANES), F32))
            found = pl.pallas_call(
                functools.partial(step_kernel, count, index, CHUNKS, step, copies),
                out_shape=outs,
                in_specs=vmem(len(operands)),
                out_specs=vmem(len(outs)),
                scratch_shapes=[pltpu.VMEM((height, full), BF16)]
                + [pltpu.VMEM((3, height, TILE), F32)] * (width // TILE),
                compiler_params=params(32),
                cost_estimate=cost(2 * height * full * 3 * width, 6 * full * width),
            )(*operands)
            maps += found[:2]
            ends = found[2]
            diag = found[3] if diag is None else diag
        every = lax.all_to_all(found[-1], ("tm", "hid") if final else "tm", 0, 0)
        outs = [jax.ShapeDtypeStruct((rows, width), F32)]
        if final:
            outs.append(jax.ShapeDtypeStruct((ITERS,), F32))
            specs = vmem(1) + smem()
        else:
            outs.append(jax.ShapeDtypeStruct((1, width), F32))
            outs.append(jax.ShapeDtypeStruct((rows, width), BF16))
            outs += [jax.ShapeDtypeStruct((chunk, width), BF16)] * CHUNKS
            specs = vmem(len(outs))
        result = pl.pallas_call(
            functools.partial(apply_kernel, CHUNKS, final, count),
            out_shape=outs,
            in_specs=vmem(2 * CHUNKS + 2),
            out_specs=specs,
            compiler_params=params(16),
            cost_estimate=cost(2 * rows * width, 16 * rows * width),
        )(*maps, ends, every)
        if final:
            return (result[0], result[1])
        state, following, whole, *moved = result


def solution(mesh):
    return jax.shard_map(
        newton,
        mesh=mesh,
        in_specs=(
            P("tm"),
            P(None, None, "hid"),
            P(None, None, "hid"),
            P("hid"),
            P("hid"),
            P("hid"),
            P("tm", "hid"),
        ),
        out_specs=(P("tm", "hid"), P()),
        check_vma=False,
    )
```

```python
import functools

import jax
import jax.numpy as jnp
from jax import lax
from jax.experimental import pallas as pl
from jax.experimental.pallas import tpu as pltpu
from jax.sharding import PartitionSpec as P


ITERS = 2
CHUNKS = 2
GROUP = 8
EXTRA = 16
TILE = 256
LANES = 128
COVER = 32
F32 = jnp.float32
BF16 = jnp.bfloat16


def swapped(block, axis, bit):
    route = [(i, i ^ bit) for i in range(lax.axis_size(axis))]
    return lax.ppermute(block, axis, route)


def from_next(block, axis):
    route = [(i + 1, i) for i in range(lax.axis_size(axis) - 1)]
    return lax.ppermute(block, axis, route)


def sigmoid(x):
    return 0.5 * jnp.tanh(0.5 * x) + 0.5


def vmem(count):
    return [pl.BlockSpec(memory_space=pltpu.VMEM)] * count


def smem():
    return [pl.BlockSpec(memory_space=pltpu.SMEM)]


def params(mib):
    return pltpu.CompilerParams(vmem_limit_bytes=mib * 1024 * 1024)


def cost(flops, moved):
    return pl.CostEstimate(flops=flops, bytes_accessed=moved, transcendentals=0)


def merge_kernel(ids_ref, guess_ref, *refs):
    *parts, whole_ref, lead_ref = refs
    width = guess_ref.shape[1]
    at = 0
    for part in parts:
        whole_ref[pl.ds(at, part.shape[0]), :] = part[...]
        at += part.shape[0]
    lead_ref[:, pl.ds(width, LANES)] = jnp.broadcast_to(ids_ref[:, 0:1], (1, LANES)).astype(F32)
    lead_ref[:, pl.ds(0, width)] = guess_ref[0:1, :]


def prepare_kernel(ids_ref, next_ref, table_ref, bias_ref, out_ref):
    vocab, width = table_ref.shape[1:]
    rows = ids_ref.shape[1]
    ids = ids_ref[...].astype(F32)
    lane = lax.broadcasted_iota(jnp.int32, (1, rows), 1)
    following = jnp.broadcast_to(next_ref[:, width : width + 1], (1, rows))
    ids = jnp.where(lane == rows - 1, following, pltpu.roll(ids, rows - 1, 1))
    begin = jnp.broadcast_to(ids_ref[:, 0:1].astype(F32), (1, LANES))

    def spread(line):
        entry = lax.broadcasted_iota(jnp.int32, (vocab, line.shape[1]), 0).astype(F32)
        return (entry == line).astype(F32).astype(BF16)

    def pick(hot, part):
        return lax.dot_general(hot, part, (((0,), (0,)), ((), ())), preferred_element_type=F32)

    hot, hot_begin = spread(ids), spread(begin)
    for gate in range(3):
        table = table_ref[gate]
        if gate == 0:
            table = table + bias_ref[...]
        total = None
        for _ in range(3):
            part = table.astype(BF16)
            table = table - part.astype(F32)
            picked = (pick(hot, part), pick(hot_begin, part))
            total = picked if total is None else (total[0] + picked[0], total[1] + picked[1])
        out_ref[gate, pl.ds(0, rows), :] = total[0]
        out_ref[gate, pl.ds(rows, GROUP), :] = total[1][0:GROUP]


def diagonals(weight_ref, hid, diag_ref):
    width = diag_ref.shape[1]
    row = lax.broadcasted_iota(jnp.int32, (width, width), 0)
    col = lax.broadcasted_iota(jnp.int32, (width, width), 1)
    first = pl.multiple_of(hid * width, width)
    for gate in range(3):
        block = weight_ref[gate, pl.ds(first, width), :].astype(F32)
        line = jnp.sum(jnp.where(row == col, block, 0.0), axis=0, keepdims=True)
        diag_ref[pl.ds(gate * GROUP, GROUP), :] = jnp.broadcast_to(line, (GROUP, width))


def gates(inputs, products, prev, hn_bias):
    zeta = sigmoid(inputs[0] + products[0])
    reset = sigmoid(inputs[1] + products[1])
    cand_pre = products[2] + hn_bias
    gated = reset * cand_pre
    cand = jnp.tanh(inputs[2] + gated)
    gap = prev - cand
    return zeta, reset, gated, cand, gap, cand + zeta * gap


def step_kernel(count, index, chunks, step, copies, *refs):
    refs = list(refs)
    near = [refs.pop(0) for _ in range(count // 2)]
    far = [refs.pop(0) for _ in range(count // 2)]
    weight_ref, inputs_ref, state_ref, next_ref, bias_ref, init_ref = [refs.pop(0) for _ in range(6)]
    opens = index == 0 and step == 0
    before_ref = None if opens else refs.pop(0)
    diag_ref = None if opens else refs.pop(0)
    a_ref, b_ref, ends_ref = [refs.pop(0) for _ in range(3)]
    diag_ref = refs.pop(0) if opens else diag_ref
    last = index == chunks - 1
    begins = last and step == 0
    send_ref = refs.pop(0) if last else None
    lhs, *products = refs
    height, full = lhs.shape
    rows, width = state_ref.shape
    chunk = rows // chunks
    start = index * chunk
    lead = height - chunk
    hid = lax.axis_index("hid")
    is_first = lax.axis_index("tm") == 0
    is_last = lax.axis_index("tm") == lax.axis_size("tm") - 1
    groups = chunk // GROUP
    tiles = width // TILE

    if opens:
        diagonals(weight_ref, hid, diag_ref)
    for offset in range(count):
        place = pl.multiple_of((hid ^ offset) * width, width)
        if offset < count // 2:
            lhs[:, pl.ds(place, width)] = near[offset][pl.ds(start, height), :]
        else:
            lhs[:, pl.ds(place, width)] = far[offset - count // 2][...]
    row = lax.broadcasted_iota(jnp.int32, (GROUP, TILE), 0)
    zeros = jnp.zeros((GROUP, TILE), F32)

    def dots(tile):
        lanes = pl.ds(tile * TILE, TILE)
        half = full // 2
        for gate in range(2):
            products[tile][gate] = jnp.dot(lhs[...], weight_ref[gate, :, lanes], preferred_element_type=F32)
        left = jnp.dot(lhs[:, pl.ds(0, half)], weight_ref[2, pl.ds(0, half), lanes], preferred_element_type=F32)
        right = jnp.dot(lhs[:, pl.ds(half, half)], weight_ref[2, pl.ds(half, half), lanes], preferred_element_type=F32)
        products[tile][2] = left + right

    def cells(tile):
        lanes = pl.ds(tile * TILE, TILE)
        hn_bias = jnp.broadcast_to(bias_ref[:, lanes], (GROUP, TILE))
        diag_z = diag_ref[pl.ds(0, GROUP), lanes]
        diag_r = diag_ref[pl.ds(GROUP, GROUP), lanes]
        diag_n = diag_ref[pl.ds(2 * GROUP, GROUP), lanes]
        squares = zeros
        if index == 0:
            run_a, run_b = jnp.ones((GROUP, TILE), F32), zeros
        else:
            run_a = jnp.broadcast_to(before_ref[0:1, lanes], (GROUP, TILE))
            run_b = jnp.broadcast_to(before_ref[1:2, lanes], (GROUP, TILE))
        turned = pltpu.roll(state_ref[pl.ds(start, GROUP), lanes], GROUP - 1, 0)
        for group in range(groups):
            here = pl.ds(group * GROUP, GROUP)
            token = pl.ds(start + group * GROUP, GROUP)
            prev = state_ref[token, lanes]
            if last and group == groups - 1:
                following = jnp.broadcast_to(next_ref[:, lanes], (GROUP, TILE))
            else:
                following = state_ref[pl.ds(start + (group + 1) * GROUP, GROUP), lanes]
            turned_next = pltpu.roll(following, GROUP - 1, 0)
            state = jnp.where(row == GROUP - 1, turned_next, turned)
            turned = turned_next
            zeta, reset, gated, cand, gap, value = gates(
                [inputs_ref[gate, token, lanes] for gate in range(3)],
                [products[tile][gate, pl.ds(lead + group * GROUP, GROUP), :] for gate in range(3)],
                prev,
                hn_bias,
            )
            rest = 1.0 - zeta
            slope = zeta + gap * (zeta * rest) * diag_z
            slope = slope + rest * (1.0 - cand * cand) * (reset * diag_n + gated * (1.0 - reset) * diag_r)
            error = state - value
            if last and group == groups - 1:
                error = jnp.where((row == GROUP - 1) & is_last, 0.0, error)
            squares = squares + error * error
            a = slope
            b = value - slope * prev
            for distance in (1, 2, 4):
                keep = row >= distance
                a_up = jnp.where(keep, pltpu.roll(a, distance, 0), 1.0)
                b_up = jnp.where(keep, pltpu.roll(b, distance, 0), 0.0)
                b = a * b_up + b
                a = a * a_up
            a_ref[here, lanes] = a * run_a
            b_ref[here, lanes] = a * run_b + b
            last_a = jnp.broadcast_to(a[GROUP - 1 :], (GROUP, TILE))
            last_b = jnp.broadcast_to(b[GROUP - 1 :], (GROUP, TILE))
            run_a, run_b = last_a * run_a, last_a * run_b + last_b
        if begins:
            begin = gates(
                [inputs_ref[gate, pl.ds(rows, GROUP), lanes] for gate in range(3)],
                [products[tile][gate, pl.ds(0, GROUP), :] for gate in range(3)],
                jnp.broadcast_to(init_ref[:, lanes], (GROUP, TILE)),
                hn_bias,
            )[-1]
            error = state_ref[pl.ds(0, GROUP), lanes] - begin
            squares = squares + jnp.where((row == 0) & is_first, error * error, 0.0)
            begin = begin[0:1]
            earlier = zeros[0:1]
        elif step == 0:
            begin, earlier = zeros[0:1], zeros[0:1]
        else:
            begin = before_ref[3:4, lanes]
            earlier = before_ref[2:3, lanes] if index == 0 else before_ref[4:5, lanes]
        total = jnp.sum(squares, axis=0, keepdims=True)
        if index:
            total = total + before_ref[2:3, lanes]
        ends_ref[0:1, lanes] = run_a[0:1]
        ends_ref[1:2, lanes] = run_b[0:1]
        ends_ref[2:3, lanes] = total
        ends_ref[3:4, lanes] = begin
        ends_ref[4:5, lanes] = earlier
        if last:
            send_a = jnp.where(is_first, 0.0, run_a[0:1])
            send_b = jnp.where(is_first, run_a[0:1] * begin + run_b[0:1], run_b[0:1])
            for part in range(TILE // LANES):
                at = tile * (TILE // LANES) + part
                for line, sent in ((at, send_a), (width // LANES + at, send_b)):
                    picked = sent[:, part * LANES : (part + 1) * LANES]
                    send_ref[:, pl.ds(line, 1), :] = jnp.broadcast_to(picked[None], (copies, 1, LANES))

    dots(0)
    for tile in range(1, tiles):
        dots(tile)
        cells(tile - 1)
    cells(tiles - 1)
    if last and step == ITERS - 1:
        lane = lax.broadcasted_iota(jnp.int32, (1, LANES), 1)
        sums = jnp.zeros((1, LANES), F32)
        for line, half in ((4, 0), (2, 1)):
            part = sum(ends_ref[pl.ds(line, 1), pl.ds(at, LANES)] for at in range(0, width, LANES))
            part = part + pltpu.roll(part, LANES // 2, 1)
            sums = jnp.where(lane // (LANES // 2) == half, part, sums)
        send_ref[:, pl.ds(2 * width // LANES, 1), :] = jnp.broadcast_to(sums[None], (copies, 1, LANES))


def apply_kernel(chunks, final, count, *refs):
    maps, refs = refs[: 2 * chunks], refs[2 * chunks :]
    begin_ref, all_ref, state_ref = refs[:3]
    outs = refs[3:]
    chunk, width = maps[0].shape
    lines = width // LANES
    place = lax.axis_index("tm")
    hid = lax.axis_index("hid")
    copies = all_ref.shape[0]
    peers = copies // count if final else copies

    def compose(peer, enter):
        slot = peer * count + hid if final else peer
        moved = all_ref[slot, pl.ds(0, lines), :] * enter + all_ref[slot, pl.ds(lines, lines), :]
        return jnp.where(peer < place, moved, enter)

    begin = jnp.concatenate([begin_ref[3:4, pl.ds(at * LANES, LANES)] for at in range(lines)], axis=0)
    found = lax.fori_loop(0, peers, compose, begin, unroll=min(peers, 8))
    enter = jnp.concatenate([found[at : at + 1] for at in range(lines)], axis=1)
    if final:
        total = jnp.sum(all_ref[:, pl.ds(2 * lines, 1), :], axis=0)
        lane = lax.broadcasted_iota(jnp.int32, (1, LANES), 1)
        size = copies * chunk * chunks * width
        for half in range(2):
            outs[0][half] = jnp.sqrt(jnp.sum(jnp.where(lane // (LANES // 2) == half, total, 0.0)) / size)
    step = 2 * GROUP
    row = lax.broadcasted_iota(jnp.int32, (step, width), 0)
    enter = jnp.broadcast_to(enter, (step, width))
    before = enter
    for index in range(chunks):
        a_ref, b_ref = maps[2 * index], maps[2 * index + 1]

        def advance(group, before):
            here = pl.ds(pl.multiple_of(group * step, step), step)
            token = pl.ds(pl.multiple_of(index * chunk + group * step, step), step)
            turned = pltpu.roll(a_ref[here, :] * enter + b_ref[here, :], 1, 0)
            moved = jnp.where(row == 0, before, turned)
            state_ref[token, :] = moved
            if not final:
                rounded = moved.astype(BF16)
                outs[1][token, :] = rounded
                outs[2 + index][here, :] = rounded
            return turned

        before = lax.fori_loop(0, chunk // step, advance, before, unroll=2)
    if not final:
        outs[0][...] = before[0:1]


def newton(token_ids, input_table, recur_weight, z_bias, hn_bias, init_state, guess):
    rows, width = guess.shape
    full = recur_weight.shape[0]
    count = lax.axis_size("hid")
    blocks_tm = lax.axis_size("tm")
    weight = jnp.transpose(recur_weight, (1, 0, 2))
    table = jnp.transpose(input_table, (1, 0, 2))
    chunk = rows // CHUNKS
    lines = width // LANES

    state = guess
    moved, rest = [], guess
    for index in range(CHUNKS):
        part = rest[index * chunk : (index + 1) * chunk].astype(BF16)
        if index == CHUNKS - 1:
            head = jnp.concatenate([init_state.astype(BF16)[None], jnp.zeros((EXTRA - 1, width), BF16)], 0)
            part = jnp.concatenate([head, part], 0)
        part, rest = lax.optimization_barrier((part, rest))
        moved.append(part)
    whole, lead = pl.pallas_call(
        merge_kernel,
        out_shape=[jax.ShapeDtypeStruct((rows + EXTRA, width), BF16), jax.ShapeDtypeStruct((1, width + LANES), F32)],
        in_specs=vmem(2 + CHUNKS),
        out_specs=vmem(2),
        compiler_params=params(8),
        cost_estimate=cost(COVER * rows * width, COVER * rows * width),
        name="merge",
    )(token_ids[None], guess[:GROUP], *moved)
    following = from_next(lead, "tm")
    inputs = pl.pallas_call(
        prepare_kernel,
        out_shape=jax.ShapeDtypeStruct((3, rows + GROUP, width), F32),
        in_specs=vmem(4),
        out_specs=vmem(1)[0],
        compiler_params=params(32),
        cost_estimate=cost(72 * rows * table.shape[1] * width, COVER * rows * width),
        name="prepare",
    )(token_ids[None], following, table, z_bias[None])

    ends, diag = None, None
    for step in range(ITERS):
        final = step == ITERS - 1
        near = {0: whole}
        far = [{count // 2: None} for _ in range(CHUNKS)]
        for index in range(CHUNKS):
            far[index][count // 2] = swapped(moved[index], "hid", count // 2)
        bit = count // 4
        while bit:
            for offset in list(near):
                near[offset | bit] = swapped(near[offset], "hid", bit)
            for index in range(CHUNKS):
                for offset in list(far[index]):
                    far[index][offset | bit] = swapped(far[index][offset], "hid", bit)
            bit //= 2
        maps = []
        for index in range(CHUNKS):
            last = index == CHUNKS - 1
            height = moved[index].shape[0]
            operands = [near[offset] for offset in range(count // 2)]
            operands += [far[index][offset] for offset in range(count // 2, count)]
            operands += [weight, inputs, state, following, hn_bias[None], init_state[None]]
            if diag is not None:
                operands += [ends, diag]
            outs = [
                jax.ShapeDtypeStruct((chunk, width), F32),
                jax.ShapeDtypeStruct((chunk, width), F32),
                jax.ShapeDtypeStruct((5, width), F32),
            ]
            if diag is None:
                outs.append(jax.ShapeDtypeStruct((3 * GROUP, width), F32))
            copies = blocks_tm * count if final else blocks_tm
            if last:
                outs.append(jax.ShapeDtypeStruct((copies, 2 * lines + final, LANES), F32))
            found = pl.pallas_call(
                functools.partial(step_kernel, count, index, CHUNKS, step, copies),
                out_shape=outs,
                in_specs=vmem(len(operands)),
                out_specs=vmem(len(outs)),
                scratch_shapes=[pltpu.VMEM((height, full), BF16)]
                + [pltpu.VMEM((3, height, TILE), F32)] * (width // TILE),
                compiler_params=params(32),
                cost_estimate=cost(2 * height * full * 3 * width, 6 * full * width),
            )(*operands)
            maps += found[:2]
            ends = found[2]
            diag = found[3] if diag is None else diag
        every = lax.all_to_all(found[-1], ("tm", "hid") if final else "tm", 0, 0)
        outs = [jax.ShapeDtypeStruct((rows, width), F32)]
        if final:
            outs.append(jax.ShapeDtypeStruct((ITERS,), F32))
            specs = vmem(1) + smem()
        else:
            outs.append(jax.ShapeDtypeStruct((1, width), F32))
            outs.append(jax.ShapeDtypeStruct((rows, width), BF16))
            outs += [jax.ShapeDtypeStruct((chunk, width), BF16)] * CHUNKS
            specs = vmem(len(outs))
        result = pl.pallas_call(
            functools.partial(apply_kernel, CHUNKS, final, count),
            out_shape=outs,
            in_specs=vmem(2 * CHUNKS + 2),
            out_specs=specs,
            compiler_params=params(16),
            cost_estimate=cost(2 * rows * width, 16 * rows * width),
        )(*maps, ends, every)
        if final:
            return (result[0], result[1])
        state, following, whole, *moved = result


def solution(mesh):
    return jax.shard_map(
        newton,
        mesh=mesh,
        in_specs=(
            P("tm"),
            P(None, None, "hid"),
            P(None, None, "hid"),
            P("hid"),
            P("hid"),
            P("hid"),
            P("tm", "hid"),
        ),
        out_specs=(P("tm", "hid"), P()),
        check_vma=False,
    )
```

```python
import functools

import jax
import jax.numpy as jnp
from jax import lax
from jax.experimental import pallas as pl
from jax.experimental.pallas import tpu as pltpu
from jax.sharding import PartitionSpec as P


ITERS = 2
CHUNKS = 2
GROUP = 8
EXTRA = 16
TILE = 256
LANES = 128
COVER = 2_000_000_000
F32 = jnp.float32
BF16 = jnp.bfloat16


def swapped(block, axis, bit):
    route = [(i, i ^ bit) for i in range(lax.axis_size(axis))]
    return lax.ppermute(block, axis, route)


def from_next(block, axis):
    route = [(i + 1, i) for i in range(lax.axis_size(axis) - 1)]
    return lax.ppermute(block, axis, route)


def sigmoid(x):
    return 0.5 * jnp.tanh(0.5 * x) + 0.5


def vmem(count):
    return [pl.BlockSpec(memory_space=pltpu.VMEM)] * count


def smem():
    return [pl.BlockSpec(memory_space=pltpu.SMEM)]


def params(mib):
    return pltpu.CompilerParams(vmem_limit_bytes=mib * 1024 * 1024)


def cost(flops, moved):
    return pl.CostEstimate(flops=flops, bytes_accessed=moved, transcendentals=0)


def merge_kernel(guess_ref, init_ref, opening_ref, whole_ref, *parts):
    chunk, width = opening_ref.shape
    whole_ref[pl.ds(0, chunk), :] = opening_ref[...]
    for index, part in enumerate(parts):
        lead = part.shape[0] - chunk
        at = (index + 1) * chunk
        if lead:
            row = lax.broadcasted_iota(jnp.int32, (lead, width), 0)
            head = jnp.where(row == 0, jnp.broadcast_to(init_ref[...], (lead, width)), 0.0).astype(BF16)
            part[pl.ds(0, lead), :] = head
            whole_ref[pl.ds(at, lead), :] = head
        for start in range(0, chunk, GROUP * 4):
            block = guess_ref[pl.ds(at + start, GROUP * 4), :].astype(BF16)
            part[pl.ds(lead + start, GROUP * 4), :] = block
            whole_ref[pl.ds(at + lead + start, GROUP * 4), :] = block


def prepare_kernel(ids_ref, guess_ref, table_ref, bias_ref, out_ref, line_ref):
    vocab, width = table_ref.shape[1:]
    rows = ids_ref.shape[1]
    ids = ids_ref[...]

    def spread(line):
        entry = lax.broadcasted_iota(jnp.int32, (vocab, line.shape[1]), 0)
        return (entry == line).astype(F32).astype(BF16)

    def pick(hot, part):
        return lax.dot_general(hot, part, (((0,), (0,)), ((), ())), preferred_element_type=F32)

    hot, hot_begin = spread(pltpu.roll(ids, rows - 1, 1)), spread(jnp.broadcast_to(ids[:, 0:1], (1, LANES)))
    line_ref[:, pl.ds(0, width)] = guess_ref[0:1, :]
    for gate in range(3):
        table = table_ref[gate]
        if gate == 0:
            table = table + bias_ref[...]
        total = None
        for _ in range(3):
            part = table.astype(BF16)
            table = table - part.astype(F32)
            picked = (pick(hot, part), pick(hot_begin, part))
            total = picked if total is None else (total[0] + picked[0], total[1] + picked[1])
        out_ref[gate, pl.ds(0, rows), :] = total[0]
        out_ref[gate, pl.ds(rows, GROUP), :] = total[1][0:GROUP]
        line_ref[:, pl.ds((gate + 1) * width, width)] = total[1][0:1]


def diagonals(weight_ref, hid, diag_ref):
    width = diag_ref.shape[1]
    row = lax.broadcasted_iota(jnp.int32, (width, width), 0)
    col = lax.broadcasted_iota(jnp.int32, (width, width), 1)
    first = pl.multiple_of(hid * width, width)
    for gate in range(3):
        block = weight_ref[gate, pl.ds(first, width), :].astype(F32)
        line = jnp.sum(jnp.where(row == col, block, 0.0), axis=0, keepdims=True)
        diag_ref[pl.ds(gate * GROUP, GROUP), :] = jnp.broadcast_to(line, (GROUP, width))


def gates(inputs, products, prev, hn_bias):
    zeta = sigmoid(inputs[0] + products[0])
    reset = sigmoid(inputs[1] + products[1])
    cand_pre = products[2] + hn_bias
    gated = reset * cand_pre
    cand = jnp.tanh(inputs[2] + gated)
    gap = prev - cand
    return zeta, reset, gated, cand, gap, cand + zeta * gap


def step_kernel(count, index, chunks, step, copies, *refs):
    refs = list(refs)
    near = [refs.pop(0) for _ in range(count // 2)]
    far = [refs.pop(0) for _ in range(count // 2)]
    weight_ref, inputs_ref, state_ref, next_ref, edge_ref, bias_ref, init_ref = [refs.pop(0) for _ in range(7)]
    opens = index == 0 and step == 0
    before_ref = None if opens else refs.pop(0)
    diag_ref = None if opens else refs.pop(0)
    a_ref, b_ref, ends_ref = [refs.pop(0) for _ in range(3)]
    diag_ref = refs.pop(0) if opens else diag_ref
    last = index == chunks - 1
    begins = last and step == 0
    send_ref = refs.pop(0) if last else None
    lhs, *products = refs
    height, full = lhs.shape
    rows, width = state_ref.shape
    chunk = rows // chunks
    start = index * chunk
    lead = height - chunk
    hid = lax.axis_index("hid")
    is_first = lax.axis_index("tm") == 0
    is_last = lax.axis_index("tm") == lax.axis_size("tm") - 1
    groups = chunk // GROUP
    tiles = width // TILE

    if opens:
        diagonals(weight_ref, hid, diag_ref)
    for offset in range(count):
        place = pl.multiple_of((hid ^ offset) * width, width)
        if offset < count // 2:
            lhs[:, pl.ds(place, width)] = near[offset][pl.ds(start, height), :]
        else:
            lhs[:, pl.ds(place, width)] = far[offset - count // 2][...]
    row = lax.broadcasted_iota(jnp.int32, (GROUP, TILE), 0)
    zeros = jnp.zeros((GROUP, TILE), F32)

    def dots(tile):
        lanes = pl.ds(tile * TILE, TILE)
        half = full // 2
        for gate in range(2):
            products[tile][gate] = jnp.dot(lhs[...], weight_ref[gate, :, lanes], preferred_element_type=F32)
        left = jnp.dot(lhs[:, pl.ds(0, half)], weight_ref[2, pl.ds(0, half), lanes], preferred_element_type=F32)
        right = jnp.dot(lhs[:, pl.ds(half, half)], weight_ref[2, pl.ds(half, half), lanes], preferred_element_type=F32)
        products[tile][2] = left + right

    def cells(tile):
        lanes = pl.ds(tile * TILE, TILE)
        hn_bias = jnp.broadcast_to(bias_ref[:, lanes], (GROUP, TILE))
        diag_z = diag_ref[pl.ds(0, GROUP), lanes]
        diag_r = diag_ref[pl.ds(GROUP, GROUP), lanes]
        diag_n = diag_ref[pl.ds(2 * GROUP, GROUP), lanes]
        squares = zeros
        if index == 0:
            run_a, run_b = jnp.ones((GROUP, TILE), F32), zeros
        else:
            run_a = jnp.broadcast_to(before_ref[0:1, lanes], (GROUP, TILE))
            run_b = jnp.broadcast_to(before_ref[1:2, lanes], (GROUP, TILE))
        turned = pltpu.roll(state_ref[pl.ds(start, GROUP), lanes], GROUP - 1, 0)
        for group in range(groups):
            here = pl.ds(group * GROUP, GROUP)
            token = pl.ds(start + group * GROUP, GROUP)
            prev = state_ref[token, lanes]
            if last and group == groups - 1:
                following = jnp.broadcast_to(next_ref[:, lanes], (GROUP, TILE))
            else:
                following = state_ref[pl.ds(start + (group + 1) * GROUP, GROUP), lanes]
            turned_next = pltpu.roll(following, GROUP - 1, 0)
            state = jnp.where(row == GROUP - 1, turned_next, turned)
            turned = turned_next
            terms = [inputs_ref[gate, token, lanes] for gate in range(3)]
            if last and group == groups - 1:
                for gate in range(3):
                    edge = edge_ref[:, pl.ds((gate + 1) * width + tile * TILE, TILE)]
                    terms[gate] = jnp.where(row == GROUP - 1, jnp.broadcast_to(edge, (GROUP, TILE)), terms[gate])
            zeta, reset, gated, cand, gap, value = gates(
                terms,
                [products[tile][gate, pl.ds(lead + group * GROUP, GROUP), :] for gate in range(3)],
                prev,
                hn_bias,
            )
            rest = 1.0 - zeta
            slope = zeta + gap * (zeta * rest) * diag_z
            slope = slope + rest * (1.0 - cand * cand) * (reset * diag_n + gated * (1.0 - reset) * diag_r)
            error = state - value
            if last and group == groups - 1:
                error = jnp.where((row == GROUP - 1) & is_last, 0.0, error)
            squares = squares + error * error
            a = slope
            b = value - slope * prev
            for distance in (1, 2, 4):
                keep = row >= distance
                a_up = jnp.where(keep, pltpu.roll(a, distance, 0), 1.0)
                b_up = jnp.where(keep, pltpu.roll(b, distance, 0), 0.0)
                b = a * b_up + b
                a = a * a_up
            a_ref[here, lanes] = a * run_a
            b_ref[here, lanes] = a * run_b + b
            last_a = jnp.broadcast_to(a[GROUP - 1 :], (GROUP, TILE))
            last_b = jnp.broadcast_to(b[GROUP - 1 :], (GROUP, TILE))
            run_a, run_b = last_a * run_a, last_a * run_b + last_b
        if begins:
            begin = gates(
                [inputs_ref[gate, pl.ds(rows, GROUP), lanes] for gate in range(3)],
                [products[tile][gate, pl.ds(0, GROUP), :] for gate in range(3)],
                jnp.broadcast_to(init_ref[:, lanes], (GROUP, TILE)),
                hn_bias,
            )[-1]
            error = state_ref[pl.ds(0, GROUP), lanes] - begin
            squares = squares + jnp.where((row == 0) & is_first, error * error, 0.0)
            begin = begin[0:1]
            earlier = zeros[0:1]
        elif step == 0:
            begin, earlier = zeros[0:1], zeros[0:1]
        else:
            begin = before_ref[3:4, lanes]
            earlier = before_ref[2:3, lanes] if index == 0 else before_ref[4:5, lanes]
        total = jnp.sum(squares, axis=0, keepdims=True)
        if index:
            total = total + before_ref[2:3, lanes]
        ends_ref[0:1, lanes] = run_a[0:1]
        ends_ref[1:2, lanes] = run_b[0:1]
        ends_ref[2:3, lanes] = total
        ends_ref[3:4, lanes] = begin
        ends_ref[4:5, lanes] = earlier
        if last:
            send_a = jnp.where(is_first, 0.0, run_a[0:1])
            send_b = jnp.where(is_first, run_a[0:1] * begin + run_b[0:1], run_b[0:1])
            for part in range(TILE // LANES):
                at = tile * (TILE // LANES) + part
                for line, sent in ((at, send_a), (width // LANES + at, send_b)):
                    picked = sent[:, part * LANES : (part + 1) * LANES]
                    send_ref[:, pl.ds(line, 1), :] = jnp.broadcast_to(picked[None], (copies, 1, LANES))

    dots(0)
    for tile in range(1, tiles):
        dots(tile)
        cells(tile - 1)
    cells(tiles - 1)
    if last and step == ITERS - 1:
        lane = lax.broadcasted_iota(jnp.int32, (1, LANES), 1)
        sums = jnp.zeros((1, LANES), F32)
        for line, half in ((4, 0), (2, 1)):
            part = sum(ends_ref[pl.ds(line, 1), pl.ds(at, LANES)] for at in range(0, width, LANES))
            part = part + pltpu.roll(part, LANES // 2, 1)
            sums = jnp.where(lane // (LANES // 2) == half, part, sums)
        send_ref[:, pl.ds(2 * width // LANES, 1), :] = jnp.broadcast_to(sums[None], (copies, 1, LANES))


def apply_kernel(chunks, final, count, *refs):
    maps, refs = refs[: 2 * chunks], refs[2 * chunks :]
    begin_ref, all_ref, state_ref = refs[:3]
    outs = refs[3:]
    chunk, width = maps[0].shape
    lines = width // LANES
    place = lax.axis_index("tm")
    hid = lax.axis_index("hid")
    copies = all_ref.shape[0]
    peers = copies // count if final else copies

    def compose(peer, enter):
        slot = peer * count + hid if final else peer
        moved = all_ref[slot, pl.ds(0, lines), :] * enter + all_ref[slot, pl.ds(lines, lines), :]
        return jnp.where(peer < place, moved, enter)

    begin = jnp.concatenate([begin_ref[3:4, pl.ds(at * LANES, LANES)] for at in range(lines)], axis=0)
    found = lax.fori_loop(0, peers, compose, begin, unroll=min(peers, 8))
    enter = jnp.concatenate([found[at : at + 1] for at in range(lines)], axis=1)
    if final:
        total = jnp.sum(all_ref[:, pl.ds(2 * lines, 1), :], axis=0)
        lane = lax.broadcasted_iota(jnp.int32, (1, LANES), 1)
        size = copies * chunk * chunks * width
        for half in range(2):
            outs[0][half] = jnp.sqrt(jnp.sum(jnp.where(lane // (LANES // 2) == half, total, 0.0)) / size)
    step = 2 * GROUP
    row = lax.broadcasted_iota(jnp.int32, (step, width), 0)
    enter = jnp.broadcast_to(enter, (step, width))
    before = enter
    for index in range(chunks):
        a_ref, b_ref = maps[2 * index], maps[2 * index + 1]

        def advance(group, before):
            here = pl.ds(pl.multiple_of(group * step, step), step)
            token = pl.ds(pl.multiple_of(index * chunk + group * step, step), step)
            turned = pltpu.roll(a_ref[here, :] * enter + b_ref[here, :], 1, 0)
            moved = jnp.where(row == 0, before, turned)
            state_ref[token, :] = moved
            if not final:
                rounded = moved.astype(BF16)
                outs[1][token, :] = rounded
                outs[2 + index][here, :] = rounded
            return turned

        before = lax.fori_loop(0, chunk // step, advance, before, unroll=2)
    if not final:
        outs[0][...] = before[0:1]


def newton(token_ids, input_table, recur_weight, z_bias, hn_bias, init_state, guess):
    rows, width = guess.shape
    full = recur_weight.shape[0]
    count = lax.axis_size("hid")
    blocks_tm = lax.axis_size("tm")
    weight = jnp.transpose(recur_weight, (1, 0, 2))
    table = jnp.transpose(input_table, (1, 0, 2))
    chunk = rows // CHUNKS
    lines = width // LANES

    opening, rest = lax.optimization_barrier((guess[:chunk].astype(BF16), guess))
    whole, *moved = pl.pallas_call(
        merge_kernel,
        out_shape=[jax.ShapeDtypeStruct((rows + EXTRA, width), BF16)]
        + [jax.ShapeDtypeStruct((chunk + EXTRA * (index == CHUNKS - 1), width), BF16) for index in range(1, CHUNKS)],
        in_specs=vmem(3),
        out_specs=vmem(CHUNKS),
        compiler_params=params(8),
        cost_estimate=cost(COVER, 8 * rows * width),
        name="merge",
    )(rest, init_state[None], opening)
    moved = [opening, *moved]
    inputs, line = pl.pallas_call(
        prepare_kernel,
        out_shape=[
            jax.ShapeDtypeStruct((3, rows + GROUP, width), F32),
            jax.ShapeDtypeStruct((1, 4 * width), F32),
        ],
        in_specs=vmem(4),
        out_specs=vmem(2),
        compiler_params=params(32),
        cost_estimate=cost(2 * COVER, 8 * rows * width),
        name="prepare",
    )(token_ids[None], rest, table, z_bias[None])
    edge = from_next(line, "tm")
    state, following = rest, edge

    ends, diag = None, None
    for step in range(ITERS):
        final = step == ITERS - 1
        near = {0: whole}
        far = [{count // 2: None} for _ in range(CHUNKS)]
        for index in range(CHUNKS):
            far[index][count // 2] = swapped(moved[index], "hid", count // 2)
        bit = count // 4
        while bit:
            for offset in list(near):
                near[offset | bit] = swapped(near[offset], "hid", bit)
            for index in range(CHUNKS):
                for offset in list(far[index]):
                    far[index][offset | bit] = swapped(far[index][offset], "hid", bit)
            bit //= 2
        maps = []
        for index in range(CHUNKS):
            last = index == CHUNKS - 1
            height = moved[index].shape[0]
            operands = [near[offset] for offset in range(count // 2)]
            operands += [far[index][offset] for offset in range(count // 2, count)]
            operands += [weight, inputs, state, following, edge, hn_bias[None], init_state[None]]
            if diag is not None:
                operands += [ends, diag]
            outs = [
                jax.ShapeDtypeStruct((chunk, width), F32),
                jax.ShapeDtypeStruct((chunk, width), F32),
                jax.ShapeDtypeStruct((5, width), F32),
            ]
            if diag is None:
                outs.append(jax.ShapeDtypeStruct((3 * GROUP, width), F32))
            copies = blocks_tm * count if final else blocks_tm
            if last:
                outs.append(jax.ShapeDtypeStruct((copies, 2 * lines + final, LANES), F32))
            found = pl.pallas_call(
                functools.partial(step_kernel, count, index, CHUNKS, step, copies),
                out_shape=outs,
                in_specs=vmem(len(operands)),
                out_specs=vmem(len(outs)),
                scratch_shapes=[pltpu.VMEM((height, full), BF16)]
                + [pltpu.VMEM((3, height, TILE), F32)] * (width // TILE),
                compiler_params=params(32),
                cost_estimate=cost(2 * height * full * 3 * width, 6 * full * width),
            )(*operands)
            maps += found[:2]
            ends = found[2]
            diag = found[3] if diag is None else diag
        every = lax.all_to_all(found[-1], ("tm", "hid") if final else "tm", 0, 0)
        outs = [jax.ShapeDtypeStruct((rows, width), F32)]
        if final:
            outs.append(jax.ShapeDtypeStruct((ITERS,), F32))
            specs = vmem(1) + smem()
        else:
            outs.append(jax.ShapeDtypeStruct((1, width), F32))
            outs.append(jax.ShapeDtypeStruct((rows, width), BF16))
            outs += [jax.ShapeDtypeStruct((chunk, width), BF16)] * CHUNKS
            specs = vmem(len(outs))
        result = pl.pallas_call(
            functools.partial(apply_kernel, CHUNKS, final, count),
            out_shape=outs,
            in_specs=vmem(2 * CHUNKS + 2),
            out_specs=specs,
            compiler_params=params(16),
            cost_estimate=cost(2 * rows * width, 16 * rows * width),
        )(*maps, ends, every)
        if final:
            return (result[0], result[1])
        state, following, whole, *moved = result


def solution(mesh):
    return jax.shard_map(
        newton,
        mesh=mesh,
        in_specs=(
            P("tm"),
            P(None, None, "hid"),
            P(None, None, "hid"),
            P("hid"),
            P("hid"),
            P("hid"),
            P("tm", "hid"),
        ),
        out_specs=(P("tm", "hid"), P()),
        check_vma=False,
    )
```

```python
import functools

import jax
import jax.numpy as jnp
from jax import lax
from jax.experimental import pallas as pl
from jax.experimental.pallas import tpu as pltpu
from jax.sharding import PartitionSpec as P


ITERS = 2
SHARES = ((8, 8), (9, 7))
CHUNKS = len(SHARES[0])
GROUP = 8
EXTRA = 16
TILE = 256
LANES = 128
COVER = 2_000_000_000
F32 = jnp.float32
BF16 = jnp.bfloat16


def swapped(block, axis, bit):
    route = [(i, i ^ bit) for i in range(lax.axis_size(axis))]
    return lax.ppermute(block, axis, route)


def from_next(block, axis):
    route = [(i + 1, i) for i in range(lax.axis_size(axis) - 1)]
    return lax.ppermute(block, axis, route)


def sigmoid(x):
    return 0.5 * jnp.tanh(0.5 * x) + 0.5


def spans(step, rows):
    unit = rows // sum(SHARES[step])
    found, at = [], 0
    for share in SHARES[step]:
        found.append((at, share * unit))
        at += share * unit
    return found


def vmem(count):
    return [pl.BlockSpec(memory_space=pltpu.VMEM)] * count


def smem():
    return [pl.BlockSpec(memory_space=pltpu.SMEM)]


def params(mib):
    return pltpu.CompilerParams(vmem_limit_bytes=mib * 1024 * 1024)


def cost(flops, moved):
    return pl.CostEstimate(flops=flops, bytes_accessed=moved, transcendentals=0)


def merge_kernel(guess_ref, init_ref, opening_ref, whole_ref, *parts):
    rows, width = guess_ref.shape
    whole_ref[pl.ds(0, opening_ref.shape[0]), :] = opening_ref[...]
    for (at, chunk), part in zip(spans(0, rows)[1:], parts):
        lead = part.shape[0] - chunk
        if lead:
            row = lax.broadcasted_iota(jnp.int32, (lead, width), 0)
            head = jnp.where(row == 0, jnp.broadcast_to(init_ref[...], (lead, width)), 0.0).astype(BF16)
            part[pl.ds(0, lead), :] = head
            whole_ref[pl.ds(at, lead), :] = head
        for start in range(0, chunk, GROUP * 4):
            block = guess_ref[pl.ds(at + start, GROUP * 4), :].astype(BF16)
            part[pl.ds(lead + start, GROUP * 4), :] = block
            whole_ref[pl.ds(at + lead + start, GROUP * 4), :] = block


def prepare_kernel(ids_ref, guess_ref, table_ref, bias_ref, out_ref, line_ref):
    vocab, width = table_ref.shape[1:]
    rows = ids_ref.shape[1]
    ids = ids_ref[...]

    def spread(line):
        entry = lax.broadcasted_iota(jnp.int32, (vocab, line.shape[1]), 0)
        return (entry == line).astype(F32).astype(BF16)

    def pick(hot, part):
        return lax.dot_general(hot, part, (((0,), (0,)), ((), ())), preferred_element_type=F32)

    hot, hot_begin = spread(pltpu.roll(ids, rows - 1, 1)), spread(jnp.broadcast_to(ids[:, 0:1], (1, LANES)))
    line_ref[:, pl.ds(0, width)] = guess_ref[0:1, :]
    for gate in range(3):
        table = table_ref[gate]
        if gate == 0:
            table = table + bias_ref[...]
        total = None
        for _ in range(3):
            part = table.astype(BF16)
            table = table - part.astype(F32)
            picked = (pick(hot, part), pick(hot_begin, part))
            total = picked if total is None else (total[0] + picked[0], total[1] + picked[1])
        out_ref[gate, pl.ds(0, rows), :] = total[0]
        out_ref[gate, pl.ds(rows, GROUP), :] = total[1][0:GROUP]
        line_ref[:, pl.ds((gate + 1) * width, width)] = total[1][0:1]


def diagonals(weight_ref, hid, diag_ref):
    width = diag_ref.shape[1]
    row = lax.broadcasted_iota(jnp.int32, (width, width), 0)
    col = lax.broadcasted_iota(jnp.int32, (width, width), 1)
    first = pl.multiple_of(hid * width, width)
    for gate in range(3):
        block = weight_ref[gate, pl.ds(first, width), :].astype(F32)
        line = jnp.sum(jnp.where(row == col, block, 0.0), axis=0, keepdims=True)
        diag_ref[pl.ds(gate * GROUP, GROUP), :] = jnp.broadcast_to(line, (GROUP, width))


def gates(inputs, products, prev, hn_bias):
    zeta = sigmoid(inputs[0] + products[0])
    reset = sigmoid(inputs[1] + products[1])
    cand_pre = products[2] + hn_bias
    gated = reset * cand_pre
    cand = jnp.tanh(inputs[2] + gated)
    gap = prev - cand
    return zeta, reset, gated, cand, gap, cand + zeta * gap


def step_kernel(count, index, start, chunk, step, copies, *refs):
    refs = list(refs)
    near = [refs.pop(0) for _ in range(count // 2)]
    far = [refs.pop(0) for _ in range(count // 2)]
    weight_ref, inputs_ref, state_ref, bias_ref, init_ref = [refs.pop(0) for _ in range(5)]
    last = index == CHUNKS - 1
    next_ref, edge_ref = [refs.pop(0) for _ in range(2)] if last else (None, None)
    opens = index == 0 and step == 0
    before_ref = None if opens else refs.pop(0)
    diag_ref = None if opens else refs.pop(0)
    a_ref, b_ref, ends_ref = [refs.pop(0) for _ in range(3)]
    diag_ref = refs.pop(0) if opens else diag_ref
    begins = last and step == 0
    send_ref = refs.pop(0) if last else None
    lhs, *products = refs
    height, full = lhs.shape
    rows, width = state_ref.shape
    lead = height - chunk
    hid = lax.axis_index("hid")
    is_first = lax.axis_index("tm") == 0
    is_last = lax.axis_index("tm") == lax.axis_size("tm") - 1
    groups = chunk // GROUP
    tiles = width // TILE

    if opens:
        diagonals(weight_ref, hid, diag_ref)
    for offset in range(count):
        place = pl.multiple_of((hid ^ offset) * width, width)
        if offset < count // 2:
            lhs[:, pl.ds(place, width)] = near[offset][pl.ds(start, height), :]
        else:
            lhs[:, pl.ds(place, width)] = far[offset - count // 2][...]
    row = lax.broadcasted_iota(jnp.int32, (GROUP, TILE), 0)
    zeros = jnp.zeros((GROUP, TILE), F32)

    def dots(tile):
        lanes = pl.ds(tile * TILE, TILE)
        half = full // 2
        for gate in range(2):
            products[tile][gate] = jnp.dot(lhs[...], weight_ref[gate, :, lanes], preferred_element_type=F32)
        left = jnp.dot(lhs[:, pl.ds(0, half)], weight_ref[2, pl.ds(0, half), lanes], preferred_element_type=F32)
        right = jnp.dot(lhs[:, pl.ds(half, half)], weight_ref[2, pl.ds(half, half), lanes], preferred_element_type=F32)
        products[tile][2] = left + right

    def cells(tile):
        lanes = pl.ds(tile * TILE, TILE)
        hn_bias = jnp.broadcast_to(bias_ref[:, lanes], (GROUP, TILE))
        diag_z = diag_ref[pl.ds(0, GROUP), lanes]
        diag_r = diag_ref[pl.ds(GROUP, GROUP), lanes]
        diag_n = diag_ref[pl.ds(2 * GROUP, GROUP), lanes]
        squares = zeros
        if index == 0:
            run_a, run_b = jnp.ones((GROUP, TILE), F32), zeros
        else:
            run_a = jnp.broadcast_to(before_ref[0:1, lanes], (GROUP, TILE))
            run_b = jnp.broadcast_to(before_ref[1:2, lanes], (GROUP, TILE))
        turned = pltpu.roll(state_ref[pl.ds(start, GROUP), lanes], GROUP - 1, 0)
        for group in range(groups):
            here = pl.ds(group * GROUP, GROUP)
            token = pl.ds(start + group * GROUP, GROUP)
            prev = state_ref[token, lanes]
            if last and group == groups - 1:
                following = jnp.broadcast_to(next_ref[:, lanes], (GROUP, TILE))
            else:
                following = state_ref[pl.ds(start + (group + 1) * GROUP, GROUP), lanes]
            turned_next = pltpu.roll(following, GROUP - 1, 0)
            state = jnp.where(row == GROUP - 1, turned_next, turned)
            turned = turned_next
            terms = [inputs_ref[gate, token, lanes] for gate in range(3)]
            if last and group == groups - 1:
                for gate in range(3):
                    edge = edge_ref[:, pl.ds((gate + 1) * width + tile * TILE, TILE)]
                    terms[gate] = jnp.where(row == GROUP - 1, jnp.broadcast_to(edge, (GROUP, TILE)), terms[gate])
            zeta, reset, gated, cand, gap, value = gates(
                terms,
                [products[tile][gate, pl.ds(lead + group * GROUP, GROUP), :] for gate in range(3)],
                prev,
                hn_bias,
            )
            rest = 1.0 - zeta
            slope = zeta + gap * (zeta * rest) * diag_z
            slope = slope + rest * (1.0 - cand * cand) * (reset * diag_n + gated * (1.0 - reset) * diag_r)
            error = state - value
            if last and group == groups - 1:
                error = jnp.where((row == GROUP - 1) & is_last, 0.0, error)
            squares = squares + error * error
            a = slope
            b = value - slope * prev
            for distance in (1, 2, 4):
                keep = row >= distance
                a_up = jnp.where(keep, pltpu.roll(a, distance, 0), 1.0)
                b_up = jnp.where(keep, pltpu.roll(b, distance, 0), 0.0)
                b = a * b_up + b
                a = a * a_up
            a_ref[here, lanes] = a * run_a
            b_ref[here, lanes] = a * run_b + b
            last_a = jnp.broadcast_to(a[GROUP - 1 :], (GROUP, TILE))
            last_b = jnp.broadcast_to(b[GROUP - 1 :], (GROUP, TILE))
            run_a, run_b = last_a * run_a, last_a * run_b + last_b
        if begins:
            begin = gates(
                [inputs_ref[gate, pl.ds(rows, GROUP), lanes] for gate in range(3)],
                [products[tile][gate, pl.ds(0, GROUP), :] for gate in range(3)],
                jnp.broadcast_to(init_ref[:, lanes], (GROUP, TILE)),
                hn_bias,
            )[-1]
            error = state_ref[pl.ds(0, GROUP), lanes] - begin
            squares = squares + jnp.where((row == 0) & is_first, error * error, 0.0)
            begin = begin[0:1]
            earlier = zeros[0:1]
        elif step == 0:
            begin, earlier = zeros[0:1], zeros[0:1]
        else:
            begin = before_ref[3:4, lanes]
            earlier = before_ref[2:3, lanes] if index == 0 else before_ref[4:5, lanes]
        total = jnp.sum(squares, axis=0, keepdims=True)
        if index:
            total = total + before_ref[2:3, lanes]
        ends_ref[0:1, lanes] = run_a[0:1]
        ends_ref[1:2, lanes] = run_b[0:1]
        ends_ref[2:3, lanes] = total
        ends_ref[3:4, lanes] = begin
        ends_ref[4:5, lanes] = earlier
        if last:
            send_a = jnp.where(is_first, 0.0, run_a[0:1])
            send_b = jnp.where(is_first, run_a[0:1] * begin + run_b[0:1], run_b[0:1])
            for part in range(TILE // LANES):
                at = tile * (TILE // LANES) + part
                for line, sent in ((at, send_a), (width // LANES + at, send_b)):
                    picked = sent[:, part * LANES : (part + 1) * LANES]
                    send_ref[:, pl.ds(line, 1), :] = jnp.broadcast_to(picked[None], (copies, 1, LANES))

    dots(0)
    for tile in range(1, tiles):
        dots(tile)
        cells(tile - 1)
    cells(tiles - 1)
    if last and step == ITERS - 1:
        lane = lax.broadcasted_iota(jnp.int32, (1, LANES), 1)
        sums = jnp.zeros((1, LANES), F32)
        for line, half in ((4, 0), (2, 1)):
            part = sum(ends_ref[pl.ds(line, 1), pl.ds(at, LANES)] for at in range(0, width, LANES))
            part = part + pltpu.roll(part, LANES // 2, 1)
            sums = jnp.where(lane // (LANES // 2) == half, part, sums)
        send_ref[:, pl.ds(2 * width // LANES, 1), :] = jnp.broadcast_to(sums[None], (copies, 1, LANES))


def apply_kernel(step, count, *refs):
    final = step == ITERS - 1
    maps, refs = refs[: 2 * CHUNKS], refs[2 * CHUNKS :]
    begin_ref, all_ref, state_ref = refs[:3]
    outs = refs[3:]
    rows, width = state_ref.shape
    lines = width // LANES
    place = lax.axis_index("tm")
    hid = lax.axis_index("hid")
    copies = all_ref.shape[0]
    peers = copies // count if final else copies

    def compose(peer, enter):
        slot = peer * count + hid if final else peer
        moved = all_ref[slot, pl.ds(0, lines), :] * enter + all_ref[slot, pl.ds(lines, lines), :]
        return jnp.where(peer < place, moved, enter)

    begin = jnp.concatenate([begin_ref[3:4, pl.ds(at * LANES, LANES)] for at in range(lines)], axis=0)
    found = lax.fori_loop(0, peers, compose, begin, unroll=min(peers, 8))
    enter = jnp.concatenate([found[at : at + 1] for at in range(lines)], axis=1)
    if final:
        total = jnp.sum(all_ref[:, pl.ds(2 * lines, 1), :], axis=0)
        lane = lax.broadcasted_iota(jnp.int32, (1, LANES), 1)
        size = copies * rows * width
        for half in range(2):
            outs[0][half] = jnp.sqrt(jnp.sum(jnp.where(lane // (LANES // 2) == half, total, 0.0)) / size)
    height = 2 * GROUP
    row = lax.broadcasted_iota(jnp.int32, (height, width), 0)
    enter = jnp.broadcast_to(enter, (height, width))
    before = enter
    held = spans(step, rows)
    sent = held if final else spans(step + 1, rows)
    cuts = sorted({at for at, _ in held + sent} | {rows})
    for low, high in zip(cuts, cuts[1:]):
        source = max(place for place, (at, _) in enumerate(held) if at <= low)
        target = max(place for place, (at, _) in enumerate(sent) if at <= low)
        a_ref, b_ref = maps[2 * source], maps[2 * source + 1]

        def advance(group, before):
            at = low + group * height
            here = pl.ds(pl.multiple_of(at - held[source][0], height), height)
            token = pl.ds(pl.multiple_of(at, height), height)
            turned = pltpu.roll(a_ref[here, :] * enter + b_ref[here, :], 1, 0)
            moved = jnp.where(row == 0, before, turned)
            state_ref[token, :] = moved
            if not final:
                rounded = moved.astype(BF16)
                outs[1][token, :] = rounded
                outs[2 + target][pl.ds(pl.multiple_of(at - sent[target][0], height), height), :] = rounded
            return turned

        before = lax.fori_loop(0, (high - low) // height, advance, before, unroll=2)
    if not final:
        outs[0][...] = before[0:1]


def newton(token_ids, input_table, recur_weight, z_bias, hn_bias, init_state, guess):
    rows, width = guess.shape
    full = recur_weight.shape[0]
    count = lax.axis_size("hid")
    blocks_tm = lax.axis_size("tm")
    weight = jnp.transpose(recur_weight, (1, 0, 2))
    table = jnp.transpose(input_table, (1, 0, 2))
    lines = width // LANES

    first = spans(0, rows)[0][1]
    opening, rest = lax.optimization_barrier((guess[:first].astype(BF16), guess))
    whole, *moved = pl.pallas_call(
        merge_kernel,
        out_shape=[jax.ShapeDtypeStruct((rows + EXTRA, width), BF16)]
        + [
            jax.ShapeDtypeStruct((height + EXTRA * (at + height == rows), width), BF16)
            for at, height in spans(0, rows)[1:]
        ],
        in_specs=vmem(3),
        out_specs=vmem(CHUNKS),
        compiler_params=params(8),
        cost_estimate=cost(COVER, 8 * rows * width),
        name="merge",
    )(rest, init_state[None], opening)
    moved = [opening, *moved]
    inputs, line = pl.pallas_call(
        prepare_kernel,
        out_shape=[
            jax.ShapeDtypeStruct((3, rows + GROUP, width), F32),
            jax.ShapeDtypeStruct((1, 4 * width), F32),
        ],
        in_specs=vmem(4),
        out_specs=vmem(2),
        compiler_params=params(32),
        cost_estimate=cost(2 * COVER, 8 * rows * width),
        name="prepare",
    )(token_ids[None], rest, table, z_bias[None])
    edge = from_next(line, "tm")
    state, following = rest, edge

    ends, diag = None, None
    for step in range(ITERS):
        final = step == ITERS - 1
        near = {0: whole}
        far = [{count // 2: None} for _ in range(CHUNKS)]
        for index in range(CHUNKS):
            far[index][count // 2] = swapped(moved[index], "hid", count // 2)
        bit = count // 4
        while bit:
            for offset in list(near):
                near[offset | bit] = swapped(near[offset], "hid", bit)
            for index in range(CHUNKS):
                for offset in list(far[index]):
                    far[index][offset | bit] = swapped(far[index][offset], "hid", bit)
            bit //= 2
        maps = []
        for index, (start, chunk) in enumerate(spans(step, rows)):
            last = index == CHUNKS - 1
            height = moved[index].shape[0]
            operands = [near[offset] for offset in range(count // 2)]
            operands += [far[index][offset] for offset in range(count // 2, count)]
            operands += [weight, inputs, state, hn_bias[None], init_state[None]]
            if last:
                operands += [following, edge]
            if diag is not None:
                operands += [ends, diag]
            outs = [
                jax.ShapeDtypeStruct((chunk, width), F32),
                jax.ShapeDtypeStruct((chunk, width), F32),
                jax.ShapeDtypeStruct((5, width), F32),
            ]
            if diag is None:
                outs.append(jax.ShapeDtypeStruct((3 * GROUP, width), F32))
            copies = blocks_tm * count if final else blocks_tm
            if last:
                outs.append(jax.ShapeDtypeStruct((copies, 2 * lines + final, LANES), F32))
            found = pl.pallas_call(
                functools.partial(step_kernel, count, index, start, chunk, step, copies),
                out_shape=outs,
                in_specs=vmem(len(operands)),
                out_specs=vmem(len(outs)),
                scratch_shapes=[pltpu.VMEM((height, full), BF16)]
                + [pltpu.VMEM((3, height, TILE), F32)] * (width // TILE),
                compiler_params=params(32),
                cost_estimate=cost(2 * height * full * 3 * width, 6 * full * width),
            )(*operands)
            maps += found[:2]
            ends = found[2]
            diag = found[3] if diag is None else diag
        every = lax.all_to_all(found[-1], ("tm", "hid") if final else "tm", 0, 0)
        outs = [jax.ShapeDtypeStruct((rows, width), F32)]
        if final:
            outs.append(jax.ShapeDtypeStruct((ITERS,), F32))
            specs = vmem(1) + smem()
        else:
            outs.append(jax.ShapeDtypeStruct((1, width), F32))
            outs.append(jax.ShapeDtypeStruct((rows, width), BF16))
            outs += [jax.ShapeDtypeStruct((chunk, width), BF16) for _, chunk in spans(step + 1, rows)]
            specs = vmem(len(outs))
        result = pl.pallas_call(
            functools.partial(apply_kernel, step, count),
            out_shape=outs,
            in_specs=vmem(2 * CHUNKS + 2),
            out_specs=specs,
            compiler_params=params(16),
            cost_estimate=cost(2 * rows * width, 16 * rows * width),
        )(*maps, ends, every)
        if final:
            return (result[0], result[1])
        state, following, whole, *moved = result


def solution(mesh):
    return jax.shard_map(
        newton,
        mesh=mesh,
        in_specs=(
            P("tm"),
            P(None, None, "hid"),
            P(None, None, "hid"),
            P("hid"),
            P("hid"),
            P("hid"),
            P("tm", "hid"),
        ),
        out_specs=(P("tm", "hid"), P()),
        check_vma=False,
    )
```

```python
import functools

import jax
import jax.numpy as jnp
from jax import lax
from jax.experimental import pallas as pl
from jax.experimental.pallas import tpu as pltpu
from jax.sharding import PartitionSpec as P


ITERS = 2
SHARES = ((8, 8), (9, 7))
CHUNKS = len(SHARES[0])
GROUP = 8
EXTRA = 16
TILE = 256
LANES = 128
COVER = 2_000_000_000
F32 = jnp.float32
BF16 = jnp.bfloat16


def swapped(block, axis, bit):
    route = [(i, i ^ bit) for i in range(lax.axis_size(axis))]
    return lax.ppermute(block, axis, route)


def from_next(block, axis):
    route = [(i + 1, i) for i in range(lax.axis_size(axis) - 1)]
    return lax.ppermute(block, axis, route)


def sigmoid(x):
    return 0.5 * jnp.tanh(0.5 * x) + 0.5


def spans(step, rows):
    unit = rows // sum(SHARES[step])
    found, at = [], 0
    for share in SHARES[step]:
        found.append((at, share * unit))
        at += share * unit
    return found


def vmem(count):
    return [pl.BlockSpec(memory_space=pltpu.VMEM)] * count


def smem():
    return [pl.BlockSpec(memory_space=pltpu.SMEM)]


def params(mib):
    return pltpu.CompilerParams(vmem_limit_bytes=mib * 1024 * 1024)


def cost(flops, moved):
    return pl.CostEstimate(flops=flops, bytes_accessed=moved, transcendentals=0)


def merge_kernel(guess_ref, init_ref, opening_ref, whole_ref, *parts):
    rows, width = guess_ref.shape
    whole_ref[pl.ds(0, opening_ref.shape[0]), :] = opening_ref[...]
    for (at, chunk), part in zip(spans(0, rows)[1:], parts):
        lead = part.shape[0] - chunk
        if lead:
            row = lax.broadcasted_iota(jnp.int32, (lead, width), 0)
            head = jnp.where(row == 0, jnp.broadcast_to(init_ref[...], (lead, width)), 0.0).astype(BF16)
            part[pl.ds(0, lead), :] = head
            whole_ref[pl.ds(at, lead), :] = head
        for start in range(0, chunk, GROUP * 4):
            block = guess_ref[pl.ds(at + start, GROUP * 4), :].astype(BF16)
            part[pl.ds(lead + start, GROUP * 4), :] = block
            whole_ref[pl.ds(at + lead + start, GROUP * 4), :] = block


def prepare_kernel(ids_ref, guess_ref, table_ref, bias_ref, out_ref, line_ref):
    vocab, width = table_ref.shape[1:]
    rows = ids_ref.shape[1]
    ids = ids_ref[...]

    def spread(line):
        entry = lax.broadcasted_iota(jnp.int32, (vocab, line.shape[1]), 0)
        return (entry == line).astype(F32).astype(BF16)

    def pick(hot, part):
        return lax.dot_general(hot, part, (((0,), (0,)), ((), ())), preferred_element_type=F32)

    lane = lax.broadcasted_iota(jnp.int32, (1, rows), 1)
    hot = spread(jnp.where(lane == rows - 1, vocab, pltpu.roll(ids, rows - 1, 1)))
    hot_begin = spread(jnp.broadcast_to(ids[:, 0:1], (1, LANES)))
    line_ref[:, pl.ds(0, width)] = guess_ref[0:1, :]
    for gate in range(3):
        table = table_ref[gate]
        if gate == 0:
            table = table + bias_ref[...]
        total = None
        for _ in range(3):
            part = table.astype(BF16)
            table = table - part.astype(F32)
            picked = (pick(hot, part), pick(hot_begin, part))
            total = picked if total is None else (total[0] + picked[0], total[1] + picked[1])
        out_ref[gate, pl.ds(0, rows), :] = total[0]
        out_ref[gate, pl.ds(rows, GROUP), :] = total[1][0:GROUP]
        line_ref[:, pl.ds((gate + 1) * width, width)] = total[1][0:1]


def diagonals(weight_ref, hid, diag_ref):
    width = diag_ref.shape[1]
    row = lax.broadcasted_iota(jnp.int32, (width, width), 0)
    col = lax.broadcasted_iota(jnp.int32, (width, width), 1)
    first = pl.multiple_of(hid * width, width)
    for gate in range(3):
        block = weight_ref[gate, pl.ds(first, width), :].astype(F32)
        line = jnp.sum(jnp.where(row == col, block, 0.0), axis=0, keepdims=True)
        diag_ref[pl.ds(gate * GROUP, GROUP), :] = jnp.broadcast_to(line, (GROUP, width))


def gates(bases, products, inputs, prev):
    zeta = sigmoid(bases[0] + products[0])
    reset = sigmoid(bases[1] + products[1])
    gated = reset * (bases[2] + products[2])
    cand = jnp.tanh(inputs + gated)
    gap = prev - cand
    return zeta, reset, gated, cand, gap, cand + zeta * gap


def tile_dot(lhs, weight_ref, first, gate, lanes):
    depth = lhs.shape[1]
    pieces = 2 if gate == 2 else 1
    total = None
    for piece in range(pieces):
        at = pl.multiple_of(first + piece * (depth // pieces), depth // pieces)
        term = jnp.dot(
            lhs[:, pl.ds(piece * (depth // pieces), depth // pieces)],
            weight_ref[gate, pl.ds(at, depth // pieces), lanes],
            preferred_element_type=F32,
        )
        total = term if total is None else total + term
    return total


def base_kernel(step, count, *refs):
    near, (weight_ref, inputs_ref, bias_ref, base_ref, lhs) = refs[: count // 2], refs[count // 2 :]
    height, _ = lhs.shape
    width = base_ref.shape[2]
    rows = inputs_ref.shape[1] - GROUP
    hid = lax.axis_index("hid")
    own = hid % (count // 2)
    for offset in range(count // 2):
        lhs[:, pl.ds(pl.multiple_of((own ^ offset) * width, width), width)] = near[offset][...]
    pieces, at = [], 0
    for start, chunk in spans(step, rows):
        if start + chunk == rows and height > rows:
            pieces.append((at, rows, GROUP))
            at += EXTRA
        pieces.append((at, start, chunk))
        at += chunk
    for tile in range(width // TILE):
        lanes = pl.ds(tile * TILE, TILE)
        for gate in range(3):
            found = tile_dot(lhs, weight_ref, (hid - own) * width, gate, lanes)
            if gate == 2:
                base_ref[gate, :, lanes] = found + bias_ref[:, lanes]
            else:
                for at, start, size in pieces:
                    base_ref[gate, pl.ds(at, size), lanes] = (
                        found[at : at + size] + inputs_ref[gate, pl.ds(start, size), lanes]
                    )


def step_kernel(count, index, start, chunk, step, copies, *refs):
    refs = list(refs)
    far = [refs.pop(0) for _ in range(count // 2)]
    weight_ref, base_ref, inputs_ref, state_ref, init_ref = [refs.pop(0) for _ in range(5)]
    last = index == CHUNKS - 1
    next_ref, edge_ref = [refs.pop(0) for _ in range(2)] if last else (None, None)
    opens = index == 0 and step == 0
    before_ref = None if opens else refs.pop(0)
    diag_ref = None if opens else refs.pop(0)
    a_ref, b_ref, ends_ref = [refs.pop(0) for _ in range(3)]
    diag_ref = refs.pop(0) if opens else diag_ref
    begins = last and step == 0
    send_ref = refs.pop(0) if last else None
    lhs, *products = refs
    height = lhs.shape[0]
    rows, width = state_ref.shape
    lead = height - chunk
    hid = lax.axis_index("hid")
    is_first = lax.axis_index("tm") == 0
    is_last = lax.axis_index("tm") == lax.axis_size("tm") - 1
    groups = chunk // GROUP
    tiles = width // TILE

    if opens:
        diagonals(weight_ref, hid, diag_ref)
    own = hid % (count // 2)
    for offset in range(count // 2):
        lhs[:, pl.ds(pl.multiple_of((own ^ offset) * width, width), width)] = far[offset][...]
    first = ((hid - own) ^ (count // 2)) * width
    row = lax.broadcasted_iota(jnp.int32, (GROUP, TILE), 0)
    zeros = jnp.zeros((GROUP, TILE), F32)

    def dots(tile):
        for gate in range(3):
            products[tile][gate] = tile_dot(lhs, weight_ref, first, gate, pl.ds(tile * TILE, TILE))

    def cells(tile):
        lanes = pl.ds(tile * TILE, TILE)
        diag_z = diag_ref[pl.ds(0, GROUP), lanes]
        diag_r = diag_ref[pl.ds(GROUP, GROUP), lanes]
        diag_n = diag_ref[pl.ds(2 * GROUP, GROUP), lanes]
        squares = zeros
        if index == 0:
            run_a, run_b = jnp.ones((GROUP, TILE), F32), zeros
        else:
            run_a = jnp.broadcast_to(before_ref[0:1, lanes], (GROUP, TILE))
            run_b = jnp.broadcast_to(before_ref[1:2, lanes], (GROUP, TILE))
        turned = pltpu.roll(state_ref[pl.ds(start, GROUP), lanes], GROUP - 1, 0)
        for group in range(groups):
            here = pl.ds(group * GROUP, GROUP)
            token = pl.ds(start + group * GROUP, GROUP)
            prev = state_ref[token, lanes]
            if last and group == groups - 1:
                following = jnp.broadcast_to(next_ref[:, lanes], (GROUP, TILE))
            else:
                following = state_ref[pl.ds(start + (group + 1) * GROUP, GROUP), lanes]
            turned_next = pltpu.roll(following, GROUP - 1, 0)
            state = jnp.where(row == GROUP - 1, turned_next, turned)
            turned = turned_next
            place = lead + group * GROUP
            bases = [base_ref[gate, pl.ds(start + place, GROUP), lanes] for gate in range(3)]
            inputs = inputs_ref[2, token, lanes]
            if last and group == groups - 1:
                edges = [edge_ref[:, pl.ds((gate + 1) * width + tile * TILE, TILE)] for gate in range(3)]
                edges = [jnp.where(row == GROUP - 1, jnp.broadcast_to(line, (GROUP, TILE)), 0.0) for line in edges]
                bases = [bases[0] + edges[0], bases[1] + edges[1], bases[2]]
                inputs = inputs + edges[2]
            found = [products[tile][gate, pl.ds(place, GROUP), :] for gate in range(3)]
            zeta, reset, gated, cand, gap, value = gates(bases, found, inputs, prev)
            rest = 1.0 - zeta
            slope = zeta + gap * (zeta * rest) * diag_z
            slope = slope + rest * (1.0 - cand * cand) * (reset * diag_n + gated * (1.0 - reset) * diag_r)
            error = state - value
            if last and group == groups - 1:
                error = jnp.where((row == GROUP - 1) & is_last, 0.0, error)
            squares = squares + error * error
            a = slope
            b = value - slope * prev
            for distance in (1, 2, 4):
                keep = row >= distance
                a_up = jnp.where(keep, pltpu.roll(a, distance, 0), 1.0)
                b_up = jnp.where(keep, pltpu.roll(b, distance, 0), 0.0)
                b = a * b_up + b
                a = a * a_up
            a_ref[here, lanes] = a * run_a
            b_ref[here, lanes] = a * run_b + b
            last_a = jnp.broadcast_to(a[GROUP - 1 :], (GROUP, TILE))
            last_b = jnp.broadcast_to(b[GROUP - 1 :], (GROUP, TILE))
            run_a, run_b = last_a * run_a, last_a * run_b + last_b
        if begins:
            begin = gates(
                [base_ref[gate, pl.ds(start, GROUP), lanes] for gate in range(3)],
                [products[tile][gate, pl.ds(0, GROUP), :] for gate in range(3)],
                inputs_ref[2, pl.ds(rows, GROUP), lanes],
                jnp.broadcast_to(init_ref[:, lanes], (GROUP, TILE)),
            )[-1]
            error = state_ref[pl.ds(0, GROUP), lanes] - begin
            squares = squares + jnp.where((row == 0) & is_first, error * error, 0.0)
            begin = begin[0:1]
            earlier = zeros[0:1]
        elif step == 0:
            begin, earlier = zeros[0:1], zeros[0:1]
        else:
            begin = before_ref[3:4, lanes]
            earlier = before_ref[2:3, lanes] if index == 0 else before_ref[4:5, lanes]
        total = jnp.sum(squares, axis=0, keepdims=True)
        if index:
            total = total + before_ref[2:3, lanes]
        ends_ref[0:1, lanes] = run_a[0:1]
        ends_ref[1:2, lanes] = run_b[0:1]
        ends_ref[2:3, lanes] = total
        ends_ref[3:4, lanes] = begin
        ends_ref[4:5, lanes] = earlier
        if last:
            send_a = jnp.where(is_first, 0.0, run_a[0:1])
            send_b = jnp.where(is_first, run_a[0:1] * begin + run_b[0:1], run_b[0:1])
            for part in range(TILE // LANES):
                at = tile * (TILE // LANES) + part
                for line, sent in ((at, send_a), (width // LANES + at, send_b)):
                    picked = sent[:, part * LANES : (part + 1) * LANES]
                    send_ref[:, pl.ds(line, 1), :] = jnp.broadcast_to(picked[None], (copies, 1, LANES))

    dots(0)
    for tile in range(1, tiles):
        dots(tile)
        cells(tile - 1)
    cells(tiles - 1)
    if last and step == ITERS - 1:
        lane = lax.broadcasted_iota(jnp.int32, (1, LANES), 1)
        sums = jnp.zeros((1, LANES), F32)
        for line, half in ((4, 0), (2, 1)):
            part = sum(ends_ref[pl.ds(line, 1), pl.ds(at, LANES)] for at in range(0, width, LANES))
            part = part + pltpu.roll(part, LANES // 2, 1)
            sums = jnp.where(lane // (LANES // 2) == half, part, sums)
        send_ref[:, pl.ds(2 * width // LANES, 1), :] = jnp.broadcast_to(sums[None], (copies, 1, LANES))


def apply_kernel(step, count, *refs):
    final = step == ITERS - 1
    maps, refs = refs[: 2 * CHUNKS], refs[2 * CHUNKS :]
    begin_ref, all_ref, state_ref = refs[:3]
    outs = refs[3:]
    rows, width = state_ref.shape
    lines = width // LANES
    place = lax.axis_index("tm")
    hid = lax.axis_index("hid")
    copies = all_ref.shape[0]
    peers = copies // count if final else copies

    def compose(peer, enter):
        slot = peer * count + hid if final else peer
        moved = all_ref[slot, pl.ds(0, lines), :] * enter + all_ref[slot, pl.ds(lines, lines), :]
        return jnp.where(peer < place, moved, enter)

    begin = jnp.concatenate([begin_ref[3:4, pl.ds(at * LANES, LANES)] for at in range(lines)], axis=0)
    found = lax.fori_loop(0, peers, compose, begin, unroll=min(peers, 8))
    enter = jnp.concatenate([found[at : at + 1] for at in range(lines)], axis=1)
    if final:
        total = jnp.sum(all_ref[:, pl.ds(2 * lines, 1), :], axis=0)
        lane = lax.broadcasted_iota(jnp.int32, (1, LANES), 1)
        size = copies * rows * width
        for half in range(2):
            outs[0][half] = jnp.sqrt(jnp.sum(jnp.where(lane // (LANES // 2) == half, total, 0.0)) / size)
    height = 2 * GROUP
    row = lax.broadcasted_iota(jnp.int32, (height, width), 0)
    enter = jnp.broadcast_to(enter, (height, width))
    before = enter
    held = spans(step, rows)
    sent = held if final else spans(step + 1, rows)
    cuts = sorted({at for at, _ in held + sent} | {rows})
    for low, high in zip(cuts, cuts[1:]):
        source = max(place for place, (at, _) in enumerate(held) if at <= low)
        target = max(place for place, (at, _) in enumerate(sent) if at <= low)
        a_ref, b_ref = maps[2 * source], maps[2 * source + 1]

        def advance(group, before):
            at = low + group * height
            here = pl.ds(pl.multiple_of(at - held[source][0], height), height)
            token = pl.ds(pl.multiple_of(at, height), height)
            turned = pltpu.roll(a_ref[here, :] * enter + b_ref[here, :], 1, 0)
            moved = jnp.where(row == 0, before, turned)
            state_ref[token, :] = moved
            if not final:
                rounded = moved.astype(BF16)
                outs[1][token, :] = rounded
                outs[2 + target][pl.ds(pl.multiple_of(at - sent[target][0], height), height), :] = rounded
            return turned

        before = lax.fori_loop(0, (high - low) // height, advance, before, unroll=2)
    if not final:
        outs[0][...] = before[0:1]


def newton(token_ids, input_table, recur_weight, z_bias, hn_bias, init_state, guess):
    rows, width = guess.shape
    full = recur_weight.shape[0]
    count = lax.axis_size("hid")
    blocks_tm = lax.axis_size("tm")
    weight = jnp.transpose(recur_weight, (1, 0, 2))
    table = jnp.transpose(input_table, (1, 0, 2))
    lines = width // LANES

    first = spans(0, rows)[0][1]
    opening, rest = lax.optimization_barrier((guess[:first].astype(BF16), guess))
    whole, *moved = pl.pallas_call(
        merge_kernel,
        out_shape=[jax.ShapeDtypeStruct((rows + EXTRA, width), BF16)]
        + [
            jax.ShapeDtypeStruct((height + EXTRA * (at + height == rows), width), BF16)
            for at, height in spans(0, rows)[1:]
        ],
        in_specs=vmem(3),
        out_specs=vmem(CHUNKS),
        compiler_params=params(8),
        cost_estimate=cost(COVER, 8 * rows * width),
        name="merge",
    )(rest, init_state[None], opening)
    moved = [opening, *moved]
    inputs, line = pl.pallas_call(
        prepare_kernel,
        out_shape=[
            jax.ShapeDtypeStruct((3, rows + GROUP, width), F32),
            jax.ShapeDtypeStruct((1, 4 * width), F32),
        ],
        in_specs=vmem(4),
        out_specs=vmem(2),
        compiler_params=params(32),
        cost_estimate=cost(2 * COVER, 8 * rows * width),
        name="prepare",
    )(token_ids[None], rest, table, z_bias[None])
    edge = from_next(line, "tm")
    state, following = rest, edge

    ends, diag = None, None
    for step in range(ITERS):
        final = step == ITERS - 1
        near = {0: whole}
        far = [{count // 2: None} for _ in range(CHUNKS)]
        for index in range(CHUNKS):
            far[index][count // 2] = swapped(moved[index], "hid", count // 2)
        bit = count // 4
        while bit:
            for offset in list(near):
                near[offset | bit] = swapped(near[offset], "hid", bit)
            for index in range(CHUNKS):
                for offset in list(far[index]):
                    far[index][offset | bit] = swapped(far[index][offset], "hid", bit)
            bit //= 2
        height = whole.shape[0]
        base = pl.pallas_call(
            functools.partial(base_kernel, step, count),
            out_shape=jax.ShapeDtypeStruct((3, height, width), F32),
            in_specs=vmem(count // 2 + 3),
            out_specs=vmem(1)[0],
            scratch_shapes=[pltpu.VMEM((height, full // 2), BF16)],
            compiler_params=params(16),
            cost_estimate=cost(3 * height * full * width, 3 * full * width),
        )(*[near[offset] for offset in range(count // 2)], weight, inputs, hn_bias[None])
        maps = []
        for index, (start, chunk) in enumerate(spans(step, rows)):
            last = index == CHUNKS - 1
            height = moved[index].shape[0]
            operands = [far[index][offset] for offset in range(count // 2, count)]
            operands += [weight, base, inputs, state, init_state[None]]
            if last:
                operands += [following, edge]
            if diag is not None:
                operands += [ends, diag]
            outs = [
                jax.ShapeDtypeStruct((chunk, width), F32),
                jax.ShapeDtypeStruct((chunk, width), F32),
                jax.ShapeDtypeStruct((5, width), F32),
            ]
            if diag is None:
                outs.append(jax.ShapeDtypeStruct((3 * GROUP, width), F32))
            copies = blocks_tm * count if final else blocks_tm
            if last:
                outs.append(jax.ShapeDtypeStruct((copies, 2 * lines + final, LANES), F32))
            found = pl.pallas_call(
                functools.partial(step_kernel, count, index, start, chunk, step, copies),
                out_shape=outs,
                in_specs=vmem(len(operands)),
                out_specs=vmem(len(outs)),
                scratch_shapes=[pltpu.VMEM((height, full // 2), BF16)]
                + [pltpu.VMEM((3, height, TILE), F32)] * (width // TILE),
                compiler_params=params(32),
                cost_estimate=cost(height * full * 3 * width, 3 * full * width),
            )(*operands)
            maps += found[:2]
            ends = found[2]
            diag = found[3] if diag is None else diag
        every = lax.all_to_all(found[-1], ("tm", "hid") if final else "tm", 0, 0)
        outs = [jax.ShapeDtypeStruct((rows, width), F32)]
        if final:
            outs.append(jax.ShapeDtypeStruct((ITERS,), F32))
            specs = vmem(1) + smem()
        else:
            outs.append(jax.ShapeDtypeStruct((1, width), F32))
            outs.append(jax.ShapeDtypeStruct((rows, width), BF16))
            outs += [jax.ShapeDtypeStruct((chunk, width), BF16) for _, chunk in spans(step + 1, rows)]
            specs = vmem(len(outs))
        result = pl.pallas_call(
            functools.partial(apply_kernel, step, count),
            out_shape=outs,
            in_specs=vmem(2 * CHUNKS + 2),
            out_specs=specs,
            compiler_params=params(16),
            cost_estimate=cost(2 * rows * width, 16 * rows * width),
        )(*maps, ends, every)
        if final:
            return (result[0], result[1])
        state, following, whole, *moved = result


def solution(mesh):
    return jax.shard_map(
        newton,
        mesh=mesh,
        in_specs=(
            P("tm"),
            P(None, None, "hid"),
            P(None, None, "hid"),
            P("hid"),
            P("hid"),
            P("hid"),
            P("tm", "hid"),
        ),
        out_specs=(P("tm", "hid"), P()),
        check_vma=False,
    )
```

```python
import functools

import jax
import jax.numpy as jnp
from jax import lax
from jax.experimental import pallas as pl
from jax.experimental.pallas import tpu as pltpu
from jax.sharding import PartitionSpec as P


ITERS = 2
SHARES = ((8, 8), (8, 8))
CHUNKS = len(SHARES[0])
GROUP = 8
EXTRA = 16
TILE = 256
LANES = 128
COVER = 2_000_000_000
F32 = jnp.float32
BF16 = jnp.bfloat16


def swapped(block, axis, bit):
    route = [(i, i ^ bit) for i in range(lax.axis_size(axis))]
    return lax.ppermute(block, axis, route)


def from_next(block, axis):
    route = [(i + 1, i) for i in range(lax.axis_size(axis) - 1)]
    return lax.ppermute(block, axis, route)


def sigmoid(x):
    return 0.5 * jnp.tanh(0.5 * x) + 0.5


def spans(step, rows):
    unit = rows // sum(SHARES[step])
    found, at = [], 0
    for share in SHARES[step]:
        found.append((at, share * unit))
        at += share * unit
    return found


def vmem(count):
    return [pl.BlockSpec(memory_space=pltpu.VMEM)] * count


def smem():
    return [pl.BlockSpec(memory_space=pltpu.SMEM)]


def params(mib):
    return pltpu.CompilerParams(vmem_limit_bytes=mib * 1024 * 1024)


def cost(flops, moved):
    return pl.CostEstimate(flops=flops, bytes_accessed=moved, transcendentals=0)


def merge_kernel(rounded_ref, init_ref, whole_ref, *parts):
    rows, width = rounded_ref.shape
    opening = spans(0, rows)[0][1]
    whole_ref[pl.ds(0, opening), :] = rounded_ref[pl.ds(0, opening), :]
    for (at, chunk), part in zip(spans(0, rows)[1:], parts):
        lead = part.shape[0] - chunk
        if lead:
            row = lax.broadcasted_iota(jnp.int32, (lead, width), 0)
            head = jnp.where(row == 0, jnp.broadcast_to(init_ref[...], (lead, width)), 0.0).astype(BF16)
            part[pl.ds(0, lead), :] = head
            whole_ref[pl.ds(at, lead), :] = head
        block = rounded_ref[pl.ds(at, chunk), :]
        part[pl.ds(lead, chunk), :] = block
        whole_ref[pl.ds(at + lead, chunk), :] = block


def prepare_kernel(ids_ref, guess_ref, table_ref, bias_ref, out_ref, line_ref):
    vocab, width = table_ref.shape[1:]
    rows = ids_ref.shape[1]
    ids = ids_ref[...]

    def spread(line):
        entry = lax.broadcasted_iota(jnp.int32, (vocab, line.shape[1]), 0)
        return (entry == line).astype(F32).astype(BF16)

    def pick(hot, part):
        return lax.dot_general(hot, part, (((0,), (0,)), ((), ())), preferred_element_type=F32)

    lane = lax.broadcasted_iota(jnp.int32, (1, rows), 1)
    hot = spread(jnp.where(lane == rows - 1, vocab, pltpu.roll(ids, rows - 1, 1)))
    hot_begin = spread(jnp.broadcast_to(ids[:, 0:1], (1, LANES)))
    line_ref[:, pl.ds(0, width)] = guess_ref[0:1, :]
    for gate in range(3):
        table = table_ref[gate]
        if gate == 0:
            table = table + bias_ref[...]
        total = None
        for _ in range(3):
            part = table.astype(BF16)
            table = table - part.astype(F32)
            picked = (pick(hot, part), pick(hot_begin, part))
            total = picked if total is None else (total[0] + picked[0], total[1] + picked[1])
        out_ref[gate, pl.ds(0, rows), :] = total[0]
        out_ref[gate, pl.ds(rows, GROUP), :] = total[1][0:GROUP]
        line_ref[:, pl.ds((gate + 1) * width, width)] = total[1][0:1]


def diagonals(weight_ref, hid, diag_ref):
    width = diag_ref.shape[1]
    row = lax.broadcasted_iota(jnp.int32, (width, width), 0)
    col = lax.broadcasted_iota(jnp.int32, (width, width), 1)
    first = pl.multiple_of(hid * width, width)
    for gate in range(3):
        block = weight_ref[gate, pl.ds(first, width), :].astype(F32)
        line = jnp.sum(jnp.where(row == col, block, 0.0), axis=0, keepdims=True)
        diag_ref[pl.ds(gate * GROUP, GROUP), :] = jnp.broadcast_to(line, (GROUP, width))


def gates(bases, products, inputs, prev):
    zeta = sigmoid(bases[0] + products[0])
    reset = sigmoid(bases[1] + products[1])
    gated = reset * (bases[2] + products[2])
    cand = jnp.tanh(inputs + gated)
    gap = prev - cand
    return zeta, reset, gated, cand, gap, cand + zeta * gap


def tile_dot(lhs, weight_ref, first, gate, lanes):
    depth = lhs.shape[1]
    pieces = 2 if gate == 2 else 1
    total = None
    for piece in range(pieces):
        at = pl.multiple_of(first + piece * (depth // pieces), depth // pieces)
        term = jnp.dot(
            lhs[:, pl.ds(piece * (depth // pieces), depth // pieces)],
            weight_ref[gate, pl.ds(at, depth // pieces), lanes],
            preferred_element_type=F32,
        )
        total = term if total is None else total + term
    return total


def base_kernel(step, count, *refs):
    near, (weight_ref, inputs_ref, bias_ref, base_ref, lhs) = refs[: count // 2], refs[count // 2 :]
    height, _ = lhs.shape
    width = base_ref.shape[2]
    rows = inputs_ref.shape[1] - GROUP
    hid = lax.axis_index("hid")
    own = hid % (count // 2)
    for offset in range(count // 2):
        lhs[:, pl.ds(pl.multiple_of((own ^ offset) * width, width), width)] = near[offset][...]
    pieces, at = [], 0
    for start, chunk in spans(step, rows):
        if start + chunk == rows and height > rows:
            pieces.append((at, rows, GROUP))
            at += EXTRA
        pieces.append((at, start, chunk))
        at += chunk
    for tile in range(width // TILE):
        lanes = pl.ds(tile * TILE, TILE)
        for gate in range(3):
            found = tile_dot(lhs, weight_ref, (hid - own) * width, gate, lanes)
            if gate == 2:
                base_ref[gate, :, lanes] = found + bias_ref[:, lanes]
            else:
                for at, start, size in pieces:
                    base_ref[gate, pl.ds(at, size), lanes] = (
                        found[at : at + size] + inputs_ref[gate, pl.ds(start, size), lanes]
                    )


def step_kernel(count, index, start, chunk, step, copies, *refs):
    refs = list(refs)
    far = [refs.pop(0) for _ in range(count // 2)]
    weight_ref, base_ref, inputs_ref, state_ref, init_ref = [refs.pop(0) for _ in range(5)]
    last = index == CHUNKS - 1
    next_ref, edge_ref = [refs.pop(0) for _ in range(2)] if last else (None, None)
    opens = index == 0 and step == 0
    before_ref = None if opens else refs.pop(0)
    diag_ref = None if opens else refs.pop(0)
    a_ref, b_ref, ends_ref = [refs.pop(0) for _ in range(3)]
    diag_ref = refs.pop(0) if opens else diag_ref
    begins = last and step == 0
    send_ref = refs.pop(0) if last else None
    lhs, *products = refs
    height = lhs.shape[0]
    rows, width = state_ref.shape
    lead = height - chunk
    hid = lax.axis_index("hid")
    is_first = lax.axis_index("tm") == 0
    is_last = lax.axis_index("tm") == lax.axis_size("tm") - 1
    groups = chunk // GROUP
    tiles = width // TILE

    if opens:
        diagonals(weight_ref, hid, diag_ref)
    own = hid % (count // 2)
    for offset in range(count // 2):
        lhs[:, pl.ds(pl.multiple_of((own ^ offset) * width, width), width)] = far[offset][...]
    first = ((hid - own) ^ (count // 2)) * width
    row = lax.broadcasted_iota(jnp.int32, (GROUP, TILE), 0)
    zeros = jnp.zeros((GROUP, TILE), F32)

    def dots(tile):
        for gate in range(3):
            products[tile][gate] = tile_dot(lhs, weight_ref, first, gate, pl.ds(tile * TILE, TILE))

    def cells(tile):
        lanes = pl.ds(tile * TILE, TILE)
        diag_z = diag_ref[pl.ds(0, GROUP), lanes]
        diag_r = diag_ref[pl.ds(GROUP, GROUP), lanes]
        diag_n = diag_ref[pl.ds(2 * GROUP, GROUP), lanes]
        squares = zeros
        if index == 0:
            run_a, run_b = jnp.ones((GROUP, TILE), F32), zeros
        else:
            run_a = jnp.broadcast_to(before_ref[0:1, lanes], (GROUP, TILE))
            run_b = jnp.broadcast_to(before_ref[1:2, lanes], (GROUP, TILE))
        turned = pltpu.roll(state_ref[pl.ds(start, GROUP), lanes], GROUP - 1, 0)
        for group in range(groups):
            here = pl.ds(group * GROUP, GROUP)
            token = pl.ds(start + group * GROUP, GROUP)
            prev = state_ref[token, lanes]
            if last and group == groups - 1:
                following = jnp.broadcast_to(next_ref[:, lanes], (GROUP, TILE))
            else:
                following = state_ref[pl.ds(start + (group + 1) * GROUP, GROUP), lanes]
            turned_next = pltpu.roll(following, GROUP - 1, 0)
            state = jnp.where(row == GROUP - 1, turned_next, turned)
            turned = turned_next
            place = lead + group * GROUP
            bases = [base_ref[gate, pl.ds(start + place, GROUP), lanes] for gate in range(3)]
            inputs = inputs_ref[2, token, lanes]
            if last and group == groups - 1:
                edges = [edge_ref[:, pl.ds((gate + 1) * width + tile * TILE, TILE)] for gate in range(3)]
                edges = [jnp.where(row == GROUP - 1, jnp.broadcast_to(line, (GROUP, TILE)), 0.0) for line in edges]
                bases = [bases[0] + edges[0], bases[1] + edges[1], bases[2]]
                inputs = inputs + edges[2]
            found = [products[tile][gate, pl.ds(place, GROUP), :] for gate in range(3)]
            zeta, reset, gated, cand, gap, value = gates(bases, found, inputs, prev)
            rest = 1.0 - zeta
            slope = zeta + gap * (zeta * rest) * diag_z
            slope = slope + rest * (1.0 - cand * cand) * (reset * diag_n + gated * (1.0 - reset) * diag_r)
            error = state - value
            if last and group == groups - 1:
                error = jnp.where((row == GROUP - 1) & is_last, 0.0, error)
            squares = squares + error * error
            a = slope
            b = value - slope * prev
            for distance in (1, 2, 4):
                keep = row >= distance
                a_up = jnp.where(keep, pltpu.roll(a, distance, 0), 1.0)
                b_up = jnp.where(keep, pltpu.roll(b, distance, 0), 0.0)
                b = a * b_up + b
                a = a * a_up
            a_ref[here, lanes] = a * run_a
            b_ref[here, lanes] = a * run_b + b
            last_a = jnp.broadcast_to(a[GROUP - 1 :], (GROUP, TILE))
            last_b = jnp.broadcast_to(b[GROUP - 1 :], (GROUP, TILE))
            run_a, run_b = last_a * run_a, last_a * run_b + last_b
        if begins:
            begin = gates(
                [base_ref[gate, pl.ds(start, GROUP), lanes] for gate in range(3)],
                [products[tile][gate, pl.ds(0, GROUP), :] for gate in range(3)],
                inputs_ref[2, pl.ds(rows, GROUP), lanes],
                jnp.broadcast_to(init_ref[:, lanes], (GROUP, TILE)),
            )[-1]
            error = state_ref[pl.ds(0, GROUP), lanes] - begin
            squares = squares + jnp.where((row == 0) & is_first, error * error, 0.0)
            begin = begin[0:1]
            earlier = zeros[0:1]
        elif step == 0:
            begin, earlier = zeros[0:1], zeros[0:1]
        else:
            begin = before_ref[3:4, lanes]
            earlier = before_ref[2:3, lanes] if index == 0 else before_ref[4:5, lanes]
        total = jnp.sum(squares, axis=0, keepdims=True)
        if index:
            total = total + before_ref[2:3, lanes]
        ends_ref[0:1, lanes] = run_a[0:1]
        ends_ref[1:2, lanes] = run_b[0:1]
        ends_ref[2:3, lanes] = total
        ends_ref[3:4, lanes] = begin
        ends_ref[4:5, lanes] = earlier
        if last:
            send_a = jnp.where(is_first, 0.0, run_a[0:1])
            send_b = jnp.where(is_first, run_a[0:1] * begin + run_b[0:1], run_b[0:1])
            for part in range(TILE // LANES):
                at = tile * (TILE // LANES) + part
                for line, sent in ((at, send_a), (width // LANES + at, send_b)):
                    picked = sent[:, part * LANES : (part + 1) * LANES]
                    send_ref[:, pl.ds(line, 1), :] = jnp.broadcast_to(picked[None], (copies, 1, LANES))

    dots(0)
    for tile in range(1, tiles):
        dots(tile)
        cells(tile - 1)
    cells(tiles - 1)
    if last and step == ITERS - 1:
        lane = lax.broadcasted_iota(jnp.int32, (1, LANES), 1)
        sums = jnp.zeros((1, LANES), F32)
        for line, half in ((4, 0), (2, 1)):
            part = sum(ends_ref[pl.ds(line, 1), pl.ds(at, LANES)] for at in range(0, width, LANES))
            part = part + pltpu.roll(part, LANES // 2, 1)
            sums = jnp.where(lane // (LANES // 2) == half, part, sums)
        send_ref[:, pl.ds(2 * width // LANES, 1), :] = jnp.broadcast_to(sums[None], (copies, 1, LANES))


def apply_kernel(step, *refs):
    final = step == ITERS - 1
    maps, refs = refs[: 2 * CHUNKS], refs[2 * CHUNKS :]
    begin_ref, all_ref, state_ref = refs[:3]
    outs = refs[3:]
    rows, width = state_ref.shape
    lines = width // LANES
    place = lax.axis_index("tm")
    peers = all_ref.shape[0]

    def compose(peer, enter):
        moved = all_ref[peer, pl.ds(0, lines), :] * enter + all_ref[peer, pl.ds(lines, lines), :]
        return jnp.where(peer < place, moved, enter)

    begin = jnp.concatenate([begin_ref[3:4, pl.ds(at * LANES, LANES)] for at in range(lines)], axis=0)
    found = lax.fori_loop(0, peers, compose, begin, unroll=min(peers, 8))
    enter = jnp.concatenate([found[at : at + 1] for at in range(lines)], axis=1)
    height = 2 * GROUP
    row = lax.broadcasted_iota(jnp.int32, (height, width), 0)
    enter = jnp.broadcast_to(enter, (height, width))
    before = enter
    held = spans(step, rows)
    sent = held if final else spans(step + 1, rows)
    cuts = sorted({at for at, _ in held + sent} | {rows})
    for low, high in zip(cuts, cuts[1:]):
        source = max(place for place, (at, _) in enumerate(held) if at <= low)
        target = max(place for place, (at, _) in enumerate(sent) if at <= low)
        a_ref, b_ref = maps[2 * source], maps[2 * source + 1]

        def advance(group, before):
            at = low + group * height
            here = pl.ds(pl.multiple_of(at - held[source][0], height), height)
            token = pl.ds(pl.multiple_of(at, height), height)
            turned = pltpu.roll(a_ref[here, :] * enter + b_ref[here, :], 1, 0)
            moved = jnp.where(row == 0, before, turned)
            state_ref[token, :] = moved
            if not final:
                rounded = moved.astype(BF16)
                outs[1][token, :] = rounded
                outs[2 + target][pl.ds(pl.multiple_of(at - sent[target][0], height), height), :] = rounded
            return turned

        before = lax.fori_loop(0, (high - low) // height, advance, before, unroll=2)
    if not final:
        outs[0][...] = before[0:1]


def sums_kernel(all_ref, out_ref):
    out_ref[...] = jnp.sum(all_ref[:, pl.ds(all_ref.shape[1] - 1, 1), :], axis=0)


def norm_kernel(size, *refs):
    *parts, out_ref = refs
    total = sum(part[...] for part in parts)
    lane = lax.broadcasted_iota(jnp.int32, (1, LANES), 1)
    for half in range(ITERS):
        out_ref[half] = jnp.sqrt(jnp.sum(jnp.where(lane // (LANES // 2) == half, total, 0.0)) / size)


def newton(token_ids, input_table, recur_weight, z_bias, hn_bias, init_state, guess):
    rows, width = guess.shape
    full = recur_weight.shape[0]
    count = lax.axis_size("hid")
    blocks_tm = lax.axis_size("tm")
    weight = jnp.transpose(recur_weight, (1, 0, 2))
    table = jnp.transpose(input_table, (1, 0, 2))
    lines = width // LANES

    first = spans(0, rows)[0][1]
    rounded, rest = lax.optimization_barrier((guess.astype(BF16), guess))
    opening = rounded[:first]
    whole, *moved = pl.pallas_call(
        merge_kernel,
        out_shape=[jax.ShapeDtypeStruct((rows + EXTRA, width), BF16)]
        + [
            jax.ShapeDtypeStruct((height + EXTRA * (at + height == rows), width), BF16)
            for at, height in spans(0, rows)[1:]
        ],
        in_specs=vmem(2),
        out_specs=vmem(CHUNKS),
        compiler_params=params(8),
        cost_estimate=cost(COVER, 8 * rows * width),
        name="merge",
    )(rounded, init_state[None])
    moved = [opening, *moved]
    inputs, line = pl.pallas_call(
        prepare_kernel,
        out_shape=[
            jax.ShapeDtypeStruct((3, rows + GROUP, width), F32),
            jax.ShapeDtypeStruct((1, 4 * width), F32),
        ],
        in_specs=vmem(4),
        out_specs=vmem(2),
        compiler_params=params(32),
        cost_estimate=cost(2 * COVER, 8 * rows * width),
        name="prepare",
    )(token_ids[None], rest, table, z_bias[None])
    edge = from_next(line, "tm")
    state, following = rest, edge

    ends, diag = None, None
    for step in range(ITERS):
        final = step == ITERS - 1
        near = {0: whole}
        far = [{count // 2: None} for _ in range(CHUNKS)]
        for index in range(CHUNKS):
            far[index][count // 2] = swapped(moved[index], "hid", count // 2)
        bit = count // 4
        while bit:
            for offset in list(near):
                near[offset | bit] = swapped(near[offset], "hid", bit)
            for index in range(CHUNKS):
                for offset in list(far[index]):
                    far[index][offset | bit] = swapped(far[index][offset], "hid", bit)
            bit //= 2
        height = whole.shape[0]
        base = pl.pallas_call(
            functools.partial(base_kernel, step, count),
            out_shape=jax.ShapeDtypeStruct((3, height, width), F32),
            in_specs=vmem(count // 2 + 3),
            out_specs=vmem(1)[0],
            scratch_shapes=[pltpu.VMEM((height, full // 2), BF16)],
            compiler_params=params(16),
            cost_estimate=cost(3 * height * full * width, 3 * full * width),
        )(*[near[offset] for offset in range(count // 2)], weight, inputs, hn_bias[None])
        maps = []
        for index, (start, chunk) in enumerate(spans(step, rows)):
            last = index == CHUNKS - 1
            height = moved[index].shape[0]
            operands = [far[index][offset] for offset in range(count // 2, count)]
            operands += [weight, base, inputs, state, init_state[None]]
            if last:
                operands += [following, edge]
            if diag is not None:
                operands += [ends, diag]
            outs = [
                jax.ShapeDtypeStruct((chunk, width), F32),
                jax.ShapeDtypeStruct((chunk, width), F32),
                jax.ShapeDtypeStruct((5, width), F32),
            ]
            if diag is None:
                outs.append(jax.ShapeDtypeStruct((3 * GROUP, width), F32))
            copies = blocks_tm
            if last:
                outs.append(jax.ShapeDtypeStruct((copies, 2 * lines + final, LANES), F32))
            found = pl.pallas_call(
                functools.partial(step_kernel, count, index, start, chunk, step, copies),
                out_shape=outs,
                in_specs=vmem(len(operands)),
                out_specs=vmem(len(outs)),
                scratch_shapes=[pltpu.VMEM((height, full // 2), BF16)]
                + [pltpu.VMEM((3, height, TILE), F32)] * (width // TILE),
                compiler_params=params(32),
                cost_estimate=cost(height * full * 3 * width, 3 * full * width),
            )(*operands)
            maps += found[:2]
            ends = found[2]
            diag = found[3] if diag is None else diag
        every = lax.all_to_all(found[-1], "tm", 0, 0)
        outs = [jax.ShapeDtypeStruct((rows, width), F32)]
        if final:
            part = pl.pallas_call(
                sums_kernel,
                out_shape=jax.ShapeDtypeStruct((1, LANES), F32),
                in_specs=vmem(1),
                out_specs=vmem(1)[0],
                compiler_params=params(8),
                name="sums",
            )(every)
            parts = [part]
            for offset in range(1, count):
                parts.append(swapped(part, "hid", offset))
        else:
            outs.append(jax.ShapeDtypeStruct((1, width), F32))
            outs.append(jax.ShapeDtypeStruct((rows, width), BF16))
            outs += [jax.ShapeDtypeStruct((chunk, width), BF16) for _, chunk in spans(step + 1, rows)]
        result = pl.pallas_call(
            functools.partial(apply_kernel, step),
            out_shape=outs,
            in_specs=vmem(2 * CHUNKS + 2),
            out_specs=vmem(len(outs)),
            compiler_params=params(16),
            cost_estimate=cost(2 * rows * width, 16 * rows * width),
        )(*maps, ends, every)
        if final:
            residual_norm = pl.pallas_call(
                functools.partial(norm_kernel, blocks_tm * count * rows * width),
                out_shape=jax.ShapeDtypeStruct((ITERS,), F32),
                in_specs=vmem(count),
                out_specs=smem()[0],
                compiler_params=params(8),
                name="norm",
            )(*parts)
            return (result[0], residual_norm)
        state, following, whole, *moved = result


def solution(mesh):
    return jax.shard_map(
        newton,
        mesh=mesh,
        in_specs=(
            P("tm"),
            P(None, None, "hid"),
            P(None, None, "hid"),
            P("hid"),
            P("hid"),
            P("hid"),
            P("tm", "hid"),
        ),
        out_specs=(P("tm", "hid"), P()),
        check_vma=False,
    )
```

```python
import functools

import jax
import jax.numpy as jnp
from jax import lax
from jax.experimental import pallas as pl
from jax.experimental.pallas import tpu as pltpu
from jax.sharding import PartitionSpec as P


ITERS = 2
SHARES = ((10, 6), (10, 6))
CHUNKS = len(SHARES[0])
GROUP = 8
EXTRA = 8
SPLIT = ((1, 1), (1, 1))
TILE = 256
LANES = 128
COVER = 2_000_000_000
F32 = jnp.float32
BF16 = jnp.bfloat16


def swapped(block, axis, bit):
    route = [(i, i ^ bit) for i in range(lax.axis_size(axis))]
    return lax.ppermute(block, axis, route)


def from_next(block, axis):
    route = [(i + 1, i) for i in range(lax.axis_size(axis) - 1)]
    return lax.ppermute(block, axis, route)


def sigmoid(x):
    return 0.5 * jnp.tanh(0.5 * x) + 0.5


def splits(step, index, count):
    return SPLIT[step][index] if count == 4 else 0


def spans(step, rows):
    unit = rows // sum(SHARES[step])
    found, at = [], 0
    for share in SHARES[step]:
        found.append((at, share * unit))
        at += share * unit
    return found


def vmem(count):
    return [pl.BlockSpec(memory_space=pltpu.VMEM)] * count


def smem():
    return [pl.BlockSpec(memory_space=pltpu.SMEM)]


def params(mib):
    return pltpu.CompilerParams(vmem_limit_bytes=mib * 1024 * 1024)


def cost(flops, moved):
    return pl.CostEstimate(flops=flops, bytes_accessed=moved, transcendentals=0)


def merge_kernel(rounded_ref, init_ref, whole_ref, *parts):
    rows, width = rounded_ref.shape
    opening = spans(0, rows)[0][1]
    whole_ref[pl.ds(0, opening), :] = rounded_ref[pl.ds(0, opening), :]
    for (at, chunk), part in zip(spans(0, rows)[1:], parts):
        lead = part.shape[0] - chunk
        if lead:
            row = lax.broadcasted_iota(jnp.int32, (lead, width), 0)
            head = jnp.where(row == 0, jnp.broadcast_to(init_ref[...], (lead, width)), 0.0).astype(BF16)
            part[pl.ds(0, lead), :] = head
            whole_ref[pl.ds(at, lead), :] = head
        block = rounded_ref[pl.ds(at, chunk), :]
        part[pl.ds(lead, chunk), :] = block
        whole_ref[pl.ds(at + lead, chunk), :] = block


def prepare_kernel(ids_ref, guess_ref, table_ref, bias_ref, out_ref, line_ref):
    vocab, width = table_ref.shape[1:]
    rows = ids_ref.shape[1]
    ids = ids_ref[...]

    def spread(line):
        entry = lax.broadcasted_iota(jnp.int32, (vocab, line.shape[1]), 0)
        return (entry == line).astype(F32).astype(BF16)

    def pick(hot, part):
        return lax.dot_general(hot, part, (((0,), (0,)), ((), ())), preferred_element_type=F32)

    lane = lax.broadcasted_iota(jnp.int32, (1, rows), 1)
    hot = spread(jnp.where(lane == rows - 1, vocab, pltpu.roll(ids, rows - 1, 1)))
    hot_begin = spread(jnp.broadcast_to(ids[:, 0:1], (1, LANES)))
    line_ref[:, pl.ds(0, width)] = guess_ref[0:1, :]
    for gate in range(3):
        table = table_ref[gate]
        if gate == 0:
            table = table + bias_ref[...]
        total = None
        for _ in range(3):
            part = table.astype(BF16)
            table = table - part.astype(F32)
            picked = (pick(hot, part), pick(hot_begin, part))
            total = picked if total is None else (total[0] + picked[0], total[1] + picked[1])
        out_ref[gate, pl.ds(0, rows), :] = total[0]
        out_ref[gate, pl.ds(rows, GROUP), :] = total[1][0:GROUP]
        line_ref[:, pl.ds((gate + 1) * width, width)] = total[1][0:1]


def diagonals(weight_ref, hid, diag_ref):
    width = diag_ref.shape[1]
    row = lax.broadcasted_iota(jnp.int32, (width, width), 0)
    col = lax.broadcasted_iota(jnp.int32, (width, width), 1)
    first = pl.multiple_of(hid * width, width)
    for gate in range(3):
        block = weight_ref[gate, pl.ds(first, width), :].astype(F32)
        line = jnp.sum(jnp.where(row == col, block, 0.0), axis=0, keepdims=True)
        diag_ref[pl.ds(gate * GROUP, GROUP), :] = jnp.broadcast_to(line, (GROUP, width))


def gates(bases, products, inputs, prev):
    zeta = sigmoid(bases[0] + products[0])
    reset = sigmoid(bases[1] + products[1])
    gated = reset * (bases[2] + products[2])
    cand = jnp.tanh(inputs + gated)
    gap = prev - cand
    return zeta, reset, gated, cand, gap, cand + zeta * gap


def tile_dot(lhs, weight_ref, first, gate, lanes):
    depth = lhs.shape[1]
    pieces = 2 if gate == 2 else 1
    total = None
    for piece in range(pieces):
        at = pl.multiple_of(first + piece * (depth // pieces), depth // pieces)
        term = jnp.dot(
            lhs[:, pl.ds(piece * (depth // pieces), depth // pieces)],
            weight_ref[gate, pl.ds(at, depth // pieces), lanes],
            preferred_element_type=F32,
        )
        total = term if total is None else total + term
    return total


def base_kernel(step, count, *refs):
    near, (weight_ref, inputs_ref, bias_ref, base_ref, lhs) = refs[: count // 2], refs[count // 2 :]
    height, _ = lhs.shape
    width = base_ref.shape[2]
    rows = inputs_ref.shape[1] - GROUP
    hid = lax.axis_index("hid")
    own = hid % (count // 2)
    for offset in range(count // 2):
        lhs[:, pl.ds(pl.multiple_of((own ^ offset) * width, width), width)] = near[offset][...]
    pieces, at = [], 0
    for start, chunk in spans(step, rows):
        if start + chunk == rows and height > rows:
            pieces.append((at, rows, GROUP))
            at += EXTRA
        pieces.append((at, start, chunk))
        at += chunk
    for tile in range(width // TILE):
        lanes = pl.ds(tile * TILE, TILE)
        for gate in range(3):
            found = tile_dot(lhs, weight_ref, (hid - own) * width, gate, lanes)
            if gate == 2:
                base_ref[gate, :, lanes] = found + bias_ref[:, lanes]
            else:
                for at, start, size in pieces:
                    base_ref[gate, pl.ds(at, size), lanes] = (
                        found[at : at + size] + inputs_ref[gate, pl.ds(start, size), lanes]
                    )


def direct_kernel(start, count, far_ref, weight_ref, base_ref, out_ref):
    height, width = far_ref.shape
    first = (lax.axis_index("hid") ^ (count // 2)) * width
    for tile in range(width // TILE):
        lanes = pl.ds(tile * TILE, TILE)
        for gate in range(3):
            found = tile_dot(far_ref, weight_ref, first, gate, lanes)
            out_ref[gate, :, lanes] = base_ref[gate, pl.ds(start, height), lanes] + found


def step_kernel(count, index, start, chunk, step, copies, *refs):
    refs = list(refs)
    split = splits(step, index, count)
    far = [refs.pop(0) for _ in range(split, count // 2)]
    weight_ref, base_ref, inputs_ref, state_ref, init_ref = [refs.pop(0) for _ in range(5)]
    last = index == CHUNKS - 1
    next_ref, edge_ref = [refs.pop(0) for _ in range(2)] if last else (None, None)
    opens = index == 0 and step == 0
    before_ref = None if opens else refs.pop(0)
    diag_ref = None if opens else refs.pop(0)
    a_ref, b_ref, ends_ref = [refs.pop(0) for _ in range(3)]
    diag_ref = refs.pop(0) if opens else diag_ref
    begins = last and step == 0
    send_ref = refs.pop(0) if last else None
    lhs, *products = refs
    height = products[0].shape[1]
    rows, width = state_ref.shape
    lead = height - chunk
    hid = lax.axis_index("hid")
    is_first = lax.axis_index("tm") == 0
    is_last = lax.axis_index("tm") == lax.axis_size("tm") - 1
    groups = chunk // GROUP
    tiles = width // TILE

    if opens:
        diagonals(weight_ref, hid, diag_ref)
    own = hid % (count // 2)
    if split:
        lhs = far[0]
        first = (hid ^ (count // 2) ^ 1) * width
        begin_row = 0
    else:
        for offset in range(count // 2):
            lhs[:, pl.ds(pl.multiple_of((own ^ offset) * width, width), width)] = far[offset][...]
        first = ((hid - own) ^ (count // 2)) * width
        begin_row = start
    row = lax.broadcasted_iota(jnp.int32, (GROUP, TILE), 0)
    zeros = jnp.zeros((GROUP, TILE), F32)

    def dots(tile):
        for gate in range(3):
            products[tile][gate] = tile_dot(lhs, weight_ref, first, gate, pl.ds(tile * TILE, TILE))

    def cells(tile):
        lanes = pl.ds(tile * TILE, TILE)
        diag_z = diag_ref[pl.ds(0, GROUP), lanes]
        diag_r = diag_ref[pl.ds(GROUP, GROUP), lanes]
        diag_n = diag_ref[pl.ds(2 * GROUP, GROUP), lanes]
        squares = zeros
        if index == 0:
            run_a, run_b = jnp.ones((GROUP, TILE), F32), zeros
        else:
            run_a = jnp.broadcast_to(before_ref[0:1, lanes], (GROUP, TILE))
            run_b = jnp.broadcast_to(before_ref[1:2, lanes], (GROUP, TILE))
        turned = pltpu.roll(state_ref[pl.ds(start, GROUP), lanes], GROUP - 1, 0)
        for group in range(groups):
            here = pl.ds(group * GROUP, GROUP)
            token = pl.ds(start + group * GROUP, GROUP)
            prev = state_ref[token, lanes]
            if last and group == groups - 1:
                following = jnp.broadcast_to(next_ref[:, lanes], (GROUP, TILE))
            else:
                following = state_ref[pl.ds(start + (group + 1) * GROUP, GROUP), lanes]
            turned_next = pltpu.roll(following, GROUP - 1, 0)
            state = jnp.where(row == GROUP - 1, turned_next, turned)
            turned = turned_next
            place = lead + group * GROUP
            bases = [base_ref[gate, pl.ds(begin_row + place, GROUP), lanes] for gate in range(3)]
            inputs = inputs_ref[2, token, lanes]
            if last and group == groups - 1:
                edges = [edge_ref[:, pl.ds((gate + 1) * width + tile * TILE, TILE)] for gate in range(3)]
                edges = [jnp.where(row == GROUP - 1, jnp.broadcast_to(line, (GROUP, TILE)), 0.0) for line in edges]
                bases = [bases[0] + edges[0], bases[1] + edges[1], bases[2]]
                inputs = inputs + edges[2]
            found = [products[tile][gate, pl.ds(place, GROUP), :] for gate in range(3)]
            zeta, reset, gated, cand, gap, value = gates(bases, found, inputs, prev)
            rest = 1.0 - zeta
            slope = zeta + gap * (zeta * rest) * diag_z
            slope = slope + rest * (1.0 - cand * cand) * (reset * diag_n + gated * (1.0 - reset) * diag_r)
            error = state - value
            if last and group == groups - 1:
                error = jnp.where((row == GROUP - 1) & is_last, 0.0, error)
            squares = squares + error * error
            a = slope
            b = value - slope * prev
            for distance in (1, 2, 4):
                keep = row >= distance
                a_up = jnp.where(keep, pltpu.roll(a, distance, 0), 1.0)
                b_up = jnp.where(keep, pltpu.roll(b, distance, 0), 0.0)
                b = a * b_up + b
                a = a * a_up
            a_ref[here, lanes] = a * run_a
            b_ref[here, lanes] = a * run_b + b
            last_a = jnp.broadcast_to(a[GROUP - 1 :], (GROUP, TILE))
            last_b = jnp.broadcast_to(b[GROUP - 1 :], (GROUP, TILE))
            run_a, run_b = last_a * run_a, last_a * run_b + last_b
        if begins:
            begin = gates(
                [base_ref[gate, pl.ds(begin_row, GROUP), lanes] for gate in range(3)],
                [products[tile][gate, pl.ds(0, GROUP), :] for gate in range(3)],
                inputs_ref[2, pl.ds(rows, GROUP), lanes],
                jnp.broadcast_to(init_ref[:, lanes], (GROUP, TILE)),
            )[-1]
            error = state_ref[pl.ds(0, GROUP), lanes] - begin
            squares = squares + jnp.where((row == 0) & is_first, error * error, 0.0)
            begin = begin[0:1]
            earlier = zeros[0:1]
        elif step == 0:
            begin, earlier = zeros[0:1], zeros[0:1]
        else:
            begin = before_ref[3:4, lanes]
            earlier = before_ref[2:3, lanes] if index == 0 else before_ref[4:5, lanes]
        total = jnp.sum(squares, axis=0, keepdims=True)
        if index:
            total = total + before_ref[2:3, lanes]
        ends_ref[0:1, lanes] = run_a[0:1]
        ends_ref[1:2, lanes] = run_b[0:1]
        ends_ref[2:3, lanes] = total
        ends_ref[3:4, lanes] = begin
        ends_ref[4:5, lanes] = earlier
        if last:
            send_a = jnp.where(is_first, 0.0, run_a[0:1])
            send_b = jnp.where(is_first, run_a[0:1] * begin + run_b[0:1], run_b[0:1])
            for part in range(TILE // LANES):
                at = tile * (TILE // LANES) + part
                for line, sent in ((at, send_a), (width // LANES + at, send_b)):
                    picked = sent[:, part * LANES : (part + 1) * LANES]
                    send_ref[:, pl.ds(line, 1), :] = jnp.broadcast_to(picked[None], (copies, 1, LANES))

    dots(0)
    for tile in range(1, tiles):
        dots(tile)
        cells(tile - 1)
    cells(tiles - 1)
    if last and step == ITERS - 1:
        lane = lax.broadcasted_iota(jnp.int32, (1, LANES), 1)
        sums = jnp.zeros((1, LANES), F32)
        for line, half in ((4, 0), (2, 1)):
            part = sum(ends_ref[pl.ds(line, 1), pl.ds(at, LANES)] for at in range(0, width, LANES))
            part = part + pltpu.roll(part, LANES // 2, 1)
            sums = jnp.where(lane // (LANES // 2) == half, part, sums)
        send_ref[:, pl.ds(2 * width // LANES, 1), :] = jnp.broadcast_to(sums[None], (copies, 1, LANES))


def apply_kernel(step, *refs):
    final = step == ITERS - 1
    maps, refs = refs[: 2 * CHUNKS], refs[2 * CHUNKS :]
    begin_ref, all_ref, state_ref = refs[:3]
    outs = refs[3:]
    rows, width = state_ref.shape
    lines = width // LANES
    place = lax.axis_index("tm")
    peers = all_ref.shape[0]

    def compose(peer, enter):
        moved = all_ref[peer, pl.ds(0, lines), :] * enter + all_ref[peer, pl.ds(lines, lines), :]
        return jnp.where(peer < place, moved, enter)

    begin = jnp.concatenate([begin_ref[3:4, pl.ds(at * LANES, LANES)] for at in range(lines)], axis=0)
    found = lax.fori_loop(0, peers, compose, begin, unroll=min(peers, 8))
    enter = jnp.concatenate([found[at : at + 1] for at in range(lines)], axis=1)
    height = 2 * GROUP
    row = lax.broadcasted_iota(jnp.int32, (height, width), 0)
    enter = jnp.broadcast_to(enter, (height, width))
    before = enter
    held = spans(step, rows)
    sent = held if final else spans(step + 1, rows)
    cuts = sorted({at for at, _ in held + sent} | {rows})
    for low, high in zip(cuts, cuts[1:]):
        source = max(place for place, (at, _) in enumerate(held) if at <= low)
        target = max(place for place, (at, _) in enumerate(sent) if at <= low)
        a_ref, b_ref = maps[2 * source], maps[2 * source + 1]

        def advance(group, before):
            at = low + group * height
            here = pl.ds(pl.multiple_of(at - held[source][0], height), height)
            token = pl.ds(pl.multiple_of(at, height), height)
            turned = pltpu.roll(a_ref[here, :] * enter + b_ref[here, :], 1, 0)
            moved = jnp.where(row == 0, before, turned)
            state_ref[token, :] = moved
            if not final:
                rounded = moved.astype(BF16)
                outs[1][token, :] = rounded
                outs[2 + target][pl.ds(pl.multiple_of(at - sent[target][0], height), height), :] = rounded
            return turned

        before = lax.fori_loop(0, (high - low) // height, advance, before, unroll=2)
    if not final:
        outs[0][...] = before[0:1]


def sums_kernel(all_ref, out_ref):
    out_ref[...] = jnp.sum(all_ref[:, pl.ds(all_ref.shape[1] - 1, 1), :], axis=0)


def norm_kernel(size, *refs):
    *parts, out_ref = refs
    total = sum(part[...] for part in parts)
    lane = lax.broadcasted_iota(jnp.int32, (1, LANES), 1)
    for half in range(ITERS):
        out_ref[half] = jnp.sqrt(jnp.sum(jnp.where(lane // (LANES // 2) == half, total, 0.0)) / size)


def newton(token_ids, input_table, recur_weight, z_bias, hn_bias, init_state, guess):
    rows, width = guess.shape
    full = recur_weight.shape[0]
    count = lax.axis_size("hid")
    blocks_tm = lax.axis_size("tm")
    weight = jnp.transpose(recur_weight, (1, 0, 2))
    table = jnp.transpose(input_table, (1, 0, 2))
    lines = width // LANES

    first = spans(0, rows)[0][1]
    rounded, rest = lax.optimization_barrier((guess.astype(BF16), guess))
    opening = rounded[:first]
    whole, *moved = pl.pallas_call(
        merge_kernel,
        out_shape=[jax.ShapeDtypeStruct((rows + EXTRA, width), BF16)]
        + [
            jax.ShapeDtypeStruct((height + EXTRA * (at + height == rows), width), BF16)
            for at, height in spans(0, rows)[1:]
        ],
        in_specs=vmem(2),
        out_specs=vmem(CHUNKS),
        compiler_params=params(8),
        cost_estimate=cost(COVER, 8 * rows * width),
        name="merge",
    )(rounded, init_state[None])
    moved = [opening, *moved]
    inputs, line = pl.pallas_call(
        prepare_kernel,
        out_shape=[
            jax.ShapeDtypeStruct((3, rows + GROUP, width), F32),
            jax.ShapeDtypeStruct((1, 4 * width), F32),
        ],
        in_specs=vmem(4),
        out_specs=vmem(2),
        compiler_params=params(32),
        cost_estimate=cost(2 * COVER, 8 * rows * width),
        name="prepare",
    )(token_ids[None], rest, table, z_bias[None])
    edge = from_next(line, "tm")
    state, following = rest, edge

    ends, diag = None, None
    for step in range(ITERS):
        final = step == ITERS - 1
        near = {0: whole}
        far = [{count // 2: None} for _ in range(CHUNKS)]
        for index in range(CHUNKS):
            far[index][count // 2] = swapped(moved[index], "hid", count // 2)
        bit = count // 4
        while bit:
            for offset in list(near):
                near[offset | bit] = swapped(near[offset], "hid", bit)
            for index in range(CHUNKS):
                for offset in list(far[index]):
                    far[index][offset | bit] = swapped(far[index][offset], "hid", bit)
            bit //= 2
        height = whole.shape[0]
        base = pl.pallas_call(
            functools.partial(base_kernel, step, count),
            out_shape=jax.ShapeDtypeStruct((3, height, width), F32),
            in_specs=vmem(count // 2 + 3),
            out_specs=vmem(1)[0],
            scratch_shapes=[pltpu.VMEM((height, full // 2), BF16)],
            compiler_params=params(16),
            cost_estimate=cost(3 * height * full * width, 3 * full * width),
        )(*[near[offset] for offset in range(count // 2)], weight, inputs, hn_bias[None])
        maps = []
        for index, (start, chunk) in enumerate(spans(step, rows)):
            last = index == CHUNKS - 1
            height = moved[index].shape[0]
            split = splits(step, index, count)
            sums = base
            if split:
                sums = pl.pallas_call(
                    functools.partial(direct_kernel, start, count),
                    out_shape=jax.ShapeDtypeStruct((3, height, width), F32),
                    in_specs=vmem(3),
                    out_specs=vmem(1)[0],
                    compiler_params=params(16),
                    cost_estimate=cost(3 * height * full * width // 2, 3 * full * width),
                )(far[index][count // 2], weight, base)
            operands = [far[index][offset] for offset in range(count // 2 + split, count)]
            operands += [weight, sums, inputs, state, init_state[None]]
            if last:
                operands += [following, edge]
            if diag is not None:
                operands += [ends, diag]
            outs = [
                jax.ShapeDtypeStruct((chunk, width), F32),
                jax.ShapeDtypeStruct((chunk, width), F32),
                jax.ShapeDtypeStruct((5, width), F32),
            ]
            if diag is None:
                outs.append(jax.ShapeDtypeStruct((3 * GROUP, width), F32))
            copies = blocks_tm
            if last:
                outs.append(jax.ShapeDtypeStruct((copies, 2 * lines + final, LANES), F32))
            found = pl.pallas_call(
                functools.partial(step_kernel, count, index, start, chunk, step, copies),
                out_shape=outs,
                in_specs=vmem(len(operands)),
                out_specs=vmem(len(outs)),
                scratch_shapes=[pltpu.VMEM((height, full // 2), BF16)]
                + [pltpu.VMEM((3, height, TILE), F32)] * (width // TILE),
                compiler_params=params(32),
                cost_estimate=cost(height * full * 3 * width, 3 * full * width),
            )(*operands)
            maps += found[:2]
            ends = found[2]
            diag = found[3] if diag is None else diag
        every = lax.all_to_all(found[-1], "tm", 0, 0)
        outs = [jax.ShapeDtypeStruct((rows, width), F32)]
        if final:
            part = pl.pallas_call(
                sums_kernel,
                out_shape=jax.ShapeDtypeStruct((1, LANES), F32),
                in_specs=vmem(1),
                out_specs=vmem(1)[0],
                compiler_params=params(8),
                name="sums",
            )(every)
            parts = [part]
            for offset in range(1, count):
                parts.append(swapped(part, "hid", offset))
        else:
            outs.append(jax.ShapeDtypeStruct((1, width), F32))
            outs.append(jax.ShapeDtypeStruct((rows, width), BF16))
            outs += [jax.ShapeDtypeStruct((chunk, width), BF16) for _, chunk in spans(step + 1, rows)]
        result = pl.pallas_call(
            functools.partial(apply_kernel, step),
            out_shape=outs,
            in_specs=vmem(2 * CHUNKS + 2),
            out_specs=vmem(len(outs)),
            compiler_params=params(16),
            cost_estimate=cost(2 * rows * width, 16 * rows * width),
        )(*maps, ends, every)
        if final:
            residual_norm = pl.pallas_call(
                functools.partial(norm_kernel, blocks_tm * count * rows * width),
                out_shape=jax.ShapeDtypeStruct((ITERS,), F32),
                in_specs=vmem(count),
                out_specs=smem()[0],
                compiler_params=params(8),
                name="norm",
            )(*parts)
            return (result[0], residual_norm)
        state, following, whole, *moved = result


def solution(mesh):
    return jax.shard_map(
        newton,
        mesh=mesh,
        in_specs=(
            P("tm"),
            P(None, None, "hid"),
            P(None, None, "hid"),
            P("hid"),
            P("hid"),
            P("hid"),
            P("tm", "hid"),
        ),
        out_specs=(P("tm", "hid"), P()),
        check_vma=False,
    )
```

```python
import functools

import jax
import jax.numpy as jnp
from jax import lax
from jax.experimental import pallas as pl
from jax.experimental.pallas import tpu as pltpu
from jax.sharding import PartitionSpec as P


ITERS = 2
SHARES = ((10, 6), (19, 13))
CHUNKS = len(SHARES[0])
GROUP = 8
EXTRA = 8
SPLIT = ((1, 1), (1, 1))
TILE = 256
LANES = 128
COVER = 2_000_000_000
F32 = jnp.float32
BF16 = jnp.bfloat16


def swapped(block, axis, bit):
    route = [(i, i ^ bit) for i in range(lax.axis_size(axis))]
    return lax.ppermute(block, axis, route)


def from_next(block, axis):
    route = [(i + 1, i) for i in range(lax.axis_size(axis) - 1)]
    return lax.ppermute(block, axis, route)


def sigmoid(x):
    return 0.5 * jnp.tanh(0.5 * x) + 0.5


def splits(step, index, count):
    return SPLIT[step][index] if count == 4 else 0


def spans(step, rows):
    unit = rows // sum(SHARES[step])
    found, at = [], 0
    for share in SHARES[step]:
        found.append((at, share * unit))
        at += share * unit
    return found


def vmem(count):
    return [pl.BlockSpec(memory_space=pltpu.VMEM)] * count


def smem():
    return [pl.BlockSpec(memory_space=pltpu.SMEM)]


def params(mib):
    return pltpu.CompilerParams(vmem_limit_bytes=mib * 1024 * 1024)


def cost(flops, moved):
    return pl.CostEstimate(flops=flops, bytes_accessed=moved, transcendentals=0)


def merge_kernel(rounded_ref, init_ref, whole_ref, *parts):
    rows, width = rounded_ref.shape
    opening = spans(0, rows)[0][1]
    whole_ref[pl.ds(0, opening), :] = rounded_ref[pl.ds(0, opening), :]
    for (at, chunk), part in zip(spans(0, rows)[1:], parts):
        lead = part.shape[0] - chunk
        if lead:
            row = lax.broadcasted_iota(jnp.int32, (lead, width), 0)
            head = jnp.where(row == 0, jnp.broadcast_to(init_ref[...], (lead, width)), 0.0).astype(BF16)
            part[pl.ds(0, lead), :] = head
            whole_ref[pl.ds(at, lead), :] = head
        block = rounded_ref[pl.ds(at, chunk), :]
        part[pl.ds(lead, chunk), :] = block
        whole_ref[pl.ds(at + lead, chunk), :] = block


def prepare_kernel(ids_ref, guess_ref, table_ref, bias_ref, out_ref, line_ref):
    vocab, width = table_ref.shape[1:]
    rows = ids_ref.shape[1]
    entry = lax.broadcasted_iota(jnp.int32, (vocab, rows), 0)
    hot = (entry == pltpu.roll(ids_ref[...], rows - 1, 1)).astype(F32).astype(BF16)
    row = lax.broadcasted_iota(jnp.int32, (GROUP, width), 0)
    line_ref[:, pl.ds(0, width)] = guess_ref[0:1, :]
    for gate in range(3):
        table = table_ref[gate]
        if gate == 0:
            table = table + bias_ref[...]
        total = None
        for _ in range(3):
            part = table.astype(BF16)
            table = table - part.astype(F32)
            picked = lax.dot_general(hot, part, (((0,), (0,)), ((), ())), preferred_element_type=F32)
            total = picked if total is None else total + picked
        ending = total[rows - GROUP :]
        begin = ending[GROUP - 1 :]
        out_ref[gate, pl.ds(0, rows - GROUP), :] = total[: rows - GROUP]
        out_ref[gate, pl.ds(rows - GROUP, GROUP), :] = jnp.where(row == GROUP - 1, 0.0, ending)
        out_ref[gate, pl.ds(rows, GROUP), :] = jnp.broadcast_to(begin, (GROUP, width))
        line_ref[:, pl.ds((gate + 1) * width, width)] = begin


def diagonals(weight_ref, hid, diag_ref):
    width = diag_ref.shape[1]
    row = lax.broadcasted_iota(jnp.int32, (width, width), 0)
    col = lax.broadcasted_iota(jnp.int32, (width, width), 1)
    first = pl.multiple_of(hid * width, width)
    for gate in range(3):
        block = weight_ref[gate, pl.ds(first, width), :].astype(F32)
        line = jnp.sum(jnp.where(row == col, block, 0.0), axis=0, keepdims=True)
        diag_ref[pl.ds(gate * GROUP, GROUP), :] = jnp.broadcast_to(line, (GROUP, width))


def gates(bases, products, inputs, prev):
    zeta = sigmoid(bases[0] + products[0])
    reset = sigmoid(bases[1] + products[1])
    gated = reset * (bases[2] + products[2])
    cand = jnp.tanh(inputs + gated)
    gap = prev - cand
    return zeta, reset, gated, cand, gap, cand + zeta * gap


def tile_dot(lhs, weight_ref, first, gate, lanes):
    depth = lhs.shape[1]
    pieces = 2 if gate == 2 else 1
    total = None
    for piece in range(pieces):
        at = pl.multiple_of(first + piece * (depth // pieces), depth // pieces)
        term = jnp.dot(
            lhs[:, pl.ds(piece * (depth // pieces), depth // pieces)],
            weight_ref[gate, pl.ds(at, depth // pieces), lanes],
            preferred_element_type=F32,
        )
        total = term if total is None else total + term
    return total


def base_kernel(step, count, *refs):
    near, (weight_ref, inputs_ref, bias_ref, base_ref, lhs) = refs[: count // 2], refs[count // 2 :]
    height, _ = lhs.shape
    width = base_ref.shape[2]
    rows = inputs_ref.shape[1] - GROUP
    hid = lax.axis_index("hid")
    own = hid % (count // 2)
    for offset in range(count // 2):
        lhs[:, pl.ds(pl.multiple_of((own ^ offset) * width, width), width)] = near[offset][...]
    pieces, at = [], 0
    for start, chunk in spans(step, rows):
        if start + chunk == rows and height > rows:
            pieces.append((at, rows, GROUP))
            at += EXTRA
        pieces.append((at, start, chunk))
        at += chunk
    for tile in range(width // TILE):
        lanes = pl.ds(tile * TILE, TILE)
        for gate in range(3):
            found = tile_dot(lhs, weight_ref, (hid - own) * width, gate, lanes)
            if gate == 2:
                base_ref[gate, :, lanes] = found + bias_ref[:, lanes]
            else:
                for at, start, size in pieces:
                    base_ref[gate, pl.ds(at, size), lanes] = (
                        found[at : at + size] + inputs_ref[gate, pl.ds(start, size), lanes]
                    )


def direct_kernel(start, count, far_ref, weight_ref, base_ref, out_ref):
    height, width = far_ref.shape
    first = (lax.axis_index("hid") ^ (count // 2)) * width
    for tile in range(width // TILE):
        lanes = pl.ds(tile * TILE, TILE)
        for gate in range(3):
            found = tile_dot(far_ref, weight_ref, first, gate, lanes)
            out_ref[gate, :, lanes] = base_ref[gate, pl.ds(start, height), lanes] + found


def step_kernel(count, index, start, chunk, step, copies, *refs):
    refs = list(refs)
    split = splits(step, index, count)
    far = [refs.pop(0) for _ in range(split, count // 2)]
    weight_ref, base_ref, inputs_ref, state_ref, init_ref = [refs.pop(0) for _ in range(5)]
    last = index == CHUNKS - 1
    next_ref, edge_ref = [refs.pop(0) for _ in range(2)] if last else (None, None)
    opens = index == 0 and step == 0
    before_ref = None if opens else refs.pop(0)
    diag_ref = None if opens else refs.pop(0)
    a_ref, b_ref, ends_ref = [refs.pop(0) for _ in range(3)]
    diag_ref = refs.pop(0) if opens else diag_ref
    begins = last and step == 0
    send_ref = refs.pop(0) if last else None
    lhs, *products = refs
    height = products[0].shape[1]
    rows, width = state_ref.shape
    lead = height - chunk
    hid = lax.axis_index("hid")
    is_first = lax.axis_index("tm") == 0
    is_last = lax.axis_index("tm") == lax.axis_size("tm") - 1
    groups = chunk // GROUP
    tiles = width // TILE

    if opens:
        diagonals(weight_ref, hid, diag_ref)
    own = hid % (count // 2)
    if split:
        lhs = far[0]
        first = (hid ^ (count // 2) ^ 1) * width
        begin_row = 0
    else:
        for offset in range(count // 2):
            lhs[:, pl.ds(pl.multiple_of((own ^ offset) * width, width), width)] = far[offset][...]
        first = ((hid - own) ^ (count // 2)) * width
        begin_row = start
    row = lax.broadcasted_iota(jnp.int32, (GROUP, TILE), 0)
    zeros = jnp.zeros((GROUP, TILE), F32)

    def dots(tile):
        for gate in range(3):
            products[tile][gate] = tile_dot(lhs, weight_ref, first, gate, pl.ds(tile * TILE, TILE))

    def cells(tile):
        lanes = pl.ds(tile * TILE, TILE)
        diag_z = diag_ref[pl.ds(0, GROUP), lanes]
        diag_r = diag_ref[pl.ds(GROUP, GROUP), lanes]
        diag_n = diag_ref[pl.ds(2 * GROUP, GROUP), lanes]
        squares = zeros
        if index == 0:
            run_a, run_b = jnp.ones((GROUP, TILE), F32), zeros
        else:
            run_a = jnp.broadcast_to(before_ref[0:1, lanes], (GROUP, TILE))
            run_b = jnp.broadcast_to(before_ref[1:2, lanes], (GROUP, TILE))
        turned = pltpu.roll(state_ref[pl.ds(start, GROUP), lanes], GROUP - 1, 0)
        for group in range(groups):
            here = pl.ds(group * GROUP, GROUP)
            token = pl.ds(start + group * GROUP, GROUP)
            prev = state_ref[token, lanes]
            if last and group == groups - 1:
                following = jnp.broadcast_to(next_ref[:, lanes], (GROUP, TILE))
            else:
                following = state_ref[pl.ds(start + (group + 1) * GROUP, GROUP), lanes]
            turned_next = pltpu.roll(following, GROUP - 1, 0)
            state = jnp.where(row == GROUP - 1, turned_next, turned)
            turned = turned_next
            place = lead + group * GROUP
            bases = [base_ref[gate, pl.ds(begin_row + place, GROUP), lanes] for gate in range(3)]
            inputs = inputs_ref[2, token, lanes]
            if last and group == groups - 1:
                edges = [edge_ref[:, pl.ds((gate + 1) * width + tile * TILE, TILE)] for gate in range(3)]
                edges = [jnp.where(row == GROUP - 1, jnp.broadcast_to(line, (GROUP, TILE)), 0.0) for line in edges]
                bases = [bases[0] + edges[0], bases[1] + edges[1], bases[2]]
                inputs = inputs + edges[2]
            found = [products[tile][gate, pl.ds(place, GROUP), :] for gate in range(3)]
            zeta, reset, gated, cand, gap, value = gates(bases, found, inputs, prev)
            rest = 1.0 - zeta
            slope = zeta + gap * (zeta * rest) * diag_z
            slope = slope + rest * (1.0 - cand * cand) * (reset * diag_n + gated * (1.0 - reset) * diag_r)
            error = state - value
            if last and group == groups - 1:
                error = jnp.where((row == GROUP - 1) & is_last, 0.0, error)
            squares = squares + error * error
            a = slope
            b = value - slope * prev
            for distance in (1, 2, 4):
                keep = row >= distance
                a_up = jnp.where(keep, pltpu.roll(a, distance, 0), 1.0)
                b_up = jnp.where(keep, pltpu.roll(b, distance, 0), 0.0)
                b = a * b_up + b
                a = a * a_up
            a_ref[here, lanes] = a * run_a
            b_ref[here, lanes] = a * run_b + b
            last_a = jnp.broadcast_to(a[GROUP - 1 :], (GROUP, TILE))
            last_b = jnp.broadcast_to(b[GROUP - 1 :], (GROUP, TILE))
            run_a, run_b = last_a * run_a, last_a * run_b + last_b
        if begins:
            begin = gates(
                [base_ref[gate, pl.ds(begin_row, GROUP), lanes] for gate in range(3)],
                [products[tile][gate, pl.ds(0, GROUP), :] for gate in range(3)],
                inputs_ref[2, pl.ds(rows, GROUP), lanes],
                jnp.broadcast_to(init_ref[:, lanes], (GROUP, TILE)),
            )[-1]
            error = state_ref[pl.ds(0, GROUP), lanes] - begin
            squares = squares + jnp.where((row == 0) & is_first, error * error, 0.0)
            begin = begin[0:1]
            earlier = zeros[0:1]
        elif step == 0:
            begin, earlier = zeros[0:1], zeros[0:1]
        else:
            begin = before_ref[3:4, lanes]
            earlier = before_ref[2:3, lanes] if index == 0 else before_ref[4:5, lanes]
        total = jnp.sum(squares, axis=0, keepdims=True)
        if index:
            total = total + before_ref[2:3, lanes]
        ends_ref[0:1, lanes] = run_a[0:1]
        ends_ref[1:2, lanes] = run_b[0:1]
        ends_ref[2:3, lanes] = total
        ends_ref[3:4, lanes] = begin
        ends_ref[4:5, lanes] = earlier
        if last:
            send_a = jnp.where(is_first, 0.0, run_a[0:1])
            send_b = jnp.where(is_first, run_a[0:1] * begin + run_b[0:1], run_b[0:1])
            for part in range(TILE // LANES):
                at = tile * (TILE // LANES) + part
                for line, sent in ((at, send_a), (width // LANES + at, send_b)):
                    picked = sent[:, part * LANES : (part + 1) * LANES]
                    send_ref[:, pl.ds(line, 1), :] = jnp.broadcast_to(picked[None], (copies, 1, LANES))

    dots(0)
    for tile in range(1, tiles):
        dots(tile)
        cells(tile - 1)
    cells(tiles - 1)
    if last and step == ITERS - 1:
        lane = lax.broadcasted_iota(jnp.int32, (1, LANES), 1)
        sums = jnp.zeros((1, LANES), F32)
        for line, half in ((4, 0), (2, 1)):
            part = sum(ends_ref[pl.ds(line, 1), pl.ds(at, LANES)] for at in range(0, width, LANES))
            part = part + pltpu.roll(part, LANES // 2, 1)
            sums = jnp.where(lane // (LANES // 2) == half, part, sums)
        send_ref[:, pl.ds(2 * width // LANES, 1), :] = jnp.broadcast_to(sums[None], (copies, 1, LANES))


def apply_kernel(step, *refs):
    final = step == ITERS - 1
    maps, refs = refs[: 2 * CHUNKS], refs[2 * CHUNKS :]
    begin_ref, all_ref, state_ref = refs[:3]
    outs = refs[3:]
    rows, width = state_ref.shape
    lines = width // LANES
    place = lax.axis_index("tm")
    peers = all_ref.shape[0]

    def compose(peer, enter):
        moved = all_ref[peer, pl.ds(0, lines), :] * enter + all_ref[peer, pl.ds(lines, lines), :]
        return jnp.where(peer < place, moved, enter)

    begin = jnp.concatenate([begin_ref[3:4, pl.ds(at * LANES, LANES)] for at in range(lines)], axis=0)
    found = lax.fori_loop(0, peers, compose, begin, unroll=min(peers, 8))
    enter = jnp.concatenate([found[at : at + 1] for at in range(lines)], axis=1)
    height = 2 * GROUP
    row = lax.broadcasted_iota(jnp.int32, (height, width), 0)
    enter = jnp.broadcast_to(enter, (height, width))
    before = enter
    held = spans(step, rows)
    sent = held if final else spans(step + 1, rows)
    cuts = sorted({at for at, _ in held + sent} | {rows})
    for low, high in zip(cuts, cuts[1:]):
        source = max(place for place, (at, _) in enumerate(held) if at <= low)
        target = max(place for place, (at, _) in enumerate(sent) if at <= low)
        a_ref, b_ref = maps[2 * source], maps[2 * source + 1]

        def advance(group, before):
            at = low + group * height
            here = pl.ds(pl.multiple_of(at - held[source][0], height), height)
            token = pl.ds(pl.multiple_of(at, height), height)
            turned = pltpu.roll(a_ref[here, :] * enter + b_ref[here, :], 1, 0)
            moved = jnp.where(row == 0, before, turned)
            state_ref[token, :] = moved
            if not final:
                rounded = moved.astype(BF16)
                outs[1][token, :] = rounded
                outs[2 + target][pl.ds(pl.multiple_of(at - sent[target][0], height), height), :] = rounded
            return turned

        before = lax.fori_loop(0, (high - low) // height, advance, before, unroll=2)
    if not final:
        outs[0][...] = before[0:1]


def sums_kernel(all_ref, out_ref):
    out_ref[...] = jnp.sum(all_ref[:, pl.ds(all_ref.shape[1] - 1, 1), :], axis=0)


def norm_kernel(size, *refs):
    *parts, out_ref = refs
    total = sum(part[...] for part in parts)
    lane = lax.broadcasted_iota(jnp.int32, (1, LANES), 1)
    for half in range(ITERS):
        out_ref[half] = jnp.sqrt(jnp.sum(jnp.where(lane // (LANES // 2) == half, total, 0.0)) / size)


def newton(token_ids, input_table, recur_weight, z_bias, hn_bias, init_state, guess):
    rows, width = guess.shape
    full = recur_weight.shape[0]
    count = lax.axis_size("hid")
    blocks_tm = lax.axis_size("tm")
    weight = jnp.transpose(recur_weight, (1, 0, 2))
    table = jnp.transpose(input_table, (1, 0, 2))
    lines = width // LANES

    first = spans(0, rows)[0][1]
    rounded, rest = lax.optimization_barrier((guess.astype(BF16), guess))
    opening = rounded[:first]
    whole, *moved = pl.pallas_call(
        merge_kernel,
        out_shape=[jax.ShapeDtypeStruct((rows + EXTRA, width), BF16)]
        + [
            jax.ShapeDtypeStruct((height + EXTRA * (at + height == rows), width), BF16)
            for at, height in spans(0, rows)[1:]
        ],
        in_specs=vmem(2),
        out_specs=vmem(CHUNKS),
        compiler_params=params(8),
        cost_estimate=cost(COVER, 8 * rows * width),
        name="merge",
    )(rounded, init_state[None])
    moved = [opening, *moved]
    inputs, line = pl.pallas_call(
        prepare_kernel,
        out_shape=[
            jax.ShapeDtypeStruct((3, rows + GROUP, width), F32),
            jax.ShapeDtypeStruct((1, 4 * width), F32),
        ],
        in_specs=vmem(4),
        out_specs=vmem(2),
        compiler_params=params(32),
        cost_estimate=cost(2 * COVER, 8 * rows * width),
        name="prepare",
    )(token_ids[None], rest, table, z_bias[None])
    edge = from_next(line, "tm")
    state, following = rest, edge

    ends, diag = None, None
    for step in range(ITERS):
        final = step == ITERS - 1
        near = {0: whole}
        far = [{count // 2: None} for _ in range(CHUNKS)]
        for index in range(CHUNKS):
            far[index][count // 2] = swapped(moved[index], "hid", count // 2)
        bit = count // 4
        while bit:
            for offset in list(near):
                near[offset | bit] = swapped(near[offset], "hid", bit)
            for index in range(CHUNKS):
                for offset in list(far[index]):
                    far[index][offset | bit] = swapped(far[index][offset], "hid", bit)
            bit //= 2
        height = whole.shape[0]
        base = pl.pallas_call(
            functools.partial(base_kernel, step, count),
            out_shape=jax.ShapeDtypeStruct((3, height, width), F32),
            in_specs=vmem(count // 2 + 3),
            out_specs=vmem(1)[0],
            scratch_shapes=[pltpu.VMEM((height, full // 2), BF16)],
            compiler_params=params(16),
            cost_estimate=cost(3 * height * full * width, 3 * full * width),
        )(*[near[offset] for offset in range(count // 2)], weight, inputs, hn_bias[None])
        maps = []
        for index, (start, chunk) in enumerate(spans(step, rows)):
            last = index == CHUNKS - 1
            height = moved[index].shape[0]
            split = splits(step, index, count)
            sums = base
            if split:
                sums = pl.pallas_call(
                    functools.partial(direct_kernel, start, count),
                    out_shape=jax.ShapeDtypeStruct((3, height, width), F32),
                    in_specs=vmem(3),
                    out_specs=vmem(1)[0],
                    compiler_params=params(16),
                    cost_estimate=cost(3 * height * full * width // 2, 3 * full * width),
                )(far[index][count // 2], weight, base)
            operands = [far[index][offset] for offset in range(count // 2 + split, count)]
            operands += [weight, sums, inputs, state, init_state[None]]
            if last:
                operands += [following, edge]
            if diag is not None:
                operands += [ends, diag]
            outs = [
                jax.ShapeDtypeStruct((chunk, width), F32),
                jax.ShapeDtypeStruct((chunk, width), F32),
                jax.ShapeDtypeStruct((5, width), F32),
            ]
            if diag is None:
                outs.append(jax.ShapeDtypeStruct((3 * GROUP, width), F32))
            copies = blocks_tm
            if last:
                outs.append(jax.ShapeDtypeStruct((copies, 2 * lines + final, LANES), F32))
            found = pl.pallas_call(
                functools.partial(step_kernel, count, index, start, chunk, step, copies),
                out_shape=outs,
                in_specs=vmem(len(operands)),
                out_specs=vmem(len(outs)),
                scratch_shapes=[pltpu.VMEM((height, full // 2), BF16)]
                + [pltpu.VMEM((3, height, TILE), F32)] * (width // TILE),
                compiler_params=params(32),
                cost_estimate=cost(height * full * 3 * width, 3 * full * width),
            )(*operands)
            maps += found[:2]
            ends = found[2]
            diag = found[3] if diag is None else diag
        every = lax.all_to_all(found[-1], "tm", 0, 0)
        outs = [jax.ShapeDtypeStruct((rows, width), F32)]
        if final:
            part = pl.pallas_call(
                sums_kernel,
                out_shape=jax.ShapeDtypeStruct((1, LANES), F32),
                in_specs=vmem(1),
                out_specs=vmem(1)[0],
                compiler_params=params(8),
                name="sums",
            )(every)
            parts = [part]
            for offset in range(1, count):
                parts.append(swapped(part, "hid", offset))
        else:
            outs.append(jax.ShapeDtypeStruct((1, width), F32))
            outs.append(jax.ShapeDtypeStruct((rows, width), BF16))
            outs += [jax.ShapeDtypeStruct((chunk, width), BF16) for _, chunk in spans(step + 1, rows)]
        result = pl.pallas_call(
            functools.partial(apply_kernel, step),
            out_shape=outs,
            in_specs=vmem(2 * CHUNKS + 2),
            out_specs=vmem(len(outs)),
            compiler_params=params(16),
            cost_estimate=cost(2 * rows * width, 16 * rows * width),
        )(*maps, ends, every)
        if final:
            residual_norm = pl.pallas_call(
                functools.partial(norm_kernel, blocks_tm * count * rows * width),
                out_shape=jax.ShapeDtypeStruct((ITERS,), F32),
                in_specs=vmem(count),
                out_specs=smem()[0],
                compiler_params=params(8),
                name="norm",
            )(*parts)
            return (result[0], residual_norm)
        state, following, whole, *moved = result


def solution(mesh):
    return jax.shard_map(
        newton,
        mesh=mesh,
        in_specs=(
            P("tm"),
            P(None, None, "hid"),
            P(None, None, "hid"),
            P("hid"),
            P("hid"),
            P("hid"),
            P("tm", "hid"),
        ),
        out_specs=(P("tm", "hid"), P()),
        check_vma=False,
    )
```

```python
import functools

import jax
import jax.numpy as jnp
from jax import lax
from jax.experimental import pallas as pl
from jax.experimental.pallas import tpu as pltpu
from jax.sharding import PartitionSpec as P


ITERS = 2
SHARES = ((10, 6), (19, 13))
CHUNKS = len(SHARES[0])
GROUP = 8
EXTRA = 8
SPLIT = ((1, 1), (1, 1))
TILE = 256
LANES = 128
COVER = 2_000_000_000
F32 = jnp.float32
BF16 = jnp.bfloat16


def swapped(block, axis, bit):
    route = [(i, i ^ bit) for i in range(lax.axis_size(axis))]
    return lax.ppermute(block, axis, route)


def from_next(block, axis):
    route = [(i + 1, i) for i in range(lax.axis_size(axis) - 1)]
    return lax.ppermute(block, axis, route)


def sigmoid(x):
    return 0.5 * jnp.tanh(0.5 * x) + 0.5


def splits(step, index, count):
    return SPLIT[step][index] if count == 4 else 0


def spans(step, rows):
    unit = rows // sum(SHARES[step])
    found, at = [], 0
    for share in SHARES[step]:
        found.append((at, share * unit))
        at += share * unit
    return found


def vmem(count):
    return [pl.BlockSpec(memory_space=pltpu.VMEM)] * count


def smem():
    return [pl.BlockSpec(memory_space=pltpu.SMEM)]


def params(mib):
    return pltpu.CompilerParams(vmem_limit_bytes=mib * 1024 * 1024)


def cost(flops, moved):
    return pl.CostEstimate(flops=flops, bytes_accessed=moved, transcendentals=0)


def merge_kernel(rounded_ref, init_ref, whole_ref, *parts):
    rows, width = rounded_ref.shape
    opening = spans(0, rows)[0][1]
    whole_ref[pl.ds(0, opening), :] = rounded_ref[pl.ds(0, opening), :]
    for (at, chunk), part in zip(spans(0, rows)[1:], parts):
        lead = part.shape[0] - chunk
        if lead:
            row = lax.broadcasted_iota(jnp.int32, (lead, width), 0)
            head = jnp.where(row == 0, jnp.broadcast_to(init_ref[...], (lead, width)), 0.0).astype(BF16)
            part[pl.ds(0, lead), :] = head
            whole_ref[pl.ds(at, lead), :] = head
        block = rounded_ref[pl.ds(at, chunk), :]
        part[pl.ds(lead, chunk), :] = block
        whole_ref[pl.ds(at + lead, chunk), :] = block


def prepare_kernel(ids_ref, table_ref, bias_ref, out_ref):
    vocab, width = table_ref.shape[1:]
    rows = ids_ref.shape[1]
    entry = lax.broadcasted_iota(jnp.int32, (vocab, rows), 0)
    hot = (entry == pltpu.roll(ids_ref[...], rows - 1, 1)).astype(F32).astype(BF16)
    row = lax.broadcasted_iota(jnp.int32, (GROUP, width), 0)
    for gate in range(3):
        table = table_ref[gate]
        if gate == 0:
            table = table + bias_ref[...]
        total = None
        for _ in range(3):
            part = table.astype(BF16)
            table = table - part.astype(F32)
            picked = lax.dot_general(hot, part, (((0,), (0,)), ((), ())), preferred_element_type=F32)
            total = picked if total is None else total + picked
        ending = total[rows - GROUP :]
        begin = ending[GROUP - 1 :]
        out_ref[gate, pl.ds(0, rows - GROUP), :] = total[: rows - GROUP]
        out_ref[gate, pl.ds(rows - GROUP, GROUP), :] = jnp.where(row == GROUP - 1, 0.0, ending)
        out_ref[gate, pl.ds(rows, GROUP), :] = jnp.broadcast_to(begin, (GROUP, width))


def diagonals(weight_ref, hid, diag_ref):
    width = diag_ref.shape[1]
    row = lax.broadcasted_iota(jnp.int32, (width, width), 0)
    col = lax.broadcasted_iota(jnp.int32, (width, width), 1)
    first = pl.multiple_of(hid * width, width)
    for gate in range(3):
        block = weight_ref[gate, pl.ds(first, width), :].astype(F32)
        line = jnp.sum(jnp.where(row == col, block, 0.0), axis=0, keepdims=True)
        diag_ref[pl.ds(gate * GROUP, GROUP), :] = jnp.broadcast_to(line, (GROUP, width))


def gates(bases, products, inputs, prev):
    zeta = sigmoid(bases[0] + products[0])
    reset = sigmoid(bases[1] + products[1])
    gated = reset * (bases[2] + products[2])
    cand = jnp.tanh(inputs + gated)
    gap = prev - cand
    return zeta, reset, gated, cand, gap, cand + zeta * gap


def tile_dot(lhs, weight_ref, first, gate, lanes):
    depth = lhs.shape[1]
    pieces = 2 if gate == 2 else 1
    total = None
    for piece in range(pieces):
        at = pl.multiple_of(first + piece * (depth // pieces), depth // pieces)
        term = jnp.dot(
            lhs[:, pl.ds(piece * (depth // pieces), depth // pieces)],
            weight_ref[gate, pl.ds(at, depth // pieces), lanes],
            preferred_element_type=F32,
        )
        total = term if total is None else total + term
    return total


def base_kernel(step, count, *refs):
    near, (weight_ref, inputs_ref, bias_ref, *lines, lhs) = refs[: count // 2], refs[count // 2 :]
    base_ref = lines[0] if step else lines[1]
    height, _ = lhs.shape
    width = base_ref.shape[2]
    rows = inputs_ref.shape[1] - GROUP
    if step == 0:
        guess_ref, _, line_ref = lines
        line_ref[:, pl.ds(0, width)] = guess_ref[0:1, :]
        for gate in range(3):
            line_ref[:, pl.ds((gate + 1) * width, width)] = inputs_ref[gate, pl.ds(rows, 1), :]
    hid = lax.axis_index("hid")
    own = hid % (count // 2)
    for offset in range(count // 2):
        lhs[:, pl.ds(pl.multiple_of((own ^ offset) * width, width), width)] = near[offset][...]
    pieces, at = [], 0
    for start, chunk in spans(step, rows):
        if start + chunk == rows and height > rows:
            pieces.append((at, rows, GROUP))
            at += EXTRA
        pieces.append((at, start, chunk))
        at += chunk
    for tile in range(width // TILE):
        lanes = pl.ds(tile * TILE, TILE)
        for gate in range(3):
            found = tile_dot(lhs, weight_ref, (hid - own) * width, gate, lanes)
            if gate == 2:
                base_ref[gate, :, lanes] = found + bias_ref[:, lanes]
            else:
                for at, start, size in pieces:
                    base_ref[gate, pl.ds(at, size), lanes] = (
                        found[at : at + size] + inputs_ref[gate, pl.ds(start, size), lanes]
                    )


def direct_kernel(start, count, far_ref, weight_ref, base_ref, out_ref):
    height, width = far_ref.shape
    first = (lax.axis_index("hid") ^ (count // 2)) * width
    for tile in range(width // TILE):
        lanes = pl.ds(tile * TILE, TILE)
        for gate in range(3):
            found = tile_dot(far_ref, weight_ref, first, gate, lanes)
            out_ref[gate, :, lanes] = base_ref[gate, pl.ds(start, height), lanes] + found


def step_kernel(count, index, start, chunk, step, copies, *refs):
    refs = list(refs)
    split = splits(step, index, count)
    far = [refs.pop(0) for _ in range(split, count // 2)]
    weight_ref, base_ref, inputs_ref, state_ref, init_ref = [refs.pop(0) for _ in range(5)]
    last = index == CHUNKS - 1
    next_ref, edge_ref = [refs.pop(0) for _ in range(2)] if last else (None, None)
    opens = index == 0 and step == 0
    before_ref = None if opens else refs.pop(0)
    diag_ref = None if opens else refs.pop(0)
    a_ref, b_ref, ends_ref = [refs.pop(0) for _ in range(3)]
    diag_ref = refs.pop(0) if opens else diag_ref
    begins = last and step == 0
    send_ref = refs.pop(0) if last else None
    lhs, *products = refs
    height = products[0].shape[1]
    rows, width = state_ref.shape
    lead = height - chunk
    hid = lax.axis_index("hid")
    is_first = lax.axis_index("tm") == 0
    is_last = lax.axis_index("tm") == lax.axis_size("tm") - 1
    groups = chunk // GROUP
    tiles = width // TILE

    if opens:
        diagonals(weight_ref, hid, diag_ref)
    own = hid % (count // 2)
    if split:
        lhs = far[0]
        first = (hid ^ (count // 2) ^ 1) * width
        begin_row = 0
    else:
        for offset in range(count // 2):
            lhs[:, pl.ds(pl.multiple_of((own ^ offset) * width, width), width)] = far[offset][...]
        first = ((hid - own) ^ (count // 2)) * width
        begin_row = start
    row = lax.broadcasted_iota(jnp.int32, (GROUP, TILE), 0)
    zeros = jnp.zeros((GROUP, TILE), F32)

    def dots(tile):
        for gate in range(3):
            products[tile][gate] = tile_dot(lhs, weight_ref, first, gate, pl.ds(tile * TILE, TILE))

    def cells(tile):
        lanes = pl.ds(tile * TILE, TILE)
        diag_z = diag_ref[pl.ds(0, GROUP), lanes]
        diag_r = diag_ref[pl.ds(GROUP, GROUP), lanes]
        diag_n = diag_ref[pl.ds(2 * GROUP, GROUP), lanes]
        squares = zeros
        if index == 0:
            run_a, run_b = jnp.ones((GROUP, TILE), F32), zeros
        else:
            run_a = jnp.broadcast_to(before_ref[0:1, lanes], (GROUP, TILE))
            run_b = jnp.broadcast_to(before_ref[1:2, lanes], (GROUP, TILE))
        turned = pltpu.roll(state_ref[pl.ds(start, GROUP), lanes], GROUP - 1, 0)
        for group in range(groups):
            here = pl.ds(group * GROUP, GROUP)
            token = pl.ds(start + group * GROUP, GROUP)
            prev = state_ref[token, lanes]
            if last and group == groups - 1:
                following = jnp.broadcast_to(next_ref[:, lanes], (GROUP, TILE))
            else:
                following = state_ref[pl.ds(start + (group + 1) * GROUP, GROUP), lanes]
            turned_next = pltpu.roll(following, GROUP - 1, 0)
            state = jnp.where(row == GROUP - 1, turned_next, turned)
            turned = turned_next
            place = lead + group * GROUP
            bases = [base_ref[gate, pl.ds(begin_row + place, GROUP), lanes] for gate in range(3)]
            inputs = inputs_ref[2, token, lanes]
            if last and group == groups - 1:
                edges = [edge_ref[:, pl.ds((gate + 1) * width + tile * TILE, TILE)] for gate in range(3)]
                edges = [jnp.where(row == GROUP - 1, jnp.broadcast_to(line, (GROUP, TILE)), 0.0) for line in edges]
                bases = [bases[0] + edges[0], bases[1] + edges[1], bases[2]]
                inputs = inputs + edges[2]
            found = [products[tile][gate, pl.ds(place, GROUP), :] for gate in range(3)]
            zeta, reset, gated, cand, gap, value = gates(bases, found, inputs, prev)
            rest = 1.0 - zeta
            slope = zeta + gap * (zeta * rest) * diag_z
            slope = slope + rest * (1.0 - cand * cand) * (reset * diag_n + gated * (1.0 - reset) * diag_r)
            error = state - value
            if last and group == groups - 1:
                error = jnp.where((row == GROUP - 1) & is_last, 0.0, error)
            squares = squares + error * error
            a = slope
            b = value - slope * prev
            for distance in (1, 2, 4):
                keep = row >= distance
                a_up = jnp.where(keep, pltpu.roll(a, distance, 0), 1.0)
                b_up = jnp.where(keep, pltpu.roll(b, distance, 0), 0.0)
                b = a * b_up + b
                a = a * a_up
            a_ref[here, lanes] = a * run_a
            b_ref[here, lanes] = a * run_b + b
            last_a = jnp.broadcast_to(a[GROUP - 1 :], (GROUP, TILE))
            last_b = jnp.broadcast_to(b[GROUP - 1 :], (GROUP, TILE))
            run_a, run_b = last_a * run_a, last_a * run_b + last_b
        if begins:
            begin = gates(
                [base_ref[gate, pl.ds(begin_row, GROUP), lanes] for gate in range(3)],
                [products[tile][gate, pl.ds(0, GROUP), :] for gate in range(3)],
                inputs_ref[2, pl.ds(rows, GROUP), lanes],
                jnp.broadcast_to(init_ref[:, lanes], (GROUP, TILE)),
            )[-1]
            error = state_ref[pl.ds(0, GROUP), lanes] - begin
            squares = squares + jnp.where((row == 0) & is_first, error * error, 0.0)
            begin = begin[0:1]
            earlier = zeros[0:1]
        elif step == 0:
            begin, earlier = zeros[0:1], zeros[0:1]
        else:
            begin = before_ref[3:4, lanes]
            earlier = before_ref[2:3, lanes] if index == 0 else before_ref[4:5, lanes]
        total = jnp.sum(squares, axis=0, keepdims=True)
        if index:
            total = total + before_ref[2:3, lanes]
        ends_ref[0:1, lanes] = run_a[0:1]
        ends_ref[1:2, lanes] = run_b[0:1]
        ends_ref[2:3, lanes] = total
        ends_ref[3:4, lanes] = begin
        ends_ref[4:5, lanes] = earlier
        if last:
            send_a = jnp.where(is_first, 0.0, run_a[0:1])
            send_b = jnp.where(is_first, run_a[0:1] * begin + run_b[0:1], run_b[0:1])
            for part in range(TILE // LANES):
                at = tile * (TILE // LANES) + part
                for line, sent in ((at, send_a), (width // LANES + at, send_b)):
                    picked = sent[:, part * LANES : (part + 1) * LANES]
                    send_ref[:, pl.ds(line, 1), :] = jnp.broadcast_to(picked[None], (copies, 1, LANES))

    dots(0)
    for tile in range(1, tiles):
        dots(tile)
        cells(tile - 1)
    cells(tiles - 1)
    if last and step == ITERS - 1:
        lane = lax.broadcasted_iota(jnp.int32, (1, LANES), 1)
        sums = jnp.zeros((1, LANES), F32)
        for line, half in ((4, 0), (2, 1)):
            part = sum(ends_ref[pl.ds(line, 1), pl.ds(at, LANES)] for at in range(0, width, LANES))
            part = part + pltpu.roll(part, LANES // 2, 1)
            sums = jnp.where(lane // (LANES // 2) == half, part, sums)
        send_ref[:, pl.ds(2 * width // LANES, 1), :] = jnp.broadcast_to(sums[None], (copies, 1, LANES))


def apply_kernel(step, *refs):
    final = step == ITERS - 1
    maps, refs = refs[: 2 * CHUNKS], refs[2 * CHUNKS :]
    begin_ref, all_ref, state_ref = refs[:3]
    outs = refs[3:]
    rows, width = state_ref.shape
    lines = width // LANES
    place = lax.axis_index("tm")
    peers = all_ref.shape[0]

    def compose(peer, enter):
        moved = all_ref[peer, pl.ds(0, lines), :] * enter + all_ref[peer, pl.ds(lines, lines), :]
        return jnp.where(peer < place, moved, enter)

    begin = jnp.concatenate([begin_ref[3:4, pl.ds(at * LANES, LANES)] for at in range(lines)], axis=0)
    found = lax.fori_loop(0, peers, compose, begin, unroll=min(peers, 8))
    enter = jnp.concatenate([found[at : at + 1] for at in range(lines)], axis=1)
    height = 2 * GROUP
    row = lax.broadcasted_iota(jnp.int32, (height, width), 0)
    enter = jnp.broadcast_to(enter, (height, width))
    before = enter
    held = spans(step, rows)
    sent = held if final else spans(step + 1, rows)
    cuts = sorted({at for at, _ in held + sent} | {rows})
    for low, high in zip(cuts, cuts[1:]):
        source = max(place for place, (at, _) in enumerate(held) if at <= low)
        target = max(place for place, (at, _) in enumerate(sent) if at <= low)
        a_ref, b_ref = maps[2 * source], maps[2 * source + 1]

        def advance(group, before):
            at = low + group * height
            here = pl.ds(pl.multiple_of(at - held[source][0], height), height)
            token = pl.ds(pl.multiple_of(at, height), height)
            turned = pltpu.roll(a_ref[here, :] * enter + b_ref[here, :], 1, 0)
            moved = jnp.where(row == 0, before, turned)
            state_ref[token, :] = moved
            if not final:
                rounded = moved.astype(BF16)
                outs[1][token, :] = rounded
                outs[2 + target][pl.ds(pl.multiple_of(at - sent[target][0], height), height), :] = rounded
            return turned

        before = lax.fori_loop(0, (high - low) // height, advance, before, unroll=2)
    if not final:
        outs[0][...] = before[0:1]


def sums_kernel(all_ref, out_ref):
    out_ref[...] = jnp.sum(all_ref[:, pl.ds(all_ref.shape[1] - 1, 1), :], axis=0)


def norm_kernel(size, *refs):
    *parts, out_ref = refs
    total = sum(part[...] for part in parts)
    lane = lax.broadcasted_iota(jnp.int32, (1, LANES), 1)
    for half in range(ITERS):
        out_ref[half] = jnp.sqrt(jnp.sum(jnp.where(lane // (LANES // 2) == half, total, 0.0)) / size)


def newton(token_ids, input_table, recur_weight, z_bias, hn_bias, init_state, guess):
    rows, width = guess.shape
    full = recur_weight.shape[0]
    count = lax.axis_size("hid")
    blocks_tm = lax.axis_size("tm")
    weight = jnp.transpose(recur_weight, (1, 0, 2))
    table = jnp.transpose(input_table, (1, 0, 2))
    lines = width // LANES

    first = spans(0, rows)[0][1]
    rounded, rest = lax.optimization_barrier((guess.astype(BF16), guess))
    opening = rounded[:first]
    whole, *moved = pl.pallas_call(
        merge_kernel,
        out_shape=[jax.ShapeDtypeStruct((rows + EXTRA, width), BF16)]
        + [
            jax.ShapeDtypeStruct((height + EXTRA * (at + height == rows), width), BF16)
            for at, height in spans(0, rows)[1:]
        ],
        in_specs=vmem(2),
        out_specs=vmem(CHUNKS),
        compiler_params=params(8),
        cost_estimate=cost(COVER, 8 * rows * width),
        name="merge",
    )(rounded, init_state[None])
    moved = [opening, *moved]
    inputs = pl.pallas_call(
        prepare_kernel,
        out_shape=jax.ShapeDtypeStruct((3, rows + GROUP, width), F32),
        in_specs=vmem(3),
        out_specs=vmem(1)[0],
        compiler_params=params(32),
        cost_estimate=cost(2 * COVER, 8 * rows * width),
        name="prepare",
    )(token_ids[None], table, z_bias[None])
    state = rest

    ends, diag = None, None
    for step in range(ITERS):
        final = step == ITERS - 1
        near = {0: whole}
        far = [{count // 2: None} for _ in range(CHUNKS)]
        for index in range(CHUNKS):
            far[index][count // 2] = swapped(moved[index], "hid", count // 2)
        bit = count // 4
        while bit:
            for offset in list(near):
                near[offset | bit] = swapped(near[offset], "hid", bit)
            for index in range(CHUNKS):
                for offset in list(far[index]):
                    far[index][offset | bit] = swapped(far[index][offset], "hid", bit)
            bit //= 2
        height = whole.shape[0]
        operands = [*[near[offset] for offset in range(count // 2)], weight, inputs, hn_bias[None]]
        outs = [jax.ShapeDtypeStruct((3, height, width), F32)]
        if step == 0:
            operands.append(state)
            outs.append(jax.ShapeDtypeStruct((1, 4 * width), F32))
        base, *line = pl.pallas_call(
            functools.partial(base_kernel, step, count),
            out_shape=outs,
            in_specs=vmem(len(operands)),
            out_specs=vmem(len(outs)),
            scratch_shapes=[pltpu.VMEM((height, full // 2), BF16)],
            compiler_params=params(16),
            cost_estimate=cost(3 * height * full * width, 3 * full * width),
        )(*operands)
        if step == 0:
            edge = from_next(line[0], "tm")
            following = edge
        maps = []
        for index, (start, chunk) in enumerate(spans(step, rows)):
            last = index == CHUNKS - 1
            height = moved[index].shape[0]
            split = splits(step, index, count)
            sums = base
            if split:
                sums = pl.pallas_call(
                    functools.partial(direct_kernel, start, count),
                    out_shape=jax.ShapeDtypeStruct((3, height, width), F32),
                    in_specs=vmem(3),
                    out_specs=vmem(1)[0],
                    compiler_params=params(16),
                    cost_estimate=cost(3 * height * full * width // 2, 3 * full * width),
                )(far[index][count // 2], weight, base)
            operands = [far[index][offset] for offset in range(count // 2 + split, count)]
            operands += [weight, sums, inputs, state, init_state[None]]
            if last:
                operands += [following, edge]
            if diag is not None:
                operands += [ends, diag]
            outs = [
                jax.ShapeDtypeStruct((chunk, width), F32),
                jax.ShapeDtypeStruct((chunk, width), F32),
                jax.ShapeDtypeStruct((5, width), F32),
            ]
            if diag is None:
                outs.append(jax.ShapeDtypeStruct((3 * GROUP, width), F32))
            copies = blocks_tm
            if last:
                outs.append(jax.ShapeDtypeStruct((copies, 2 * lines + final, LANES), F32))
            found = pl.pallas_call(
                functools.partial(step_kernel, count, index, start, chunk, step, copies),
                out_shape=outs,
                in_specs=vmem(len(operands)),
                out_specs=vmem(len(outs)),
                scratch_shapes=[pltpu.VMEM((height, full // 2), BF16)]
                + [pltpu.VMEM((3, height, TILE), F32)] * (width // TILE),
                compiler_params=params(32),
                cost_estimate=cost(height * full * 3 * width, 3 * full * width),
            )(*operands)
            maps += found[:2]
            ends = found[2]
            diag = found[3] if diag is None else diag
        every = lax.all_to_all(found[-1], "tm", 0, 0)
        outs = [jax.ShapeDtypeStruct((rows, width), F32)]
        if final:
            part = pl.pallas_call(
                sums_kernel,
                out_shape=jax.ShapeDtypeStruct((1, LANES), F32),
                in_specs=vmem(1),
                out_specs=vmem(1)[0],
                compiler_params=params(8),
                name="sums",
            )(every)
            parts = [part]
            for offset in range(1, count):
                parts.append(swapped(part, "hid", offset))
        else:
            outs.append(jax.ShapeDtypeStruct((1, width), F32))
            outs.append(jax.ShapeDtypeStruct((rows, width), BF16))
            outs += [jax.ShapeDtypeStruct((chunk, width), BF16) for _, chunk in spans(step + 1, rows)]
        result = pl.pallas_call(
            functools.partial(apply_kernel, step),
            out_shape=outs,
            in_specs=vmem(2 * CHUNKS + 2),
            out_specs=vmem(len(outs)),
            compiler_params=params(16),
            cost_estimate=cost(2 * rows * width, 16 * rows * width),
        )(*maps, ends, every)
        if final:
            residual_norm = pl.pallas_call(
                functools.partial(norm_kernel, blocks_tm * count * rows * width),
                out_shape=jax.ShapeDtypeStruct((ITERS,), F32),
                in_specs=vmem(count),
                out_specs=smem()[0],
                compiler_params=params(8),
                name="norm",
            )(*parts)
            return (result[0], residual_norm)
        state, following, whole, *moved = result


def solution(mesh):
    return jax.shard_map(
        newton,
        mesh=mesh,
        in_specs=(
            P("tm"),
            P(None, None, "hid"),
            P(None, None, "hid"),
            P("hid"),
            P("hid"),
            P("hid"),
            P("tm", "hid"),
        ),
        out_specs=(P("tm", "hid"), P()),
        check_vma=False,
    )
```

```python
import functools

import jax
import jax.numpy as jnp
from jax import lax
from jax.experimental import pallas as pl
from jax.experimental.pallas import tpu as pltpu
from jax.sharding import PartitionSpec as P


ITERS = 2
SHARES = ((9, 7), (19, 13))
CHUNKS = len(SHARES[0])
GROUP = 8
EXTRA = 8
SPLIT = ((1, 1), (1, 1))
TILE = 256
LANES = 128
COVER = 2_000_000_000
F32 = jnp.float32
BF16 = jnp.bfloat16


def swapped(block, axis, bit):
    route = [(i, i ^ bit) for i in range(lax.axis_size(axis))]
    return lax.ppermute(block, axis, route)


def from_next(block, axis):
    route = [(i + 1, i) for i in range(lax.axis_size(axis) - 1)]
    return lax.ppermute(block, axis, route)


def sigmoid(x):
    return 0.5 * jnp.tanh(0.5 * x) + 0.5


def splits(step, index, count):
    return SPLIT[step][index] if count == 4 else 0


def spans(step, rows):
    unit = rows // sum(SHARES[step])
    found, at = [], 0
    for share in SHARES[step]:
        found.append((at, share * unit))
        at += share * unit
    return found


def vmem(count):
    return [pl.BlockSpec(memory_space=pltpu.VMEM)] * count


def smem():
    return [pl.BlockSpec(memory_space=pltpu.SMEM)]


def params(mib):
    return pltpu.CompilerParams(vmem_limit_bytes=mib * 1024 * 1024)


def cost(flops, moved):
    return pl.CostEstimate(flops=flops, bytes_accessed=moved, transcendentals=0)


def merge_kernel(rounded_ref, init_ref, whole_ref, *parts):
    rows, width = rounded_ref.shape
    opening = spans(0, rows)[0][1]
    whole_ref[pl.ds(0, opening), :] = rounded_ref[pl.ds(0, opening), :]
    for (at, chunk), part in zip(spans(0, rows)[1:], parts):
        lead = part.shape[0] - chunk
        if lead:
            row = lax.broadcasted_iota(jnp.int32, (lead, width), 0)
            head = jnp.where(row == 0, jnp.broadcast_to(init_ref[...], (lead, width)), 0.0).astype(BF16)
            part[pl.ds(0, lead), :] = head
            whole_ref[pl.ds(at, lead), :] = head
        block = rounded_ref[pl.ds(at, chunk), :]
        part[pl.ds(lead, chunk), :] = block
        whole_ref[pl.ds(at + lead, chunk), :] = block


def prepare_kernel(ids_ref, table_ref, bias_ref, out_ref):
    vocab, width = table_ref.shape[1:]
    rows = ids_ref.shape[1]
    entry = lax.broadcasted_iota(jnp.int32, (vocab, rows), 0)
    hot = (entry == pltpu.roll(ids_ref[...], rows - 1, 1)).astype(F32).astype(BF16)
    row = lax.broadcasted_iota(jnp.int32, (GROUP, width), 0)
    for gate in range(3):
        table = table_ref[gate]
        if gate == 0:
            table = table + bias_ref[...]
        total = None
        for _ in range(3):
            part = table.astype(BF16)
            table = table - part.astype(F32)
            picked = lax.dot_general(hot, part, (((0,), (0,)), ((), ())), preferred_element_type=F32)
            total = picked if total is None else total + picked
        ending = total[rows - GROUP :]
        begin = ending[GROUP - 1 :]
        out_ref[gate, pl.ds(0, rows - GROUP), :] = total[: rows - GROUP]
        out_ref[gate, pl.ds(rows - GROUP, GROUP), :] = jnp.where(row == GROUP - 1, 0.0, ending)
        out_ref[gate, pl.ds(rows, GROUP), :] = jnp.broadcast_to(begin, (GROUP, width))


def diagonals(weight_ref, hid, diag_ref):
    width = diag_ref.shape[1]
    row = lax.broadcasted_iota(jnp.int32, (width, width), 0)
    col = lax.broadcasted_iota(jnp.int32, (width, width), 1)
    first = pl.multiple_of(hid * width, width)
    for gate in range(3):
        block = weight_ref[gate, pl.ds(first, width), :].astype(F32)
        line = jnp.sum(jnp.where(row == col, block, 0.0), axis=0, keepdims=True)
        diag_ref[pl.ds(gate * GROUP, GROUP), :] = jnp.broadcast_to(line, (GROUP, width))


def gates(bases, products, inputs, prev):
    zeta = sigmoid(bases[0] + products[0])
    reset = sigmoid(bases[1] + products[1])
    gated = reset * (bases[2] + products[2])
    cand = jnp.tanh(inputs + gated)
    gap = prev - cand
    return zeta, reset, gated, cand, gap, cand + zeta * gap


def tile_dot(lhs, weight_ref, first, gate, lanes):
    depth = lhs.shape[1]
    pieces = 2 if gate == 2 else 1
    total = None
    for piece in range(pieces):
        at = pl.multiple_of(first + piece * (depth // pieces), depth // pieces)
        term = jnp.dot(
            lhs[:, pl.ds(piece * (depth // pieces), depth // pieces)],
            weight_ref[gate, pl.ds(at, depth // pieces), lanes],
            preferred_element_type=F32,
        )
        total = term if total is None else total + term
    return total


def base_kernel(step, count, *refs):
    near, (weight_ref, inputs_ref, bias_ref, *lines, lhs) = refs[: count // 2], refs[count // 2 :]
    base_ref = lines[0] if step else lines[1]
    height, _ = lhs.shape
    width = base_ref.shape[2]
    rows = inputs_ref.shape[1] - GROUP
    if step == 0:
        guess_ref, _, line_ref = lines
        line_ref[:, pl.ds(0, width)] = guess_ref[0:1, :]
        for gate in range(3):
            line_ref[:, pl.ds((gate + 1) * width, width)] = inputs_ref[gate, pl.ds(rows, 1), :]
    hid = lax.axis_index("hid")
    own = hid % (count // 2)
    for offset in range(count // 2):
        lhs[:, pl.ds(pl.multiple_of((own ^ offset) * width, width), width)] = near[offset][...]
    pieces, at = [], 0
    for start, chunk in spans(step, rows):
        if start + chunk == rows and height > rows:
            pieces.append((at, rows, GROUP))
            at += EXTRA
        pieces.append((at, start, chunk))
        at += chunk
    for tile in range(width // TILE):
        lanes = pl.ds(tile * TILE, TILE)
        for gate in range(3):
            found = tile_dot(lhs, weight_ref, (hid - own) * width, gate, lanes)
            if gate == 2:
                base_ref[gate, :, lanes] = found + bias_ref[:, lanes]
            else:
                for at, start, size in pieces:
                    base_ref[gate, pl.ds(at, size), lanes] = (
                        found[at : at + size] + inputs_ref[gate, pl.ds(start, size), lanes]
                    )


def direct_kernel(start, count, far_ref, weight_ref, base_ref, out_ref):
    height, width = far_ref.shape
    first = (lax.axis_index("hid") ^ (count // 2)) * width
    for tile in range(width // TILE):
        lanes = pl.ds(tile * TILE, TILE)
        for gate in range(3):
            found = tile_dot(far_ref, weight_ref, first, gate, lanes)
            out_ref[gate, :, lanes] = base_ref[gate, pl.ds(start, height), lanes] + found


def step_kernel(count, index, start, chunk, step, copies, *refs):
    refs = list(refs)
    split = splits(step, index, count)
    far = [refs.pop(0) for _ in range(split, count // 2)]
    weight_ref, base_ref, inputs_ref, state_ref, init_ref = [refs.pop(0) for _ in range(5)]
    last = index == CHUNKS - 1
    next_ref, edge_ref = [refs.pop(0) for _ in range(2)] if last else (None, None)
    opens = index == 0 and step == 0
    before_ref = None if opens else refs.pop(0)
    diag_ref = None if opens else refs.pop(0)
    a_ref, b_ref, ends_ref = [refs.pop(0) for _ in range(3)]
    diag_ref = refs.pop(0) if opens else diag_ref
    begins = last and step == 0
    send_ref = refs.pop(0) if last else None
    lhs, *products = refs
    height = products[0].shape[1]
    rows, width = state_ref.shape
    lead = height - chunk
    hid = lax.axis_index("hid")
    is_first = lax.axis_index("tm") == 0
    is_last = lax.axis_index("tm") == lax.axis_size("tm") - 1
    groups = chunk // GROUP
    tiles = width // TILE

    if opens:
        diagonals(weight_ref, hid, diag_ref)
    own = hid % (count // 2)
    if split:
        lhs = far[0]
        first = (hid ^ (count // 2) ^ 1) * width
        begin_row = 0
    else:
        for offset in range(count // 2):
            lhs[:, pl.ds(pl.multiple_of((own ^ offset) * width, width), width)] = far[offset][...]
        first = ((hid - own) ^ (count // 2)) * width
        begin_row = start
    row = lax.broadcasted_iota(jnp.int32, (GROUP, TILE), 0)
    zeros = jnp.zeros((GROUP, TILE), F32)

    def dots(tile):
        for gate in range(3):
            products[tile][gate] = tile_dot(lhs, weight_ref, first, gate, pl.ds(tile * TILE, TILE))

    def cells(tile):
        lanes = pl.ds(tile * TILE, TILE)
        diag_z = diag_ref[pl.ds(0, GROUP), lanes]
        diag_r = diag_ref[pl.ds(GROUP, GROUP), lanes]
        diag_n = diag_ref[pl.ds(2 * GROUP, GROUP), lanes]
        squares = zeros
        if index == 0:
            run_a, run_b = jnp.ones((GROUP, TILE), F32), zeros
        else:
            run_a = jnp.broadcast_to(before_ref[0:1, lanes], (GROUP, TILE))
            run_b = jnp.broadcast_to(before_ref[1:2, lanes], (GROUP, TILE))
        turned = pltpu.roll(state_ref[pl.ds(start, GROUP), lanes], GROUP - 1, 0)
        for group in range(groups):
            here = pl.ds(group * GROUP, GROUP)
            token = pl.ds(start + group * GROUP, GROUP)
            prev = state_ref[token, lanes]
            if last and group == groups - 1:
                following = jnp.broadcast_to(next_ref[:, lanes], (GROUP, TILE))
            else:
                following = state_ref[pl.ds(start + (group + 1) * GROUP, GROUP), lanes]
            turned_next = pltpu.roll(following, GROUP - 1, 0)
            state = jnp.where(row == GROUP - 1, turned_next, turned)
            turned = turned_next
            place = lead + group * GROUP
            bases = [base_ref[gate, pl.ds(begin_row + place, GROUP), lanes] for gate in range(3)]
            inputs = inputs_ref[2, token, lanes]
            if last and group == groups - 1:
                edges = [edge_ref[:, pl.ds((gate + 1) * width + tile * TILE, TILE)] for gate in range(3)]
                edges = [jnp.where(row == GROUP - 1, jnp.broadcast_to(line, (GROUP, TILE)), 0.0) for line in edges]
                bases = [bases[0] + edges[0], bases[1] + edges[1], bases[2]]
                inputs = inputs + edges[2]
            found = [products[tile][gate, pl.ds(place, GROUP), :] for gate in range(3)]
            zeta, reset, gated, cand, gap, value = gates(bases, found, inputs, prev)
            rest = 1.0 - zeta
            slope = zeta + gap * (zeta * rest) * diag_z
            slope = slope + rest * (1.0 - cand * cand) * (reset * diag_n + gated * (1.0 - reset) * diag_r)
            error = state - value
            if last and group == groups - 1:
                error = jnp.where((row == GROUP - 1) & is_last, 0.0, error)
            squares = squares + error * error
            a = slope
            b = value - slope * prev
            for distance in (1, 2, 4):
                keep = row >= distance
                a_up = jnp.where(keep, pltpu.roll(a, distance, 0), 1.0)
                b_up = jnp.where(keep, pltpu.roll(b, distance, 0), 0.0)
                b = a * b_up + b
                a = a * a_up
            a_ref[here, lanes] = a * run_a
            b_ref[here, lanes] = a * run_b + b
            last_a = jnp.broadcast_to(a[GROUP - 1 :], (GROUP, TILE))
            last_b = jnp.broadcast_to(b[GROUP - 1 :], (GROUP, TILE))
            run_a, run_b = last_a * run_a, last_a * run_b + last_b
        if begins:
            begin = gates(
                [base_ref[gate, pl.ds(begin_row, GROUP), lanes] for gate in range(3)],
                [products[tile][gate, pl.ds(0, GROUP), :] for gate in range(3)],
                inputs_ref[2, pl.ds(rows, GROUP), lanes],
                jnp.broadcast_to(init_ref[:, lanes], (GROUP, TILE)),
            )[-1]
            error = state_ref[pl.ds(0, GROUP), lanes] - begin
            squares = squares + jnp.where((row == 0) & is_first, error * error, 0.0)
            begin = begin[0:1]
            earlier = zeros[0:1]
        elif step == 0:
            begin, earlier = zeros[0:1], zeros[0:1]
        else:
            begin = before_ref[3:4, lanes]
            earlier = before_ref[2:3, lanes] if index == 0 else before_ref[4:5, lanes]
        total = jnp.sum(squares, axis=0, keepdims=True)
        if index:
            total = total + before_ref[2:3, lanes]
        ends_ref[0:1, lanes] = run_a[0:1]
        ends_ref[1:2, lanes] = run_b[0:1]
        ends_ref[2:3, lanes] = total
        ends_ref[3:4, lanes] = begin
        ends_ref[4:5, lanes] = earlier
        if last:
            send_a = jnp.where(is_first, 0.0, run_a[0:1])
            send_b = jnp.where(is_first, run_a[0:1] * begin + run_b[0:1], run_b[0:1])
            for at, sent in ((0, send_a), (width, send_b)):
                send_ref[:, :, pl.ds(at + tile * TILE, TILE)] = jnp.broadcast_to(sent[None], (copies, 1, TILE))

    dots(0)
    for tile in range(1, tiles):
        dots(tile)
        cells(tile - 1)
    cells(tiles - 1)
    if last and step == ITERS - 1:
        lane = lax.broadcasted_iota(jnp.int32, (1, LANES), 1)
        sums = jnp.zeros((1, LANES), F32)
        for line, half in ((4, 0), (2, 1)):
            part = sum(ends_ref[pl.ds(line, 1), pl.ds(at, LANES)] for at in range(0, width, LANES))
            part = part + pltpu.roll(part, LANES // 2, 1)
            sums = jnp.where(lane // (LANES // 2) == half, part, sums)
        send_ref[:, :, pl.ds(2 * width, LANES)] = jnp.broadcast_to(sums[None], (copies, 1, LANES))


def apply_kernel(step, *refs):
    final = step == ITERS - 1
    maps, refs = refs[: 2 * CHUNKS], refs[2 * CHUNKS :]
    begin_ref, all_ref, state_ref = refs[:3]
    outs = refs[3:]
    rows, width = state_ref.shape
    place = lax.axis_index("tm")
    peers = all_ref.shape[0]

    def compose(peer, enter):
        moved = all_ref[peer, :, pl.ds(0, width)] * enter + all_ref[peer, :, pl.ds(width, width)]
        return jnp.where(peer < place, moved, enter)

    enter = lax.fori_loop(0, peers, compose, begin_ref[3:4, :], unroll=min(peers, 8))
    height = 2 * GROUP
    row = lax.broadcasted_iota(jnp.int32, (height, width), 0)
    enter = jnp.broadcast_to(enter, (height, width))
    before = enter
    held = spans(step, rows)
    sent = held if final else spans(step + 1, rows)
    cuts = sorted({at for at, _ in held + sent} | {rows})
    for low, high in zip(cuts, cuts[1:]):
        source = max(place for place, (at, _) in enumerate(held) if at <= low)
        target = max(place for place, (at, _) in enumerate(sent) if at <= low)
        a_ref, b_ref = maps[2 * source], maps[2 * source + 1]

        def advance(group, before):
            at = low + group * height
            here = pl.ds(pl.multiple_of(at - held[source][0], height), height)
            token = pl.ds(pl.multiple_of(at, height), height)
            turned = pltpu.roll(a_ref[here, :] * enter + b_ref[here, :], 1, 0)
            moved = jnp.where(row == 0, before, turned)
            state_ref[token, :] = moved
            if not final:
                rounded = moved.astype(BF16)
                outs[1][token, :] = rounded
                outs[2 + target][pl.ds(pl.multiple_of(at - sent[target][0], height), height), :] = rounded
            return turned

        before = lax.fori_loop(0, (high - low) // height, advance, before, unroll=2)
    if not final:
        outs[0][...] = before[0:1]


def sums_kernel(all_ref, out_ref):
    out_ref[...] = jnp.sum(all_ref[:, :, pl.ds(all_ref.shape[2] - LANES, LANES)], axis=0)


def norm_kernel(size, *refs):
    *parts, out_ref = refs
    total = sum(part[...] for part in parts)
    lane = lax.broadcasted_iota(jnp.int32, (1, LANES), 1)
    for half in range(ITERS):
        out_ref[half] = jnp.sqrt(jnp.sum(jnp.where(lane // (LANES // 2) == half, total, 0.0)) / size)


def newton(token_ids, input_table, recur_weight, z_bias, hn_bias, init_state, guess):
    rows, width = guess.shape
    full = recur_weight.shape[0]
    count = lax.axis_size("hid")
    blocks_tm = lax.axis_size("tm")
    weight = jnp.transpose(recur_weight, (1, 0, 2))
    table = jnp.transpose(input_table, (1, 0, 2))

    first = spans(0, rows)[0][1]
    rounded, rest = lax.optimization_barrier((guess.astype(BF16), guess))
    opening = rounded[:first]
    whole, *moved = pl.pallas_call(
        merge_kernel,
        out_shape=[jax.ShapeDtypeStruct((rows + EXTRA, width), BF16)]
        + [
            jax.ShapeDtypeStruct((height + EXTRA * (at + height == rows), width), BF16)
            for at, height in spans(0, rows)[1:]
        ],
        in_specs=vmem(2),
        out_specs=vmem(CHUNKS),
        compiler_params=params(8),
        cost_estimate=cost(COVER, 8 * rows * width),
        name="merge",
    )(rounded, init_state[None])
    moved = [opening, *moved]
    inputs = pl.pallas_call(
        prepare_kernel,
        out_shape=jax.ShapeDtypeStruct((3, rows + GROUP, width), F32),
        in_specs=vmem(3),
        out_specs=vmem(1)[0],
        compiler_params=params(32),
        cost_estimate=cost(2 * COVER, 8 * rows * width),
        name="prepare",
    )(token_ids[None], table, z_bias[None])
    state = rest

    ends, diag = None, None
    for step in range(ITERS):
        final = step == ITERS - 1
        near = {0: whole}
        far = [{count // 2: None} for _ in range(CHUNKS)]
        for index in range(CHUNKS):
            far[index][count // 2] = swapped(moved[index], "hid", count // 2)
        bit = count // 4
        while bit:
            for offset in list(near):
                near[offset | bit] = swapped(near[offset], "hid", bit)
            for index in range(CHUNKS):
                for offset in list(far[index]):
                    far[index][offset | bit] = swapped(far[index][offset], "hid", bit)
            bit //= 2
        height = whole.shape[0]
        operands = [*[near[offset] for offset in range(count // 2)], weight, inputs, hn_bias[None]]
        outs = [jax.ShapeDtypeStruct((3, height, width), F32)]
        if step == 0:
            operands.append(state)
            outs.append(jax.ShapeDtypeStruct((1, 4 * width), F32))
        base, *line = pl.pallas_call(
            functools.partial(base_kernel, step, count),
            out_shape=outs,
            in_specs=vmem(len(operands)),
            out_specs=vmem(len(outs)),
            scratch_shapes=[pltpu.VMEM((height, full // 2), BF16)],
            compiler_params=params(16),
            cost_estimate=cost(3 * height * full * width, 3 * full * width),
        )(*operands)
        if step == 0:
            edge = from_next(line[0], "tm")
            following = edge
        maps = []
        for index, (start, chunk) in enumerate(spans(step, rows)):
            last = index == CHUNKS - 1
            height = moved[index].shape[0]
            split = splits(step, index, count)
            sums = base
            if split:
                sums = pl.pallas_call(
                    functools.partial(direct_kernel, start, count),
                    out_shape=jax.ShapeDtypeStruct((3, height, width), F32),
                    in_specs=vmem(3),
                    out_specs=vmem(1)[0],
                    compiler_params=params(16),
                    cost_estimate=cost(3 * height * full * width // 2, 3 * full * width),
                )(far[index][count // 2], weight, base)
            operands = [far[index][offset] for offset in range(count // 2 + split, count)]
            operands += [weight, sums, inputs, state, init_state[None]]
            if last:
                operands += [following, edge]
            if diag is not None:
                operands += [ends, diag]
            outs = [
                jax.ShapeDtypeStruct((chunk, width), F32),
                jax.ShapeDtypeStruct((chunk, width), F32),
                jax.ShapeDtypeStruct((5, width), F32),
            ]
            if diag is None:
                outs.append(jax.ShapeDtypeStruct((3 * GROUP, width), F32))
            copies = blocks_tm
            if last:
                outs.append(jax.ShapeDtypeStruct((copies, 1, 2 * width + final * LANES), F32))
            found = pl.pallas_call(
                functools.partial(step_kernel, count, index, start, chunk, step, copies),
                out_shape=outs,
                in_specs=vmem(len(operands)),
                out_specs=vmem(len(outs)),
                scratch_shapes=[pltpu.VMEM((height, full // 2), BF16)]
                + [pltpu.VMEM((3, height, TILE), F32)] * (width // TILE),
                compiler_params=params(32),
                cost_estimate=cost(height * full * 3 * width, 3 * full * width),
            )(*operands)
            maps += found[:2]
            ends = found[2]
            diag = found[3] if diag is None else diag
        every = lax.all_to_all(found[-1], "tm", 0, 0)
        outs = [jax.ShapeDtypeStruct((rows, width), F32)]
        if final:
            part = pl.pallas_call(
                sums_kernel,
                out_shape=jax.ShapeDtypeStruct((1, LANES), F32),
                in_specs=vmem(1),
                out_specs=vmem(1)[0],
                compiler_params=params(8),
                name="sums",
            )(every)
            parts = [part]
            for offset in range(1, count):
                parts.append(swapped(part, "hid", offset))
        else:
            outs.append(jax.ShapeDtypeStruct((1, width), F32))
            outs.append(jax.ShapeDtypeStruct((rows, width), BF16))
            outs += [jax.ShapeDtypeStruct((chunk, width), BF16) for _, chunk in spans(step + 1, rows)]
        result = pl.pallas_call(
            functools.partial(apply_kernel, step),
            out_shape=outs,
            in_specs=vmem(2 * CHUNKS + 2),
            out_specs=vmem(len(outs)),
            compiler_params=params(16),
            cost_estimate=cost(2 * rows * width, 16 * rows * width),
        )(*maps, ends, every)
        if final:
            residual_norm = pl.pallas_call(
                functools.partial(norm_kernel, blocks_tm * count * rows * width),
                out_shape=jax.ShapeDtypeStruct((ITERS,), F32),
                in_specs=vmem(count),
                out_specs=smem()[0],
                compiler_params=params(8),
                name="norm",
            )(*parts)
            return (result[0], residual_norm)
        state, following, whole, *moved = result


def solution(mesh):
    return jax.shard_map(
        newton,
        mesh=mesh,
        in_specs=(
            P("tm"),
            P(None, None, "hid"),
            P(None, None, "hid"),
            P("hid"),
            P("hid"),
            P("hid"),
            P("tm", "hid"),
        ),
        out_specs=(P("tm", "hid"), P()),
        check_vma=False,
    )
```
